32 devices in a mesh: cfg: 4 (over x, y), sp: 8 (over z, core).
Axes of the slice: x: 2, y: 2, z: 4, core: 2. Of those that a mesh axis runs over, the one named last changes fastest.
Arguments:
- x_txt: bfloat16 [2048, 3072], P(('cfg', 'sp')), parts along dimension 0
- x_img: bfloat16 [16384, 3072], P(('cfg', 'sp')), parts along dimension 0
- cond_vec: bfloat16 [4, 3072], P('cfg'), parts along dimension 0
- cos_img: float32 [4096, 64], P('sp')
- sin_img: float32 [4096, 64], P('sp')
- z_lat: float32 [16384, 64], P(('cfg', 'sp')), parts along dimension 0
- t_cur: float32 [1], replicated
- t_next: float32 [1], replicated
- w_mod: bfloat16 [2, 3072, 9216], replicated
- b_mod: bfloat16 [2, 9216], replicated
- w_in: bfloat16 [2, 3072, 21504], replicated
- b_in: bfloat16 [2, 21504], replicated
- qk_gain: bfloat16 [2, 2, 128], replicated
- w_out: bfloat16 [2, 15360, 3072], replicated
- b_out: bfloat16 [2, 3072], replicated
- w_fmod: bfloat16 [3072, 6144], replicated
- b_fmod: bfloat16 [6144], replicated
- w_final: bfloat16 [3072, 64], replicated
- b_final: bfloat16 [64], replicated
Outputs:
- output: float32 [16384, 64], P(('cfg', 'sp')), parts along dimension 0
There are 4 independent parts. The reference program is written for one: setup_inputs(seed, part) draws one part's arguments, and reference() takes and returns one part's arrays. A program takes and returns all parts, laid end to end along the dimension named above; an argument that names none is the same for every part.
All inputs are finite; a program needn't handle non-finite values.
Results may differ from the reference program's by a relative error of at most 0.00454191.
Values are sent between devices in bfloat16 or wider.
A program may use at most 2.5 GiB of HBM per device.

```python
import math
import jax
import jax.numpy as jnp
from jax import lax

D = 3072
HEADS = 24
HEAD = 128
TEXT = 512
IMG = 4096
LAYERS = 2
OUT_CH = 64
QBLK = 128

FF = D * 4
TOTAL = TEXT + IMG
HALF = HEAD // 2
AXIS_T = HALF // 8
AXIS_H = (HALF - AXIS_T) // 2
AXIS_W = HALF - AXIS_T - AXIS_H
EPS = 1e-6
SCORE_SCALE = 1.0 / math.sqrt(HEAD)
LOG_THETA = math.log(10000.0)


def rope_tables(key):
    grid_keys = jax.random.split(key, 3)
    grid_width = jnp.left_shift(jnp.int32(1), jax.random.randint(grid_keys[0], (), 3, 7))
    row_off = jax.random.randint(grid_keys[1], (), 0, 64)
    col_off = jax.random.randint(grid_keys[2], (), 0, 64)
    token_index = jnp.arange(IMG, dtype=jnp.int32)
    grid_rows = (token_index // grid_width + row_off).astype(jnp.float32)
    grid_cols = (token_index % grid_width + col_off).astype(jnp.float32)
    freq_h = jnp.exp(-LOG_THETA * jnp.arange(AXIS_H, dtype=jnp.float32) / AXIS_H)
    freq_w = jnp.exp(-LOG_THETA * jnp.arange(AXIS_W, dtype=jnp.float32) / AXIS_W)
    angles = jnp.concatenate([jnp.zeros((IMG, AXIS_T), jnp.float32), grid_rows[:, None] * freq_h[None, :], grid_cols[:, None] * freq_w[None, :]], axis=1)
    return jnp.cos(angles), jnp.sin(angles)


def setup_inputs(seed: int = 0, part: int = 0) -> dict:
    part_keys = jax.random.split(jax.random.fold_in(jax.random.key(seed), part), 5)
    shared_keys = jax.random.split(jax.random.key(seed + 1), 16)
    fan_d = D ** -0.5
    fan_ff = FF ** -0.5
    common_txt = jax.random.normal(part_keys[0], (1, D), jnp.float32)
    x_txt = (jax.random.normal(part_keys[1], (TEXT, D), jnp.float32) + common_txt).astype(jnp.bfloat16)
    x_img = jax.random.normal(part_keys[2], (IMG, D), jnp.float32).astype(jnp.bfloat16)
    cond_vec = jax.random.normal(part_keys[3], (1, D), jnp.float32).astype(jnp.bfloat16)
    z_lat = 0.5 * jax.random.normal(part_keys[4], (IMG, OUT_CH), jnp.float32)
    cos_img, sin_img = rope_tables(shared_keys[0])
    t_cur = jax.random.uniform(shared_keys[1], (1,), jnp.float32, 0.3, 0.9)
    t_next = t_cur - jax.random.uniform(shared_keys[2], (1,), jnp.float32, 0.06, 0.14)
    row_gain = jnp.concatenate([jnp.full((D,), fan_d, jnp.float32), jnp.full((FF,), fan_ff, jnp.float32)])
    return {
        'x_txt': x_txt,
        'x_img': x_img,
        'cond_vec': cond_vec,
        'cos_img': cos_img,
        'sin_img': sin_img,
        'z_lat': z_lat,
        't_cur': t_cur,
        't_next': t_next,
        'w_mod': (fan_d * jax.random.normal(shared_keys[3], (LAYERS, D, 3 * D), jnp.float32)).astype(jnp.bfloat16),
        'b_mod': (0.5 * jax.random.normal(shared_keys[4], (LAYERS, 3 * D), jnp.float32)).astype(jnp.bfloat16),
        'w_in': (fan_d * jax.random.normal(shared_keys[5], (LAYERS, D, 7 * D), jnp.float32)).astype(jnp.bfloat16),
        'b_in': (0.5 * jax.random.normal(shared_keys[6], (LAYERS, 7 * D), jnp.float32)).astype(jnp.bfloat16),
        'qk_gain': (2.0 + 0.3 * jax.random.normal(shared_keys[7], (LAYERS, 2, HEAD), jnp.float32)).astype(jnp.bfloat16),
        'w_out': (jax.random.normal(shared_keys[8], (LAYERS, D + FF, D), jnp.float32) * row_gain[None, :, None]).astype(jnp.bfloat16),
        'b_out': (0.3 * jax.random.normal(shared_keys[9], (LAYERS, D), jnp.float32)).astype(jnp.bfloat16),
        'w_fmod': (fan_d * jax.random.normal(shared_keys[10], (D, 2 * D), jnp.float32)).astype(jnp.bfloat16),
        'b_fmod': (0.5 * jax.random.normal(shared_keys[11], (2 * D,), jnp.float32)).astype(jnp.bfloat16),
        'w_final': (2.0 * fan_d * jax.random.normal(shared_keys[12], (D, OUT_CH), jnp.float32)).astype(jnp.bfloat16),
        'b_final': (0.5 * jax.random.normal(shared_keys[13], (OUT_CH,), jnp.float32)).astype(jnp.bfloat16),
    }


def layer_norm(x_rows):
    x_f32 = x_rows.astype(jnp.float32)
    centered = x_f32 - jnp.mean(x_f32, axis=-1, keepdims=True)
    return centered * lax.rsqrt(jnp.mean(centered * centered, axis=-1, keepdims=True) + EPS)


def head_norm(head_vals, gain_vec):
    vals_f32 = head_vals.astype(jnp.float32)
    return vals_f32 * lax.rsqrt(jnp.mean(vals_f32 * vals_f32, axis=-1, keepdims=True) + EPS) * gain_vec.astype(jnp.float32)


def rotate(head_vals, cos_tab, sin_tab):
    lead_half = head_vals[..., :HALF]
    tail_half = head_vals[..., HALF:]
    cos_b = cos_tab[:, None, :]
    sin_b = sin_tab[:, None, :]
    return jnp.concatenate([lead_half * cos_b - tail_half * sin_b, lead_half * sin_b + tail_half * cos_b], axis=-1)


def attend(q_all, k_all, v_all):
    def per_head(operands):
        q_head, k_head, v_head = operands
        key_full = k_head.astype(jnp.float32)
        value_full = v_head.astype(jnp.float32)

        def per_block(q_block):
            scores = jnp.dot(q_block.astype(jnp.float32), key_full.T) * SCORE_SCALE
            return jnp.dot(jax.nn.softmax(scores, axis=-1), value_full)

        head_out = lax.map(per_block, q_head.reshape(TOTAL // QBLK, QBLK, HEAD))
        return head_out.reshape(TOTAL, HEAD)

    per_heads = lax.map(per_head, (jnp.transpose(q_all, (1, 0, 2)), jnp.transpose(k_all, (1, 0, 2)), jnp.transpose(v_all, (1, 0, 2))))
    return jnp.transpose(per_heads, (1, 0, 2)).reshape(TOTAL, D)


def single_block(x_all, mod_in, cos_all, sin_all, weights):
    w_mod, b_mod, w_in, b_in, qk_gain, w_out, b_out = weights
    mod_vals = jnp.dot(mod_in, w_mod, preferred_element_type=jnp.float32) + b_mod.astype(jnp.float32)
    shift_m = mod_vals[:, :D]
    scale_m = mod_vals[:, D:2 * D]
    gate_m = mod_vals[:, 2 * D:]
    normed = (layer_norm(x_all) * (1.0 + scale_m) + shift_m).astype(jnp.bfloat16)
    proj_rows = (jnp.dot(normed, w_in, preferred_element_type=jnp.float32) + b_in.astype(jnp.float32)).astype(jnp.bfloat16)
    q_rows = proj_rows[:, :D].reshape(TOTAL, HEADS, HEAD)
    k_rows = proj_rows[:, D:2 * D].reshape(TOTAL, HEADS, HEAD)
    v_rows = proj_rows[:, 2 * D:3 * D].reshape(TOTAL, HEADS, HEAD)
    q_rot = rotate(head_norm(q_rows, qk_gain[0]), cos_all, sin_all).astype(jnp.bfloat16)
    k_rot = rotate(head_norm(k_rows, qk_gain[1]), cos_all, sin_all).astype(jnp.bfloat16)
    attended = attend(q_rot, k_rot, v_rows).astype(jnp.bfloat16)
    mlp_act = jax.nn.gelu(proj_rows[:, 3 * D:].astype(jnp.float32), approximate=True).astype(jnp.bfloat16)
    update = jnp.dot(attended, w_out[:D], preferred_element_type=jnp.float32) + jnp.dot(mlp_act, w_out[D:], preferred_element_type=jnp.float32) + b_out.astype(jnp.float32)
    return (x_all.astype(jnp.float32) + gate_m * update).astype(jnp.bfloat16)


def reference(x_txt, x_img, cond_vec, cos_img, sin_img, z_lat, t_cur, t_next, w_mod, b_mod, w_in, b_in, qk_gain, w_out, b_out, w_fmod, b_fmod, w_final, b_final):
    mod_in = jax.nn.silu(cond_vec.astype(jnp.float32)).astype(jnp.bfloat16)
    cos_all = jnp.concatenate([jnp.ones((TEXT, HALF), jnp.float32), cos_img], axis=0)
    sin_all = jnp.concatenate([jnp.zeros((TEXT, HALF), jnp.float32), sin_img], axis=0)

    def layer_step(x_carry, weights):
        return single_block(x_carry, mod_in, cos_all, sin_all, weights), None

    x_last, scan_rest = lax.scan(layer_step, jnp.concatenate([x_txt, x_img], axis=0), (w_mod, b_mod, w_in, b_in, qk_gain, w_out, b_out))
    fmod_vals = jnp.dot(mod_in, w_fmod, preferred_element_type=jnp.float32) + b_fmod.astype(jnp.float32)
    final_in = (layer_norm(x_last[TEXT:]) * (1.0 + fmod_vals[:, D:]) + fmod_vals[:, :D]).astype(jnp.bfloat16)
    velocity = jnp.dot(final_in, w_final, preferred_element_type=jnp.float32) + b_final.astype(jnp.float32)
    return z_lat + (t_next - t_cur) * velocity
```

```python
import functools
import math

import jax
import jax.numpy as jnp
from jax import lax
from jax.experimental import pallas as pl
from jax.experimental.pallas import tpu as pltpu
from jax.sharding import Mesh, PartitionSpec as P

EPS = 1e-6
LANES = 128
GELU_C = math.sqrt(2.0 / math.pi)
LOG2E = math.log2(math.e)
VMEM_BYTES = 60 * 2**20
PLANE = ('cfg', 'core')


def params(**kw):
    return pltpu.CompilerParams(vmem_limit_bytes=VMEM_BYTES, dimension_semantics=('arbitrary',), **kw)


def ln_mod(x, shift, scale):
    centered = x - jnp.mean(x, axis=-1, keepdims=True)
    var = jnp.mean(centered * centered, axis=-1, keepdims=True)
    return (centered * lax.rsqrt(var + EPS) * (1.0 + scale) + shift).astype(jnp.bfloat16)


def gelu_tanh(u):
    return u * (0.5 * (1.0 + jnp.tanh(GELU_C * (u + 0.044715 * (u * u * u)))))


def mlp_kernel(h_ref, w1_ref, b1_ref, w2_ref, y_ref, u_scr, act, *, row0, n, sub):
    i = pl.program_id(0)
    rows = y_ref.shape[0]
    step = rows // sub

    def up():
        for r in range(sub):
            u = jnp.dot(h_ref[row0 + r * step:row0 + (r + 1) * step, :], w1_ref[0], preferred_element_type=jnp.float32)
            u_scr[r * step:(r + 1) * step, :] = (u + b1_ref[0].astype(jnp.float32)).astype(jnp.bfloat16)

    def gelu():
        act[...] = gelu_tanh(u_scr[...].astype(jnp.float32)).astype(jnp.bfloat16)

    def down(first=False):
        for r in range(sub):
            rs = slice(r * step, (r + 1) * step)
            d = jnp.dot(act[rs, :], w2_ref[0], preferred_element_type=jnp.float32)
            if first:
                y_ref[rs, :] = d
            else:
                y_ref[rs, :] += d

    @pl.when(i == 0)
    def _():
        up()

    @pl.when(i == 1)
    def _():
        gelu()
        up()
        down(True)

    @pl.when((i > 1) & (i < n))
    def _():
        gelu()
        up()
        down()

    @pl.when(i == n)
    def _():
        gelu()
        down()


def mlp(h, w_in, b_in3, w_out, layer, row0, hc=512, sub=2):
    rows, d = h.shape
    ff = w_in.shape[2] - 3 * d
    n = ff // hc
    m = rows - row0
    return pl.pallas_call(
        functools.partial(mlp_kernel, row0=row0, n=n, sub=sub),
        grid=(n + 1,),
        in_specs=[
            pl.BlockSpec((rows, d), lambda i: (0, 0)),
            pl.BlockSpec((1, d, hc), lambda i: (layer, 0, 3 * d // hc + jnp.minimum(i, n - 1))),
            pl.BlockSpec((1, 1, hc), lambda i: (layer, 0, 3 * d // hc + jnp.minimum(i, n - 1))),
            pl.BlockSpec((1, hc, d), lambda i: (layer, d // hc + jnp.maximum(i - 1, 0), 0)),
        ],
        out_specs=pl.BlockSpec((m, d), lambda i: (0, 0)),
        out_shape=jax.ShapeDtypeStruct((m, d), jnp.float32),
        scratch_shapes=[pltpu.VMEM((m, hc), jnp.bfloat16)] * 2,
        compiler_params=params(),
        cost_estimate=pl.CostEstimate(flops=4 * m * d * ff, bytes_accessed=4 * d * ff, transcendentals=m * ff),
        name='mlp',
    )(h, w_in, b_in3, w_out)


def qkv_kernel(head_ref, H_ref, *refs, nh, rb, n_img, n_txt):
    nw = 3 * nh
    w_refs, b_refs = refs[:nw], refs[nw:2 * nw]
    gain_ref, cs_ref, qT_ref, k_ref, vT_ref, wt, bb, gg, hbuf, sem = refs[2 * nw:]
    i = pl.program_id(0)
    n_dev = H_ref.shape[0]
    per = n_img // rb
    n_steps = n_dev * per + 1

    def fetch(step, slot):
        @pl.when(step < n_dev * per)
        def _():
            dev, part = step // per, lax.rem(step, per)
            pltpu.make_async_copy(H_ref.at[dev, pl.ds(n_txt + part * rb, rb), :], hbuf.at[slot], sem.at[slot]).start()

        @pl.when(step == n_dev * per)
        def _():
            for t in range(n_dev):
                pltpu.make_async_copy(H_ref.at[t, pl.ds(0, n_txt), :], hbuf.at[slot, pl.ds(t * n_txt, n_txt), :], sem.at[slot]).start()

    slot = lax.rem(i, 2)

    @pl.when(i == 0)
    def _():
        fetch(0, 0)

    @pl.when(i + 1 < n_steps)
    def _():
        fetch(i + 1, 1 - slot)

    @pl.when(i == 0)
    def _():
        for j in range(nw):
            wt[j * LANES:(j + 1) * LANES, :] = w_refs[j][0].T
            bb[j * LANES:(j + 1) * LANES, :] = jnp.broadcast_to(b_refs[j][0].astype(jnp.float32), (LANES, LANES)).T
        for j in range(2):
            gg[j * LANES:(j + 1) * LANES, :] = jnp.broadcast_to(gain_ref[0, j:j + 1, :].astype(jnp.float32), (LANES, LANES)).T

    pltpu.make_async_copy(H_ref.at[0, pl.ds(0, rb), :], hbuf.at[slot], sem.at[slot]).wait()
    h = hbuf[slot]
    half = LANES // 2
    cos, sin = cs_ref[0:half, :], cs_ref[half:LANES, :]

    def lanes(v):
        return jnp.concatenate([v] * (rb // LANES), axis=1)

    def proj(part):
        rows = slice(part * nh * LANES, (part + 1) * nh * LANES)
        return lax.dot_general(wt[rows, :], h, (((1,), (1,)), ((), ())), preferred_element_type=jnp.float32)

    def bias(x, j):
        return (x + lanes(bb[j * LANES:(j + 1) * LANES, :])).astype(jnp.bfloat16)

    def normed(x, j, g):
        x = bias(x, j).astype(jnp.float32)
        ms = jnp.sum(x * x, axis=0, keepdims=True) * (1.0 / LANES)
        y = x * lax.rsqrt(ms + EPS) * lanes(gg[g * LANES:(g + 1) * LANES, :])
        a, b = y[:half], y[half:]
        return jnp.concatenate([a * cos - b * sin, a * sin + b * cos], axis=0).astype(jnp.bfloat16)

    q = proj(0)
    for t in range(nh):
        qT_ref[t] = normed(q[t * LANES:(t + 1) * LANES], t, 0)
    k = proj(1)
    for t in range(nh):
        k_ref[t] = normed(k[t * LANES:(t + 1) * LANES], nh + t, 1).T
    v = proj(2)
    for t in range(nh):
        vT_ref[t] = bias(v[t * LANES:(t + 1) * LANES], 2 * nh + t)


def qkv(H, head, w_in, b_in3, qk_gain, cs, layer, n_txt, nh):
    n_dev, rows, d = H.shape
    rb = n_dev * n_txt
    n_img = rows - n_txt
    n_heads = d // LANES
    S = n_dev * rows
    stride = n_heads // nh
    steps = n_dev * (n_img // rb) + 1
    blocks = [(p, t) for p in range(3) for t in range(nh)]
    w_specs = [pl.BlockSpec((1, d, LANES), lambda i, r, p=p, t=t: (layer, 0, p * n_heads + t * stride + r[0]), pipeline_mode=pl.Buffered(1)) for p, t in blocks]
    b_specs = [pl.BlockSpec((1, 1, LANES), lambda i, r, p=p, t=t: (layer, 0, p * n_heads + t * stride + r[0])) for p, t in blocks]
    return pl.pallas_call(
        functools.partial(qkv_kernel, nh=nh, rb=rb, n_img=n_img, n_txt=n_txt),
        grid_spec=pltpu.PrefetchScalarGridSpec(
            num_scalar_prefetch=1,
            grid=(steps,),
            in_specs=[pl.BlockSpec(memory_space=pl.ANY)] + w_specs + b_specs + [
                pl.BlockSpec((1, 2, LANES), lambda i, r: (layer, 0, 0)),
                pl.BlockSpec((LANES, rb), lambda i, r: (0, i)),
            ],
            out_specs=[
                pl.BlockSpec((nh, LANES, rb), lambda i, r: (0, 0, i)),
                pl.BlockSpec((nh, rb, LANES), lambda i, r: (0, i, 0)),
                pl.BlockSpec((nh, LANES, rb), lambda i, r: (0, 0, i)),
            ],
            scratch_shapes=[
                pltpu.VMEM((3 * nh * LANES, d), jnp.bfloat16),
                pltpu.VMEM((3 * nh * LANES, LANES), jnp.float32),
                pltpu.VMEM((2 * LANES, LANES), jnp.float32),
                pltpu.VMEM((2, rb, d), jnp.bfloat16),
                pltpu.SemaphoreType.DMA((2,)),
            ],
        ),
        out_shape=[
            jax.ShapeDtypeStruct((nh, LANES, S), jnp.bfloat16),
            jax.ShapeDtypeStruct((nh, S, LANES), jnp.bfloat16),
            jax.ShapeDtypeStruct((nh, LANES, S), jnp.bfloat16),
        ],
        compiler_params=params(),
        cost_estimate=pl.CostEstimate(flops=6 * S * d * nh * LANES, bytes_accessed=2 * S * d + 6 * nh * LANES * d, transcendentals=0),
        name='qkv',
    )(head, H, *([w_in] * (3 * nh)), *([b_in3] * (3 * nh)), qk_gain, cs)


def attn_kernel(qT_ref, k_ref, vT_ref, o_ref, s_scr, m_scr, *, qt, kc, n_img, n_txt, with_txt):
    S, hd = k_ref.shape[1:]
    nk = S // kc
    n_dev = o_ref.shape[0]
    c = hd ** -0.5 * LOG2E
    n_img_tiles = n_dev * n_img // qt
    nq = n_img_tiles + (n_dev * n_txt // qt if with_txt else 0)
    per = n_img // qt

    def score_chunk(q, slot, i, m):
        s = jnp.dot(k_ref[0, pl.ds(i * kc, kc), :], q, preferred_element_type=jnp.float32)
        s_scr[slot, pl.ds(i * kc, kc), :] = s
        return jnp.maximum(m, jnp.max(s.reshape(kc // 8, 8, qt), axis=0))

    def finish_max(m, slot):
        m_scr[slot] = jnp.broadcast_to(jnp.max(m, axis=0, keepdims=True) * c, (8, qt))

    def prob_chunk(mc, slot, i, l, acc):
        s = s_scr[slot, pl.ds(i * kc, kc), :].reshape(kc // 8, 8, qt)
        p = jnp.exp2(s * c - mc[None])
        l = l + jnp.sum(p, axis=0)
        d = jnp.dot(vT_ref[0, :, pl.ds(i * kc, kc)], p.reshape(kc, qt).astype(jnp.bfloat16), preferred_element_type=jnp.float32)
        return l, acc + d

    def emit(t, l, acc, txt):
        o = (acc / jnp.sum(l, axis=0, keepdims=True)).T.astype(o_ref.dtype)
        if txt:
            first = (t - n_img_tiles) * (qt // n_txt)
            for a in range(qt // n_txt):
                o_ref[first + a, 0:n_txt, :] = o[a * n_txt:(a + 1) * n_txt]
        else:
            o_ref[t // per, pl.ds(pl.multiple_of((n_txt if with_txt else 0) + lax.rem(t, per) * qt, 16), qt), :] = o

    def load_q(t):
        return qT_ref[0, :, pl.ds(pl.multiple_of(t * qt, qt), qt)]

    def empty():
        return jnp.zeros((8, qt), jnp.float32), jnp.zeros((hd, qt), jnp.float32)

    def both(t, slot, txt=False):
        q = load_q(t + 1)
        m = jnp.full((8, qt), -jnp.inf, jnp.float32)
        l, acc = empty()
        mc = m_scr[slot]
        for i in range(nk):
            m = score_chunk(q, 1 - slot, i, m)
            l, acc = prob_chunk(mc, slot, i, l, acc)
        finish_max(m, 1 - slot)
        emit(t, l, acc, txt)

    q = load_q(0)
    m = jnp.full((8, qt), -jnp.inf, jnp.float32)
    for i in range(nk):
        m = score_chunk(q, 0, i, m)
    finish_max(m, 0)

    def pair(t2, carry):
        both(2 * t2, 0)
        both(2 * t2 + 1, 1)
        return carry

    pairs = min((nq - 1) // 2, n_img_tiles // 2)
    lax.fori_loop(0, pairs, pair, 0)
    for t in range(2 * pairs, nq - 1):
        both(t, t % 2, t >= n_img_tiles)
    slot = (nq - 1) % 2
    l, acc = empty()
    mc = m_scr[slot]
    for i in range(nk):
        l, acc = prob_chunk(mc, slot, i, l, acc)
    emit(nq - 1, l, acc, nq - 1 >= n_img_tiles)


def largest(n, cap, unit):
    return max(c for c in range(unit, cap + 1, unit) if n % c == 0)


def attention(qT, k, vT, head, n_dev, n_txt, with_txt, qt=256):
    _, S, hd = k.shape
    rows = S // n_dev
    n_img = rows - n_txt
    out_rows = rows if with_txt else n_img
    kc = largest(S, 768, 256)
    SQ = n_dev * out_rows
    return pl.pallas_call(
        functools.partial(attn_kernel, qt=qt, kc=kc, n_img=n_img, n_txt=n_txt, with_txt=with_txt),
        grid=(1,),
        in_specs=[
            pl.BlockSpec((1, hd, S), lambda i: (head, 0, 0)),
            pl.BlockSpec((1, S, hd), lambda i: (head, 0, 0)),
            pl.BlockSpec((1, hd, S), lambda i: (head, 0, 0)),
        ],
        out_specs=pl.BlockSpec((n_dev, out_rows, hd), lambda i: (0, 0, 0)),
        out_shape=jax.ShapeDtypeStruct((n_dev, out_rows, hd), jnp.bfloat16),
        scratch_shapes=[pltpu.VMEM((2, S, qt), jnp.float32), pltpu.VMEM((2, 8, qt), jnp.float32)],
        compiler_params=params(),
        cost_estimate=pl.CostEstimate(flops=6 * SQ * S * hd, bytes_accessed=8 * S * hd, transcendentals=S * SQ),
        name='attn',
    )(qT, k, vT)


def out_kernel(*refs, nh, nc, ne, row0, last):
    o_refs = refs[:nh]
    if last:
        w_ref, bo_ref, mods_ref, wf_ref, bf_ref, x_hbm, y_hbm, vel_ref, lhs, acc, ybuf, xbuf, hs, sems = refs[nh:]
    else:
        w_ref, bo_ref, mods_ref, x_hbm, y_hbm, xo_ref, ho_ref, lhs, acc, ybuf, xbuf, sems = refs[nh:]
    i = pl.program_id(0)
    R = acc.shape[0]
    er = R // ne
    per = nc // nh
    hp = lhs.shape[1] // LANES
    copy_y = pltpu.make_async_copy(y_hbm, ybuf, sems.at[0])
    copy_x = pltpu.make_async_copy(x_hbm.at[pl.ds(row0, R), :], xbuf, sems.at[1])

    @pl.when(i == 0)
    def _():
        copy_y.start()
        copy_x.start()

    for j in range(nh):
        @pl.when((i >= j * per) & (i < (j + 1) * per))
        def _():
            for t in range(hp):
                lhs[:, t * LANES:(t + 1) * LANES] = o_refs[j][t]

    @pl.when(i == 0)
    def _():
        acc[...] = jnp.dot(lhs[...], w_ref[0], preferred_element_type=jnp.float32)

    @pl.when((i > 0) & (i < nc))
    def _():
        acc[...] += jnp.dot(lhs[...], w_ref[0], preferred_element_type=jnp.float32)

    @pl.when(i == nc)
    def _():
        copy_y.wait()
        copy_x.wait()

    @pl.when(i >= nc)
    def _():
        gate, shift, scale = mods_ref[0:1, :], mods_ref[1:2, :], mods_ref[2:3, :]
        bo = bo_ref[0].astype(jnp.float32)
        sub = 16

        def chunk(c, carry):
            rs = pl.ds(pl.multiple_of((i - nc) * er + c * sub, sub), sub)
            ls = pl.ds(pl.multiple_of(c * sub, sub), sub)
            y = acc[rs, :] + ybuf[rs, :] + bo
            xn = (xbuf[rs, :].astype(jnp.float32) + gate * y).astype(jnp.bfloat16)
            h = ln_mod(xn.astype(jnp.float32), shift, scale)
            if last:
                hs[ls, :] = h
            else:
                xo_ref[ls, :] = xn
                ho_ref[ls, :] = h
            return carry

        lax.fori_loop(0, er // sub, chunk, 0, unroll=3 if (er // sub) % 3 == 0 else 2)
        if last:
            vel_ref[...] = jnp.dot(hs[...], wf_ref[...], preferred_element_type=jnp.float32) + bf_ref[...].astype(jnp.float32)


def out_proj(os, w_out, b_out3, mods, x, y_mlp, layer, row0, final=None, kc=512):
    nh = len(os)
    _, R, _ = os[0].shape
    ne = 4 if R % 64 == 0 else 2
    d = w_out.shape[2]
    nc = d // kc
    per = nc // nh
    hp = kc // LANES
    last = final is not None
    in_specs = [pl.BlockSpec((hp, R, LANES), lambda i, j=j: (jnp.clip(i - j * per, 0, per - 1), 0, 0)) for j in range(nh)] + [
        pl.BlockSpec((1, kc, d), lambda i: (layer, jnp.minimum(i, nc - 1), 0)),
        pl.BlockSpec((1, 1, d), lambda i: (layer, 0, 0)),
        pl.BlockSpec((8, d), lambda i: (0, 0)),
    ]
    args = [*os, w_out, b_out3, mods]
    scratch = [pltpu.VMEM((R, kc), jnp.bfloat16), pltpu.VMEM((R, d), jnp.float32), pltpu.VMEM((R, d), jnp.float32), pltpu.VMEM((R, d), jnp.bfloat16)]
    if last:
        n_out = final[0].shape[1]
        in_specs += [pl.BlockSpec((d, n_out), lambda i: (0, 0)), pl.BlockSpec((1, n_out), lambda i: (0, 0))]
        args += list(final)
        out_specs = pl.BlockSpec((R // ne, n_out), lambda i: (jnp.maximum(i - nc, 0), 0))
        out_shape = jax.ShapeDtypeStruct((R, n_out), jnp.float32)
        scratch.append(pltpu.VMEM((R // ne, d), jnp.bfloat16))
    else:
        out_specs = [pl.BlockSpec((R // ne, d), lambda i: (jnp.maximum(i - nc, 0), 0))] * 2
        out_shape = [jax.ShapeDtypeStruct((R, d), jnp.bfloat16)] * 2
    return pl.pallas_call(
        functools.partial(out_kernel, nh=nh, nc=nc, ne=ne, row0=row0, last=last),
        grid=(nc + ne,),
        in_specs=in_specs + [pl.BlockSpec(memory_space=pl.ANY)] * 2,
        out_specs=out_specs,
        out_shape=out_shape,
        scratch_shapes=scratch + [pltpu.SemaphoreType.DMA((2,))],
        compiler_params=params(),
        cost_estimate=pl.CostEstimate(flops=2 * R * d * d, bytes_accessed=2 * d * d + 14 * R * d, transcendentals=0),
        name='outp',
    )(*args, x, y_mlp)


def solution(mesh):
    n_cfg = mesh.devices.shape[0]
    n_core = 2
    n_z = mesh.devices.shape[1] // n_core
    grid = Mesh(mesh.devices.reshape(n_cfg, n_z, n_core), ('cfg', 'z', 'core'))
    assert n_cfg == n_z
    n_dev = n_cfg * n_core
    token_spec = P(('cfg', 'z', 'core'), None)
    seq_spec = P(('z', 'core'), None)
    in_specs = (token_spec, token_spec, P('cfg', None), seq_spec, seq_spec, token_spec) + (P(),) * 13

    def to_plane(v):
        return lax.all_to_all(lax.all_to_all(v, 'cfg', 0, 0), 'z', 0, 0)

    def from_plane(v):
        return lax.all_to_all(lax.all_to_all(v, 'z', 0, 0), 'cfg', 0, 0)

    def body(x_txt, x_img, cond_vec, cos_img, sin_img, z_lat, t_cur, t_next, w_mod, b_mod, w_in, b_in, qk_gain, w_out, b_out, w_fmod, b_fmod, w_final, b_final):
        n_txt, d = x_txt.shape
        n_img = x_img.shape[0]
        n_layers = w_mod.shape[0]
        nh = d // LANES // n_dev
        half = cos_img.shape[1]
        tp, ip = n_txt // n_cfg, n_img // n_cfg
        f32 = jnp.float32

        pieces = to_plane(jnp.concatenate([x_txt.reshape(n_cfg, tp, d), x_img.reshape(n_cfg, ip, d)], axis=1))
        x = jnp.concatenate([pieces[:, :tp].reshape(n_txt, d), pieces[:, tp:].reshape(n_img, d)], axis=0)

        conds = lax.all_gather(cond_vec[0], 'cfg')
        cond = lax.dynamic_slice_in_dim(conds, lax.axis_index('z'), 1, 0)
        s = jax.nn.silu(cond.astype(f32)).astype(jnp.bfloat16)

        def modulation(w, b):
            return (jnp.dot(s, w, preferred_element_type=f32) + b.astype(f32)[None]).reshape(-1, d)

        mods = [modulation(w_mod[l], b_mod[l]) for l in range(n_layers)]
        fmod = modulation(w_fmod, b_fmod)

        tables = jnp.concatenate([cos_img, sin_img], axis=1)
        own = lax.dynamic_slice_in_dim(tables, lax.axis_index('cfg') * ip, ip, 0)
        own = lax.all_gather(own, 'z').reshape(n_img, 2 * half)
        cs = lax.all_gather(own, PLANE).reshape(n_dev * n_img, 2 * half).T
        plain = jnp.concatenate([jnp.ones((half, n_dev * n_txt), f32), jnp.zeros((half, n_dev * n_txt), f32)], axis=0)
        cs = jnp.concatenate([cs, plain], axis=1)

        head = (lax.axis_index('cfg') * n_core + lax.axis_index('core')).astype(jnp.int32).reshape(1)
        b_in3, b_out3 = b_in[:, None, :], b_out[:, None, :]
        x, h = lax.optimization_barrier((x, ln_mod(x.astype(f32), mods[0][0:1], mods[0][1:2])))
        for l in range(n_layers):
            last = l == n_layers - 1
            row0 = n_txt if last else 0
            gathered = lax.all_gather(h, PLANE)
            gathered, y_mlp = lax.optimization_barrier((gathered, mlp(h, w_in, b_in3, w_out, l, row0)))
            qT, k, vT = qkv(gathered, head, w_in, b_in3, qk_gain, cs, l, n_txt, nh)
            os = []
            for t in range(nh):
                o = attention(qT, k, vT, t, n_dev, n_txt, not last)
                os.append(lax.all_to_all(o, PLANE, 0, 0))
            following = fmod if last else mods[l + 1]
            rows = jnp.concatenate([mods[l][2:3], following[0:1], following[1:2], jnp.zeros((5, d), f32)], axis=0)
            if last:
                vel = out_proj(os, w_out, b_out3, rows, x, y_mlp, l, row0, final=(w_final, b_final[None]))
            else:
                x, h = out_proj(os, w_out, b_out3, rows, x, y_mlp, l, row0)

        back = from_plane(vel.reshape(n_z, ip, vel.shape[1])).reshape(n_img, vel.shape[1])
        return z_lat + (t_next - t_cur) * back

    return jax.shard_map(body, mesh=grid, in_specs=in_specs, out_specs=token_spec, check_vma=False)
```

```python
import functools
import math

import jax
import jax.numpy as jnp
from jax import lax
from jax.experimental import pallas as pl
from jax.experimental.pallas import tpu as pltpu
from jax.sharding import Mesh, PartitionSpec as P

EPS = 1e-6
LANES = 128
GELU_C = math.sqrt(2.0 / math.pi)
LOG2E = math.log2(math.e)
VMEM_BYTES = 60 * 2**20
N_CORE = 2
MESH = pl.DeviceIdType.MESH


def params(**kw):
    return pltpu.CompilerParams(vmem_limit_bytes=VMEM_BYTES, dimension_semantics=('arbitrary',), **kw)


def talking(collective_id):
    return dict(collective_id=collective_id, has_side_effects=True)


def whole(shape, **kw):
    return pl.BlockSpec(shape, lambda i: (0,) * len(shape), **kw)


def head_rows(j):
    return slice(j * LANES, (j + 1) * LANES)


def columns_of(v):
    return jnp.broadcast_to(v.astype(jnp.float32), (LANES, LANES)).T


def wait_for(ref, sem):
    pltpu.make_async_copy(ref, ref, sem).wait()


def dot(a, b):
    return jnp.dot(a, b, preferred_element_type=jnp.float32)


def remote(src, dst, send_sem, recv_sem, device):
    return pltpu.make_async_remote_copy(src_ref=src, dst_ref=dst, send_sem=send_sem, recv_sem=recv_sem, device_id=device, device_id_type=MESH)


def meet(devices):
    barrier = pltpu.get_barrier_semaphore()
    for device in devices:
        pl.semaphore_signal(barrier, inc=1, device_id=device, device_id_type=MESH)
    pl.semaphore_wait(barrier, len(devices))


def ln_mod(x, shift, scale):
    centered = x - jnp.mean(x, axis=-1, keepdims=True)
    var = jnp.mean(centered * centered, axis=-1, keepdims=True)
    return (centered * lax.rsqrt(var + EPS) * (1.0 + scale) + shift).astype(jnp.bfloat16)


def gelu_tanh(u):
    return u * (0.5 * (1.0 + jnp.tanh(GELU_C * (u + 0.044715 * (u * u * u)))))


def related(cfg, core, r):
    cx, cy = cfg // 2, lax.rem(cfg, 2)
    x = lax.rem(cx + lax.rem(r // 2, 2), 2)
    y = lax.rem(cy + r // 4, 2)
    return x * 2 + y, lax.rem(core + lax.rem(r, 2), 2)


def block_kernel(*refs, layer, n, n_dev, nh, n_txt, row0, with_tables, at_x, at_xx):
    h_ref, w1_ref, b1_ref, w2_ref, bias_ref, gain_ref, h_hbm, w_hbm, tab_hbm, y_hbm, H, qT_ref, k_ref, vT_ref, *refs = refs
    T = tab_hbm
    if with_tables:
        T, *refs = refs
    (y_acc, u_scr, act, wt, wbuf, bb, gg, hbuf, tbuf, w_sem, h_sem, y_sem, *refs) = refs
    i = pl.program_id(0)
    cfg, z, core = lax.axis_index('cfg'), lax.axis_index('z'), lax.axis_index('core')
    rows = y_acc.shape[0]
    total, d = h_hbm.shape
    rb = total - n_txt
    half = LANES // 2
    n_heads = d // LANES
    stride = n_heads // nh

    def device(r):
        to, c = related(cfg, core, r)
        return to, z, c

    def slot_of(r):
        to, c = related(cfg, core, r)
        return to * N_CORE + c

    own, X, Y, D = range(0, n_dev, 2)
    A, B = range(2)

    def part_of(ref, piece):
        size = ref.shape[0] // 2
        return ref.at[pl.ds(piece * size, size)]

    arrays = [(h_hbm, H)] + ([(tab_hbm, T)] if with_tables else [])
    if with_tables:
        own_sem, refs = refs[-1], refs[:-1]

    def move(origin, piece, to, send, recv, k_send, k_recv):
        out = []
        for t, (mine, every) in enumerate(arrays):
            dst = part_of(every.at[slot_of(origin)], piece)
            src = part_of(mine, piece) if origin == own else dst
            out.append(remote(src, dst, send[t].at[k_send], recv[t].at[k_recv], device(to)))
        return out

    near_send, near_recv, pair_send, pair_recv = (refs[t::4] for t in range(4))

    def near(origin, piece, to):
        order = 2 if origin else piece
        return move(origin, piece, to, near_send, near_recv, (to - X) // 2 * 3 + order, (origin ^ to) - X + piece)

    def pair(origin, piece):
        return move(origin, piece, 1, pair_send, pair_recv, origin + piece, origin + piece)

    def start(copies):
        for cp in copies:
            cp.start()

    def landed(sems, k, origin, piece):
        for t, (_, every) in enumerate(arrays):
            wait_for(part_of(every.at[slot_of(origin)], piece), sems[t].at[k])

    def landed_near(origin, piece):
        landed(near_recv, origin - X + piece, origin, piece)

    def landed_pair(origin, piece):
        landed(pair_recv, origin + piece, origin + 1, piece)

    def w_copy(j):
        p, t = j // nh, j % nh
        col = (p * n_heads + t * stride + cfg * N_CORE + core) * LANES
        return pltpu.make_async_copy(w_hbm.at[layer, :, pl.ds(pl.multiple_of(col, LANES), LANES)], wbuf.at[j % 2], w_sem.at[j % 2])

    def w_turn(j):
        p, t = j // nh, j % nh
        col = (p * n_heads + t * stride + cfg * N_CORE + core) * LANES
        w_copy(j).wait()
        wt[head_rows(j), :] = wbuf[j % 2].T
        bb[head_rows(j), :] = columns_of(bias_ref[0, :, pl.ds(pl.multiple_of(col, LANES), LANES)])

    def fetch(s, slot):
        @pl.when(s == 0)
        def _():
            pltpu.make_async_copy(h_hbm.at[pl.ds(n_txt, rb), :], hbuf.at[slot], h_sem.at[slot]).start()

        @pl.when((s > 0) & (s < n_dev))
        def _():
            pltpu.make_async_copy(H.at[slot_of(s), pl.ds(n_txt, rb), :], hbuf.at[slot], h_sem.at[slot]).start()

        @pl.when(s == n_dev)
        def _():
            pltpu.make_async_copy(h_hbm.at[pl.ds(0, n_txt), :], hbuf.at[slot, pl.ds(0, n_txt), :], h_sem.at[slot]).start()
            for r in range(1, n_dev):
                pltpu.make_async_copy(H.at[slot_of(r), pl.ds(0, n_txt), :], hbuf.at[slot, pl.ds(r * n_txt, n_txt), :], h_sem.at[slot]).start()

    def fetch_table(s, slot):
        if with_tables:
            @pl.when(s == 0)
            def _():
                pltpu.make_async_copy(tab_hbm, tbuf.at[slot], h_sem.at[2 + slot]).start()

            @pl.when((s > 0) & (s < n_dev))
            def _():
                pltpu.make_async_copy(T.at[slot_of(s)], tbuf.at[slot], h_sem.at[2 + slot]).start()
        else:
            @pl.when(s < n_dev)
            def _():
                pltpu.make_async_copy(T.at[slot_of(s)], tbuf.at[slot], h_sem.at[2 + slot]).start()

    sub = 2
    step = rows // sub

    def up():
        for r in range(sub):
            u = dot(h_ref[row0 + r * step:row0 + (r + 1) * step, :], w1_ref[0])
            u_scr[r * step:(r + 1) * step, :] = (u + b1_ref[0].astype(jnp.float32)).astype(jnp.bfloat16)

    def gelu():
        act[...] = gelu_tanh(u_scr[...].astype(jnp.float32)).astype(jnp.bfloat16)

    def down(first=False):
        for r in range(sub):
            rs = slice(r * step, (r + 1) * step)
            v = dot(act[rs, :], w2_ref[0])
            if first:
                y_acc[rs, :] = v
            else:
                y_acc[rs, :] += v

    @pl.when(i == 0)
    def _():
        w_copy(0).start()
        w_copy(1).start()
        meet([device(1), device(X), device(Y)])
        start(near(own, A, X))
        start(near(own, B, Y))
        start(pair(own, A))
        start(pair(own, B))
        start(near(own, B, X))
        start(near(own, A, Y))
        if with_tables:
            pltpu.make_async_copy(tab_hbm, T.at[slot_of(0)], own_sem).start()
        for j in range(2):
            gg[head_rows(j), :] = columns_of(gain_ref[0, j:j + 1, :])
        up()

    @pl.when(i == 1)
    def _():
        gelu()
        up()
        down(True)

    @pl.when((i > 1) & (i < n))
    def _():
        gelu()
        up()
        down()

    @pl.when(i == n)
    def _():
        gelu()
        down()

    for j in range(3 * nh):
        @pl.when(i == 1 + j)
        def _():
            w_turn(j)
            if j + 2 < 3 * nh:
                w_copy(j + 2).start()

    @pl.when(i == at_x)
    def _():
        landed_near(X, A)
        start(near(X, A, Y))
        start(pair(X, A))
        landed_near(Y, B)
        start(near(Y, B, X))
        start(pair(Y, B))
        landed_pair(own, A)
        landed_pair(own, B)

    @pl.when(i == at_xx)
    def _():
        landed_near(X, B)
        start(pair(X, B))
        landed_near(Y, A)
        start(pair(Y, A))
        landed_pair(X, A)
        landed_pair(Y, B)

    s = i - (n + 1)
    slot = lax.rem(i, 2)

    @pl.when(i == n)
    def _():
        fetch(0, 1 - slot)
        fetch_table(0, 1 - slot)

    @pl.when(s == 0)
    def _():
        pltpu.make_async_copy(y_acc, y_hbm, y_sem).start()
        landed_pair(X, B)
        landed_pair(Y, A)

    @pl.when(s == 2)
    def _():
        landed_near(D, A)
        start(pair(D, A))
        landed_near(D, B)
        start(pair(D, B))

    @pl.when(s == 5)
    def _():
        landed_pair(D, A)
        landed_pair(D, B)

    @pl.when((s >= 0) & (s < n_dev))
    def _():
        fetch(s + 1, 1 - slot)
        fetch_table(s + 1, 1 - slot)

    @pl.when(s >= 0)
    def _():
        pltpu.make_async_copy(h_hbm.at[pl.ds(0, rb), :], hbuf.at[slot], h_sem.at[slot]).wait()

        @pl.when(s < n_dev)
        def _():
            pltpu.make_async_copy(tab_hbm if with_tables else tab_hbm.at[0], tbuf.at[slot], h_sem.at[2 + slot]).wait()
        h = hbuf[slot]
        image = s < n_dev
        table = jnp.concatenate([tbuf[slot, t] for t in range(tbuf.shape[1])], axis=1)
        cos, sin = jnp.where(image, table[:half], 1.0), jnp.where(image, table[half:], 0.0)

        def lanes(v):
            return jnp.concatenate([v] * (rb // LANES), axis=1)

        def proj(part):
            rs = slice(part * nh * LANES, (part + 1) * nh * LANES)
            return lax.dot_general(wt[rs, :], h, (((1,), (1,)), ((), ())), preferred_element_type=jnp.float32)

        def biased(x, j):
            return (x + lanes(bb[head_rows(j), :])).astype(jnp.bfloat16)

        def normed(x, j, g):
            x = biased(x, j).astype(jnp.float32)
            ms = jnp.sum(x * x, axis=0, keepdims=True) * (1.0 / LANES)
            v = x * lax.rsqrt(ms + EPS) * lanes(gg[head_rows(g), :])
            a, b = v[:half], v[half:]
            return jnp.concatenate([a * cos - b * sin, a * sin + b * cos], axis=0).astype(jnp.bfloat16)

        q = proj(0)
        for t in range(nh):
            qT_ref[t] = normed(q[head_rows(t)], t, 0)
        k = proj(1)
        for t in range(nh):
            k_ref[t] = normed(k[head_rows(t)], nh + t, 1).T
        v = proj(2)
        for t in range(nh):
            vT_ref[t] = biased(v[head_rows(t)], 2 * nh + t)

    @pl.when(s == n_dev)
    def _():
        for copies in [near(own, A, X), near(own, B, X), near(own, B, Y), near(own, A, Y), near(Y, B, X), near(X, A, Y)] + [pair(o, p) for o in (own, X, Y, D) for p in (A, B)]:
            for cp in copies:
                cp.wait_send()
        pltpu.make_async_copy(y_acc, y_hbm, y_sem).wait()
        if with_tables:
            pltpu.make_async_copy(tab_hbm, T.at[slot_of(0)], own_sem).wait()


def block(h, w_in, b_in3, w_out, qk_gain, tables, layer, n_txt, nh, row0, collective_id, hc=512):
    total, d = h.shape
    n_dev = d // LANES // nh
    with_tables = tables.ndim == 3
    ff = w_in.shape[2] - 3 * d
    n = ff // hc
    m = total - row0
    rb = total - n_txt
    assert n_dev * n_txt == rb
    S = n_dev * total
    hbm = pl.BlockSpec(memory_space=pl.ANY)
    dma = pltpu.SemaphoreType.DMA
    bf, f32 = jnp.bfloat16, jnp.float32

    def at(i):
        return jnp.clip(i - (n + 1), 0, n_dev)

    t_shape = tables.shape if with_tables else tables.shape[1:]
    out_shape = [jax.ShapeDtypeStruct((m, d), f32), jax.ShapeDtypeStruct((n_dev, total, d), bf),
                 jax.ShapeDtypeStruct((nh, LANES, S), bf), jax.ShapeDtypeStruct((nh, S, LANES), bf), jax.ShapeDtypeStruct((nh, LANES, S), bf)]
    out_specs = [hbm, hbm, pl.BlockSpec((nh, LANES, rb), lambda i: (0, 0, at(i))), pl.BlockSpec((nh, rb, LANES), lambda i: (0, at(i), 0)),
                 pl.BlockSpec((nh, LANES, rb), lambda i: (0, 0, at(i)))]
    sems = [dma((2,)), dma((4,)), dma, dma((6,)), dma((6,)), dma((8,)), dma((8,))]
    if with_tables:
        out_shape.append(jax.ShapeDtypeStruct((n_dev, *tables.shape), f32))
        out_specs.append(hbm)
        sems += [dma((6,)), dma((6,)), dma((8,)), dma((8,)), dma]
    return pl.pallas_call(
        functools.partial(block_kernel, layer=layer, n=n, n_dev=n_dev, nh=nh, n_txt=n_txt, row0=row0, with_tables=with_tables, at_x=n * 5 // 12, at_xx=n * 5 // 6),
        grid=(n + 1 + n_dev + 1,),
        in_specs=[
            whole((total, d), pipeline_mode=pl.Buffered(1)),
            pl.BlockSpec((1, d, hc), lambda i: (layer, 0, 3 * d // hc + jnp.minimum(i, n - 1))),
            pl.BlockSpec((1, 1, hc), lambda i: (layer, 0, 3 * d // hc + jnp.minimum(i, n - 1))),
            pl.BlockSpec((1, hc, d), lambda i: (layer, d // hc + jnp.clip(i - 1, 0, n - 1), 0)),
            pl.BlockSpec((1, 1, b_in3.shape[2]), lambda i: (layer, 0, 0)),
            pl.BlockSpec((1, 2, LANES), lambda i: (layer, 0, 0)),
            hbm, hbm, hbm,
        ],
        out_specs=out_specs,
        out_shape=out_shape,
        scratch_shapes=[
            pltpu.VMEM((m, d), f32), pltpu.VMEM((m, hc), bf), pltpu.VMEM((m, hc), bf), pltpu.VMEM((3 * nh * LANES, d), bf), pltpu.VMEM((2, d, LANES), bf),
            pltpu.VMEM((3 * nh * LANES, LANES), f32), pltpu.VMEM((2 * LANES, LANES), f32), pltpu.VMEM((2, rb, d), bf), pltpu.VMEM((2, *t_shape), f32),
        ] + sems,
        compiler_params=params(**talking(collective_id)),
        cost_estimate=pl.CostEstimate(flops=4 * m * d * ff + 6 * S * d * nh * LANES, bytes_accessed=4 * d * ff + 2 * S * d, transcendentals=m * ff),
        name='block',
    )(h, w_in, b_in3, w_out, b_in3, qk_gain, h, w_in, tables)


def attn_kernel(qT_hbm, k_hbm, vT_hbm, *refs, qt, kc, n_dev, n_img, n_txt, with_txt):
    if with_txt:
        oi_hbm, ot_hbm, qT_ref, k_ref, vT_ref, s_scr, m_scr, obuf, tbuf, in_sem, send_sem, recv_sem, own_sem, tsend_sem, trecv_sem, town_sem = refs
    else:
        oi_hbm, qT_ref, k_ref, vT_ref, s_scr, m_scr, obuf, in_sem, send_sem, recv_sem, own_sem = refs
    nh, S, hd = k_ref.shape
    nk = S // kc
    c = hd ** -0.5 * LOG2E
    per = n_img // qt
    assert per == 2

    def load(t):
        pairs = ((qT_hbm, qT_ref), (k_hbm, k_ref), (vT_hbm, vT_ref))
        return [pltpu.make_async_copy(src.at[t], dst.at[t], in_sem.at[t, j]) for j, (src, dst) in enumerate(pairs)]

    for t in range(nh):
        for cp in load(t):
            cp.start()
    me = lax.axis_index('cfg') * N_CORE + lax.axis_index('core')
    z = lax.axis_index('z')

    def device(r):
        to, c = related(lax.axis_index('cfg'), lax.axis_index('core'), r)
        return to, z, c

    meet([device(r) for r in range(1, n_dev)])
    for cp in load(0):
        cp.wait()

    def score_chunk(head, q, slot, i, m):
        s = dot(k_ref[head, pl.ds(i * kc, kc), :], q)
        s_scr[slot, pl.ds(i * kc, kc), :] = s
        return jnp.maximum(m, jnp.max(s.reshape(kc // 8, 8, qt), axis=0))

    def finish_max(m, slot):
        m_scr[slot] = jnp.broadcast_to(jnp.max(m, axis=0, keepdims=True) * c, (8, qt))

    def prob_chunk(head, mc, slot, i, l, acc):
        s = s_scr[slot, pl.ds(i * kc, kc), :].reshape(kc // 8, 8, qt)
        p = jnp.exp2(s * c - mc[None])
        l = l + jnp.sum(p, axis=0)
        d = dot(vT_ref[head, :, pl.ds(i * kc, kc)], p.reshape(kc, qt).astype(jnp.bfloat16))
        return l, acc + d

    def load_q(tile):
        head, col = tile
        return qT_ref[head, :, pl.ds(pl.multiple_of(col, qt), qt)]

    def start(tile):
        head, _ = tile
        q = load_q(tile)
        m = jnp.full((8, qt), -jnp.inf, jnp.float32)
        for i in range(nk):
            m = score_chunk(head, q, 0, i, m)
        finish_max(m, 0)

    def both(tile, following, slot):
        head, nhead = tile[0], following[0]
        q = load_q(following)
        m = jnp.full((8, qt), -jnp.inf, jnp.float32)
        l = jnp.zeros((8, qt), jnp.float32)
        acc = jnp.zeros((hd, qt), jnp.float32)
        mc = m_scr[slot]
        for i in range(nk):
            m = score_chunk(nhead, q, 1 - slot, i, m)
            l, acc = prob_chunk(head, mc, slot, i, l, acc)
        finish_max(m, 1 - slot)
        return (acc / jnp.sum(l, axis=0, keepdims=True)).T.astype(jnp.bfloat16)

    n_pairs = nh * n_dev

    def relation_of(p):
        return lax.rem(p + 1, n_dev)

    def img_tile(p, part):
        return p // n_dev, relation_of(p) * n_img + part * qt

    def send(p):
        head, owner = p // n_dev, relation_of(p)

        @pl.when(lax.rem(p, n_dev) == n_dev - 1)
        def _():
            pltpu.make_async_copy(obuf.at[p], oi_hbm.at[me, head], own_sem).start()

        @pl.when(lax.rem(p, n_dev) < n_dev - 1)
        def _():
            remote(obuf.at[p], oi_hbm.at[me, head], send_sem, recv_sem, device(owner)).start()

    start(img_tile(0, 0))

    def pair(p, carry):
        @pl.when(p > 0)
        def _():
            send(p - 1)

        @pl.when((lax.rem(p, n_dev) == n_dev - 1) & (p < n_pairs - 1))
        def _():
            for cp in load(p // n_dev + 1):
                cp.wait()

        obuf[p, 0:qt, :] = both(img_tile(p, 0), img_tile(p, 1), 0)
        obuf[p, qt:2 * qt, :] = both(img_tile(p, 1), img_tile(lax.rem(p + 1, n_pairs), 0), 1)
        return carry

    lax.fori_loop(0, n_pairs, pair, 0)
    send(n_pairs - 1)

    if with_txt:
        n_text = n_dev * n_txt
        tiles = n_text // qt
        first = n_dev * n_img

        def txt_tile(u):
            return u // tiles, first + lax.rem(u, tiles) * qt

        def txt_send(u):
            head = u // tiles
            for a in range(qt // n_txt):
                owner = lax.rem(u, tiles) * (qt // n_txt) + a
                src = tbuf.at[u, pl.ds(a * n_txt, n_txt), :]

                @pl.when(owner == 0)
                def _():
                    pltpu.make_async_copy(src, ot_hbm.at[me, head], town_sem).start()

                @pl.when(owner != 0)
                def _():
                    remote(src, ot_hbm.at[me, head], tsend_sem, trecv_sem, device(owner)).start()

        start(txt_tile(0))

        n_tt = nh * tiles
        if n_tt % 2 == 0:
            def txt_pair(p, carry):
                u = 2 * p
                tbuf[u] = both(txt_tile(u), txt_tile(u + 1), 0)
                tbuf[u + 1] = both(txt_tile(u + 1), txt_tile(lax.rem(u + 2, n_tt)), 1)
                txt_send(u)
                txt_send(u + 1)
                return carry
            lax.fori_loop(0, n_tt // 2, txt_pair, 0)
        else:
            for u in range(n_tt):
                tbuf[u] = both(txt_tile(u), txt_tile((u + 1) % n_tt), u % 2)
                txt_send(u)

    others = pl.ds(0, n_dev - 1)
    wait_for(oi_hbm.at[others], send_sem)
    wait_for(oi_hbm.at[others], recv_sem)
    wait_for(oi_hbm.at[me], own_sem)
    if with_txt:
        wait_for(ot_hbm.at[others], tsend_sem)
        wait_for(ot_hbm.at[others], trecv_sem)
        wait_for(ot_hbm.at[me], town_sem)


def largest(n, cap, unit):
    return max(c for c in range(unit, cap + 1, unit) if n % c == 0)


def attention(qT, k, vT, n_dev, n_txt, with_txt, collective_id):
    nh, S, hd = k.shape
    n_img = S // n_dev - n_txt
    qt = n_img // 2
    kc = largest(S, 768, 256)
    SQ = n_dev * (n_img + (n_txt if with_txt else 0))
    dma = pltpu.SemaphoreType.DMA
    out_shape = [jax.ShapeDtypeStruct((n_dev, nh, n_img, hd), jnp.bfloat16)]
    scratch = [pltpu.VMEM((nh, hd, S), jnp.bfloat16), pltpu.VMEM((nh, S, hd), jnp.bfloat16), pltpu.VMEM((nh, hd, S), jnp.bfloat16),
               pltpu.VMEM((2, S, qt), jnp.float32), pltpu.VMEM((2, 8, qt), jnp.float32), pltpu.VMEM((nh * n_dev, n_img, hd), jnp.bfloat16)]
    sems = [dma((nh, 3)), dma, dma, dma]
    if with_txt:
        out_shape.append(jax.ShapeDtypeStruct((n_dev, nh, n_txt, hd), jnp.bfloat16))
        scratch.append(pltpu.VMEM((nh * n_dev * n_txt // qt, qt, hd), jnp.bfloat16))
        sems += [dma, dma, dma]
    return pl.pallas_call(
        functools.partial(attn_kernel, qt=qt, kc=kc, n_dev=n_dev, n_img=n_img, n_txt=n_txt, with_txt=with_txt),
        in_specs=[pl.BlockSpec(memory_space=pl.ANY)] * 3,
        out_specs=[pl.BlockSpec(memory_space=pl.ANY)] * len(out_shape),
        out_shape=out_shape,
        scratch_shapes=scratch + sems,
        compiler_params=pltpu.CompilerParams(vmem_limit_bytes=VMEM_BYTES, **talking(collective_id)),
        cost_estimate=pl.CostEstimate(flops=6 * nh * SQ * S * hd, bytes_accessed=8 * nh * S * hd, transcendentals=nh * S * SQ),
        name='attn',
    )(qT, k, vT)


def out_kernel(*refs, nc, ne, n_txt, row0, last, gate_row):
    if last:
        oi_ref, w_ref, bo_ref, mods_ref, wf_ref, bf_ref, x_hbm, y_hbm, vel_hbm, lhs, acc, ybuf, xbuf, hs, vel, sems, own_sem, send_sem, recv_sem = refs
    else:
        oi_ref, ot_ref, w_ref, bo_ref, mods_ref, x_hbm, y_hbm, xo_ref, ho_ref, lhs, acc, ybuf, xbuf, sems = refs
    i = pl.program_id(0)
    R = acc.shape[0]
    er = R // ne
    copy_y = pltpu.make_async_copy(y_hbm, ybuf, sems.at[0])
    copy_x = pltpu.make_async_copy(x_hbm.at[pl.ds(row0, R), :], xbuf, sems.at[1])

    @pl.when(i == 0)
    def _():
        copy_y.start()
        copy_x.start()

    if last:
        cfg, z, core = lax.axis_index('cfg'), lax.axis_index('z'), lax.axis_index('core')

        @pl.when(i == 0)
        def _():
            meet([(z, e, core) for e in range(ne)] + [(e, cfg, core) for e in range(ne)])

    @pl.when(i < nc)
    def _():
        for t in range(oi_ref.shape[0]):
            cols = head_rows(t)
            if last:
                lhs[:, cols] = oi_ref[t, 0]
            else:
                lhs[:n_txt, cols] = ot_ref[t, 0]
                lhs[n_txt:, cols] = oi_ref[t, 0]

    @pl.when(i == 0)
    def _():
        acc[...] = dot(lhs[...], w_ref[0])

    @pl.when((i > 0) & (i < nc))
    def _():
        acc[...] += dot(lhs[...], w_ref[0])

    @pl.when(i == nc)
    def _():
        copy_y.wait()
        copy_x.wait()

    @pl.when(i >= nc)
    def _():
        gate, shift, scale = (mods_ref[r:r + 1, :] for r in range(gate_row, gate_row + 3))
        bo = bo_ref[0].astype(jnp.float32)
        sub = 16 if er % 16 == 0 else 8

        def chunk(c, carry):
            rs = pl.ds(pl.multiple_of((i - nc) * er + c * sub, sub), sub)
            ls = pl.ds(pl.multiple_of(c * sub, sub), sub)
            y = acc[rs, :] + ybuf[rs, :] + bo
            xn = (xbuf[rs, :].astype(jnp.float32) + gate * y).astype(jnp.bfloat16)
            h = ln_mod(xn.astype(jnp.float32), shift, scale)
            if last:
                hs[ls, :] = h
            else:
                xo_ref[ls, :] = xn
                ho_ref[ls, :] = h
            return carry

        lax.fori_loop(0, er // sub, chunk, 0, unroll=3 if (er // sub) % 3 == 0 else 2)

    if last:
        def deliver(e):
            @pl.when((z == cfg) & (e == z))
            def _():
                pltpu.make_async_copy(vel.at[e], vel_hbm.at[cfg], own_sem).start()

            @pl.when((z != cfg) | (e != z))
            def _():
                remote(vel.at[e], vel_hbm.at[cfg], send_sem.at[e], recv_sem.at[cfg], (z, e, core)).start()

        @pl.when(i >= nc)
        def _():
            vel[i - nc] = dot(hs[...], wf_ref[...]) + bf_ref[...].astype(jnp.float32)
            deliver(i - nc)

        @pl.when(i == nc + ne - 1)
        def _():
            for e in range(ne):
                @pl.when((z == cfg) & (e == z))
                def _():
                    pltpu.make_async_copy(vel.at[e], vel_hbm.at[e], own_sem).wait()

                @pl.when((z != cfg) | (e != z))
                def _():
                    remote(vel.at[e], vel_hbm.at[e], send_sem.at[e], recv_sem.at[e], (z, e, core)).wait_send()
                    remote(vel.at[e], vel_hbm.at[e], send_sem.at[e], recv_sem.at[e], (z, e, core)).wait_recv()


def out_proj(os, w_out, b_out3, mods, x, y_mlp, layer, row0, final=None, collective_id=None, kc=512):
    oi = os[0]
    _, nh, n_img, _ = oi.shape
    R = sum(o.shape[2] for o in os)
    ne = 4
    d = w_out.shape[2]
    nc = d // kc
    per = nc // nh
    hp = kc // LANES
    last = final is not None

    def o_map(i):
        j = jnp.minimum(i, nc - 1)
        return lax.rem(j, per), j // per, 0, 0

    in_specs = [pl.BlockSpec((hp, 1, o.shape[2], LANES), o_map) for o in os] + [
        pl.BlockSpec((1, kc, d), lambda i: (layer, jnp.minimum(i, nc - 1), 0)),
        pl.BlockSpec((1, 1, d), lambda i: (layer, 0, 0)),
        whole(mods.shape),
    ]
    args = [*os, w_out, b_out3, mods]
    scratch = [pltpu.VMEM((R, kc), jnp.bfloat16), pltpu.VMEM((R, d), jnp.float32), pltpu.VMEM((R, d), jnp.float32), pltpu.VMEM((R, d), jnp.bfloat16)]
    sems = [pltpu.SemaphoreType.DMA((2,))]
    if last:
        n_out = final[0].shape[1]
        in_specs += [whole(v.shape) for v in final]
        args += list(final)
        out_specs = pl.BlockSpec(memory_space=pl.ANY)
        out_shape = jax.ShapeDtypeStruct((ne, R // ne, n_out), jnp.float32)
        scratch += [pltpu.VMEM((R // ne, d), jnp.bfloat16), pltpu.VMEM((ne, R // ne, n_out), jnp.float32)]
        sems += [pltpu.SemaphoreType.DMA, pltpu.SemaphoreType.DMA((ne,)), pltpu.SemaphoreType.DMA((ne,))]
        compiler_params = params(**talking(collective_id))
    else:
        out_specs = [pl.BlockSpec((R // ne, d), lambda i: (jnp.maximum(i - nc, 0), 0))] * 2
        out_shape = [jax.ShapeDtypeStruct((R, d), jnp.bfloat16)] * 2
        compiler_params = params()
    return pl.pallas_call(
        functools.partial(out_kernel, nc=nc, ne=ne, n_txt=R - n_img, row0=row0, last=last, gate_row=3 * layer + 2),
        grid=(nc + ne,),
        in_specs=in_specs + [pl.BlockSpec(memory_space=pl.ANY)] * 2,
        out_specs=out_specs,
        out_shape=out_shape,
        scratch_shapes=scratch + sems,
        compiler_params=compiler_params,
        cost_estimate=pl.CostEstimate(flops=2 * R * d * d, bytes_accessed=2 * d * d + 14 * R * d, transcendentals=0),
        name='outp',
    )(*args, x, y_mlp)


def enter_kernel(xt_hbm, xi_hbm, cond_ref, wm_ref, wf_ref, bias_ref, tab_hbm, mods_ref, xo_ref, ho_ref, tab_out,
                 stage, xbuf, cond_buf, s_scr,
                 cond_send, cond_recv, p_send, p_recv, c_send, c_recv, own_sem, t_send, t_recv, town_sem, *, n_mod, n_steps, per_row):
    i = pl.program_id(0)
    n, rows, d = xbuf.shape
    tp = xt_hbm.shape[0] // n
    ip = xi_hbm.shape[0] // n
    cfg, z, core = lax.axis_index('cfg'), lax.axis_index('z'), lax.axis_index('core')
    cx, cy = cfg // 2, lax.rem(cfg, 2)
    across = [(1 - cx) * 2 + cy, cx * 2 + (1 - cy), (1 - cx) * 2 + (1 - cy)]
    heights = [lax.rem(z + s, n) for s in range(1, n)]

    def piece_refs(j, dst):
        return [(xt_hbm.at[pl.ds(j * tp, tp), :], dst.at[pl.ds(0, tp), :]), (xi_hbm.at[pl.ds(j * ip, ip), :], dst.at[pl.ds(tp, ip), :])]

    def forward(group, t):
        @pl.when(group == z)
        def _():
            xbuf[z] = stage[group]

        @pl.when(group != z)
        def _():
            remote(stage.at[group], xbuf.at[z], c_send.at[t], c_recv.at[z], (cfg, group, core)).start()

    @pl.when(i == 0)
    def _():
        meet([(j, z, core) for j in across] + [(cfg, h, core) for h in heights])

        @pl.when(cfg == z)
        def _():
            for t, j in enumerate(across):
                remote(cond_ref, cond_buf, cond_send.at[t], cond_recv, (j, z, core)).start()
        for t, j in enumerate(across):
            for src, dst in piece_refs(j, stage.at[cfg]):
                remote(src, dst, p_send.at[t], p_recv.at[cfg], (j, z, core)).start()

        @pl.when(cfg == z)
        def _():
            for src, dst in piece_refs(cfg, xbuf.at[z]):
                pltpu.make_async_copy(src, dst, own_sem).start()

        @pl.when(cfg != z)
        def _():
            for src, dst in piece_refs(cfg, xbuf.at[z]):
                remote(src, dst, c_send.at[n - 1], c_recv.at[z], (cfg, cfg, core)).start()
        for t, h in enumerate(heights):
            remote(tab_hbm.at[cfg], tab_out.at[z], t_send.at[t], t_recv.at[z], (cfg, h, core)).start()
        pltpu.make_async_copy(tab_hbm.at[cfg], tab_out.at[z], town_sem).start()

        @pl.when(cfg == z)
        def _():
            v = cond_ref[...].astype(jnp.float32)
            s_scr[...] = (v * jax.nn.sigmoid(v)).astype(jnp.bfloat16)

        @pl.when(cfg != z)
        def _():
            remote(cond_ref, cond_buf, cond_send.at[0], cond_recv, (cfg, z, core)).wait_recv()
            v = cond_buf[...].astype(jnp.float32)
            s_scr[...] = (v * jax.nn.sigmoid(v)).astype(jnp.bfloat16)

    row, col = i // per_row, lax.rem(i, per_row)
    width = wm_ref.shape[2]
    cols = pl.ds(pl.multiple_of(col * width, width), width)

    @pl.when(i < n_mod)
    def _():
        v = dot(s_scr[...], wm_ref[0])
        mods_ref[pl.ds(row, 1), cols] = v[0:1]

    @pl.when(i >= n_mod)
    def _():
        v = dot(s_scr[...], wf_ref[...])
        mods_ref[pl.ds(row, 1), cols] = v[0:1]

    def arrived(t):
        j = across[t]
        remote(stage.at[j], stage.at[j], p_send.at[t], p_recv.at[j], (j, z, core)).wait_recv()
        forward(j, t)

    @pl.when(i == n_steps * 3 // 8)
    def _():
        arrived(0)
        arrived(1)

    @pl.when(i == n_steps * 3 // 4)
    def _():
        arrived(2)

    @pl.when(i == n_steps - 1)
    def _():
        mods_ref[...] += bias_ref[...].astype(jnp.float32)
        shift, scale = mods_ref[0:1, :], mods_ref[1:2, :]

        @pl.when(cfg == z)
        def _():
            wait_for(xbuf.at[z], own_sem)

        def norm_rows(k, src, dst, count):
            sub = 16 if count % 16 == 0 else 8

            def chunk(c, carry):
                v = xbuf[k, pl.ds(pl.multiple_of(src + c * sub, sub), sub), :]
                to = pl.ds(pl.multiple_of(dst + c * sub, sub), sub)
                xo_ref[to, :] = v
                ho_ref[to, :] = ln_mod(v.astype(jnp.float32), shift, scale)
                return carry
            lax.fori_loop(0, count // sub, chunk, 0, unroll=min(4, count // sub))

        for s in range(n):
            k = lax.rem(z + s, n)
            if s:
                remote(xbuf.at[k], xbuf.at[k], c_send.at[0], c_recv.at[k], (cfg, k, core)).wait_recv()
            norm_rows(k, 0, k * tp, tp)
            norm_rows(k, tp, n * tp + k * ip, ip)

        for t, j in enumerate(across):
            remote(xbuf.at[0], xbuf.at[0], p_send.at[t], p_recv.at[j], (j, z, core)).wait_send()

            @pl.when(j != z)
            def _():
                remote(xbuf.at[0], xbuf.at[0], c_send.at[t], c_recv.at[j], (cfg, j, core)).wait_send()

        @pl.when(cfg != z)
        def _():
            remote(xbuf.at[0], xbuf.at[0], c_send.at[n - 1], c_recv.at[0], (cfg, cfg, core)).wait_send()

        @pl.when(cfg == z)
        def _():
            for t, j in enumerate(across):
                remote(cond_ref, cond_buf, cond_send.at[t], cond_recv, (j, z, core)).wait_send()
        for t, h in enumerate(heights):
            remote(tab_hbm.at[cfg], tab_out.at[z], t_send.at[t], t_recv.at[z], (cfg, h, core)).wait_send()
            remote(tab_hbm.at[cfg], tab_out.at[h], t_send.at[t], t_recv.at[h], (cfg, h, core)).wait_recv()
        pltpu.make_async_copy(tab_hbm.at[cfg], tab_out.at[z], town_sem).wait()


def enter(x_txt, x_img, cond, w_mod, w_fmod, bias, tables, collective_id, width=512):
    n_txt, d = x_txt.shape
    n_img = x_img.shape[0]
    n = tables.shape[0]
    rows = (n_txt + n_img) // n
    n_layers, _, dm = w_mod.shape
    per_layer, n_fin, per_row = dm // width, w_fmod.shape[1] // width, d // width
    n_mod = n_layers * per_layer
    steps = n_mod + n_fin
    dma = pltpu.SemaphoreType.DMA
    bf = jnp.bfloat16

    def wm_map(i):
        j = jnp.minimum(i, n_mod - 1)
        return j // per_layer, 0, lax.rem(j, per_layer)

    hbm = pl.BlockSpec(memory_space=pl.ANY)
    return pl.pallas_call(
        functools.partial(enter_kernel, n_mod=n_mod, n_steps=steps, per_row=per_row),
        grid=(steps,),
        in_specs=[hbm, hbm, whole(cond.shape), pl.BlockSpec((1, d, width), wm_map), pl.BlockSpec((d, width), lambda i: (0, jnp.maximum(i - n_mod, 0))), whole(bias.shape), hbm],
        out_specs=[whole(bias.shape), whole((n_txt + n_img, d)), whole((n_txt + n_img, d)), hbm],
        out_shape=[jax.ShapeDtypeStruct(bias.shape, jnp.float32), jax.ShapeDtypeStruct((n_txt + n_img, d), bf), jax.ShapeDtypeStruct((n_txt + n_img, d), bf), jax.ShapeDtypeStruct(tables.shape, jnp.float32)],
        scratch_shapes=[pltpu.VMEM((n, rows, d), bf), pltpu.VMEM((n, rows, d), bf), pltpu.VMEM(cond.shape, bf), pltpu.VMEM(cond.shape, bf),
                        dma((n - 1,)), dma, dma((n - 1,)), dma((n,)), dma((n,)), dma((n,)), dma, dma((n - 1,)), dma((n,)), dma],
        compiler_params=params(**talking(collective_id)),
        cost_estimate=pl.CostEstimate(flops=2 * 16 * d * width * steps, bytes_accessed=2 * d * width * steps, transcendentals=0),
        name='enter',
    )(x_txt, x_img, cond, w_mod, w_fmod, bias, tables)


def solution(mesh):
    n_cfg = mesh.devices.shape[0]
    n_z = mesh.devices.shape[1] // N_CORE
    grid = Mesh(mesh.devices.reshape(n_cfg, n_z, N_CORE), ('cfg', 'z', 'core'))
    assert n_cfg == n_z == 4
    n_dev = n_cfg * N_CORE
    token_spec = P(('cfg', 'z', 'core'), None)
    seq_spec = P(('z', 'core'), None)
    in_specs = (token_spec, token_spec, P('cfg', None), seq_spec, seq_spec, token_spec) + (P(),) * 13

    def body(x_txt, x_img, cond_vec, cos_img, sin_img, z_lat, t_cur, t_next, w_mod, b_mod, w_in, b_in, qk_gain, w_out, b_out, w_fmod, b_fmod, w_final, b_final):
        n_txt, d = x_txt.shape
        n_img = x_img.shape[0]
        n_layers = w_mod.shape[0]
        nh = d // LANES // n_dev
        ip = n_img // n_cfg
        n_out = w_final.shape[1]

        tables = jnp.concatenate([cos_img.T, sin_img.T], axis=0).reshape(LANES, n_cfg, ip).transpose(1, 0, 2)
        bias = jnp.concatenate([b_mod.reshape(-1, d), b_fmod.reshape(-1, d)], axis=0)
        cond = jnp.broadcast_to(cond_vec, (16, d))
        mods, x, h, own = enter(x_txt, x_img, cond, w_mod, w_fmod, bias, tables, 1)

        b_in3, b_out3 = b_in[:, None, :], b_out[:, None, :]
        for l in range(n_layers):
            last = l == n_layers - 1
            row0 = n_txt if last else 0
            y_mlp, _, qT, k, vT, *more = block(h, w_in, b_in3, w_out, qk_gain, own, l, n_txt, nh, row0, 2 + 2 * l)
            own = more[0] if more else own
            os = attention(qT, k, vT, n_dev, n_txt, not last, 3 + 2 * l)
            if last:
                wide = [jnp.pad(v, ((0, 0), (0, LANES - n_out))) for v in (w_final, b_final[None])]
                vel = out_proj(os, w_out, b_out3, mods, x, y_mlp, l, row0, final=wide, collective_id=2 + 2 * n_layers)
            else:
                x, h = out_proj(os, w_out, b_out3, mods, x, y_mlp, l, row0)

        return z_lat + (t_next - t_cur) * vel.reshape(n_img, LANES)[:, :n_out]

    return jax.shard_map(body, mesh=grid, in_specs=in_specs, out_specs=token_spec, check_vma=False)
```

```python
import functools
import math

import jax
import jax.numpy as jnp
from jax import lax
from jax.experimental import pallas as pl
from jax.experimental.pallas import tpu as pltpu
from jax.sharding import Mesh, PartitionSpec as P

EPS = 1e-6
LANES = 128
GELU_C = math.sqrt(2.0 / math.pi)
LOG2E = math.log2(math.e)
VMEM_BYTES = 60 * 2**20
N_CORE = 2
MESH = pl.DeviceIdType.MESH


def params(**kw):
    return pltpu.CompilerParams(vmem_limit_bytes=VMEM_BYTES, dimension_semantics=('arbitrary',), **kw)


def talking(collective_id):
    return dict(collective_id=collective_id, has_side_effects=True)


def whole(shape, **kw):
    return pl.BlockSpec(shape, lambda i: (0,) * len(shape), **kw)


def head_rows(j):
    return slice(j * LANES, (j + 1) * LANES)


def columns_of(v):
    return jnp.broadcast_to(v.astype(jnp.float32), (LANES, LANES)).T


def wait_for(ref, sem):
    pltpu.make_async_copy(ref, ref, sem).wait()


def dot(a, b):
    return jnp.dot(a, b, preferred_element_type=jnp.float32)


def remote(src, dst, send_sem, recv_sem, device):
    return pltpu.make_async_remote_copy(src_ref=src, dst_ref=dst, send_sem=send_sem, recv_sem=recv_sem, device_id=device, device_id_type=MESH)


def meet(devices):
    barrier = pltpu.get_barrier_semaphore()
    for device in devices:
        pl.semaphore_signal(barrier, inc=1, device_id=device, device_id_type=MESH)
    pl.semaphore_wait(barrier, len(devices))


def ln_mod(x, shift, scale):
    centered = x - jnp.mean(x, axis=-1, keepdims=True)
    var = jnp.mean(centered * centered, axis=-1, keepdims=True)
    return (centered * lax.rsqrt(var + EPS) * (1.0 + scale) + shift).astype(jnp.bfloat16)


def gelu_tanh(u):
    return u * (0.5 * (1.0 + jnp.tanh(GELU_C * (u + 0.044715 * (u * u * u)))))


def related(cfg, core, r):
    cx, cy = cfg // 2, lax.rem(cfg, 2)
    x = lax.rem(cx + lax.rem(r // 2, 2), 2)
    y = lax.rem(cy + r // 4, 2)
    return x * 2 + y, lax.rem(core + lax.rem(r, 2), 2)


def block_kernel(*refs, layer, n, n_dev, nh, n_txt, row0, with_tables, at_x, at_xx):
    h_ref, w1_ref, b1_ref, w2_ref, bias_ref, gain_ref, h_hbm, w_hbm, tab_hbm, y_hbm, H, qT_ref, k_ref, vT_ref, *refs = refs
    T = tab_hbm
    if with_tables:
        T, *refs = refs
    (y_acc, u_scr, act, wt, wbuf, bb, gg, hbuf, tbuf, w_sem, h_sem, y_sem, *refs) = refs
    i = pl.program_id(0)
    cfg, z, core = lax.axis_index('cfg'), lax.axis_index('z'), lax.axis_index('core')
    rows = y_acc.shape[0]
    total, d = h_hbm.shape
    rb = total - n_txt
    half = LANES // 2
    n_heads = d // LANES
    stride = n_heads // nh

    def device(r):
        to, c = related(cfg, core, r)
        return to, z, c

    def slot_of(r):
        to, c = related(cfg, core, r)
        return to * N_CORE + c

    own, X, Y, D = range(0, n_dev, 2)
    A, B = range(2)

    def part_of(ref, piece):
        size = ref.shape[0] // 2
        return ref.at[pl.ds(piece * size, size)]

    arrays = [(h_hbm, H)] + ([(tab_hbm, T)] if with_tables else [])
    if with_tables:
        own_sem, refs = refs[-1], refs[:-1]

    def move(origin, piece, to, send, recv, k_send, k_recv):
        out = []
        for t, (mine, every) in enumerate(arrays):
            dst = part_of(every.at[slot_of(origin)], piece)
            src = part_of(mine, piece) if origin == own else dst
            out.append(remote(src, dst, send[t].at[k_send], recv[t].at[k_recv], device(to)))
        return out

    near_send, near_recv, pair_send, pair_recv = (refs[t::4] for t in range(4))

    def near(origin, piece, to):
        order = 2 if origin else piece
        return move(origin, piece, to, near_send, near_recv, (to - X) // 2 * 3 + order, (origin ^ to) - X + piece)

    def pair(origin, piece):
        return move(origin, piece, 1, pair_send, pair_recv, origin + piece, origin + piece)

    def start(copies):
        for cp in copies:
            cp.start()

    def landed(sems, k, origin, piece):
        for t, (_, every) in enumerate(arrays):
            wait_for(part_of(every.at[slot_of(origin)], piece), sems[t].at[k])

    def landed_near(origin, piece):
        landed(near_recv, origin - X + piece, origin, piece)

    def landed_pair(origin, piece):
        landed(pair_recv, origin + piece, origin + 1, piece)

    def w_cols(j):
        col = (j // nh * n_heads + lax.rem(j, nh) * stride + cfg * N_CORE + core) * LANES
        return pl.ds(pl.multiple_of(col, LANES), LANES)

    def w_copy(j):
        return pltpu.make_async_copy(w_hbm.at[layer, :, w_cols(j)], wbuf.at[lax.rem(j, 2)], w_sem.at[lax.rem(j, 2)])

    def w_turn(j):
        w_copy(j).wait()
        to = pl.ds(pl.multiple_of(j * LANES, LANES), LANES)
        wt[to, :] = wbuf[lax.rem(j, 2)].T
        bb[to, :] = columns_of(bias_ref[0, :, w_cols(j)])

    def fetch(s, slot):
        @pl.when(s == 0)
        def _():
            pltpu.make_async_copy(h_hbm.at[pl.ds(n_txt, rb), :], hbuf.at[slot], h_sem.at[slot]).start()

        @pl.when((s > 0) & (s < n_dev))
        def _():
            pltpu.make_async_copy(H.at[slot_of(s), pl.ds(n_txt, rb), :], hbuf.at[slot], h_sem.at[slot]).start()

        @pl.when(s == n_dev)
        def _():
            pltpu.make_async_copy(h_hbm.at[pl.ds(0, n_txt), :], hbuf.at[slot, pl.ds(0, n_txt), :], h_sem.at[slot]).start()
            for r in range(1, n_dev):
                pltpu.make_async_copy(H.at[slot_of(r), pl.ds(0, n_txt), :], hbuf.at[slot, pl.ds(r * n_txt, n_txt), :], h_sem.at[slot]).start()

    def fetch_table(s, slot):
        if with_tables:
            @pl.when(s == 0)
            def _():
                pltpu.make_async_copy(tab_hbm, tbuf.at[slot], h_sem.at[2 + slot]).start()

            @pl.when((s > 0) & (s < n_dev))
            def _():
                pltpu.make_async_copy(T.at[slot_of(s)], tbuf.at[slot], h_sem.at[2 + slot]).start()
        else:
            @pl.when(s < n_dev)
            def _():
                pltpu.make_async_copy(T.at[slot_of(s)], tbuf.at[slot], h_sem.at[2 + slot]).start()

    sub = 2
    step = rows // sub

    def up():
        for r in range(sub):
            u = dot(h_ref[row0 + r * step:row0 + (r + 1) * step, :], w1_ref[0])
            u_scr[r * step:(r + 1) * step, :] = (u + b1_ref[0].astype(jnp.float32)).astype(jnp.bfloat16)

    def gelu():
        act[...] = gelu_tanh(u_scr[...].astype(jnp.float32)).astype(jnp.bfloat16)

    def down():
        for r in range(sub):
            rs = slice(r * step, (r + 1) * step)
            y_acc[rs, :] += dot(act[rs, :], w2_ref[0])

    @pl.when(i == 0)
    def _():
        w_copy(0).start()
        w_copy(1).start()
        meet([device(1), device(X), device(Y)])
        start(near(own, A, X))
        start(near(own, B, Y))
        start(pair(own, A))
        start(pair(own, B))
        start(near(own, B, X))
        start(near(own, A, Y))
        if with_tables:
            pltpu.make_async_copy(tab_hbm, T.at[slot_of(0)], own_sem).start()
        for j in range(2):
            gg[head_rows(j), :] = columns_of(gain_ref[0, j:j + 1, :])
        y_acc[...] = jnp.zeros_like(y_acc)
        up()

    @pl.when((i > 0) & (i < n))
    def _():
        gelu()
        up()
        down()

    @pl.when(i == n)
    def _():
        gelu()
        down()

    @pl.when((i > 0) & (i <= 3 * nh))
    def _():
        w_turn(i - 1)

        @pl.when(i + 1 < 3 * nh)
        def _():
            w_copy(i + 1).start()

    @pl.when(i == at_x)
    def _():
        landed_near(X, A)
        start(near(X, A, Y))
        start(pair(X, A))
        landed_near(Y, B)
        start(near(Y, B, X))
        start(pair(Y, B))
        landed_pair(own, A)
        landed_pair(own, B)

    @pl.when(i == at_xx)
    def _():
        landed_near(X, B)
        start(pair(X, B))
        landed_near(Y, A)
        start(pair(Y, A))
        landed_pair(X, A)
        landed_pair(Y, B)

    s = i - (n + 1)
    slot = lax.rem(i, 2)

    @pl.when(i == n)
    def _():
        fetch(0, 1 - slot)
        fetch_table(0, 1 - slot)

    @pl.when(s == 0)
    def _():
        pltpu.make_async_copy(y_acc, y_hbm, y_sem).start()
        landed_pair(X, B)
        landed_pair(Y, A)

    @pl.when(s == D)
    def _():
        landed_near(D, A)
        start(pair(D, A))
        landed_near(D, B)
        start(pair(D, B))
        fetch(s, slot)
        fetch_table(s, slot)

    @pl.when(s == D + 1)
    def _():
        landed_pair(D, A)
        landed_pair(D, B)
        fetch(s, slot)
        fetch_table(s, slot)

    @pl.when((s >= 0) & (s < n_dev) & (s != D - 1) & (s != D))
    def _():
        fetch(s + 1, 1 - slot)
        fetch_table(s + 1, 1 - slot)

    @pl.when(s >= 0)
    def _():
        pltpu.make_async_copy(h_hbm.at[pl.ds(0, rb), :], hbuf.at[slot], h_sem.at[slot]).wait()

        @pl.when(s < n_dev)
        def _():
            pltpu.make_async_copy(tab_hbm if with_tables else tab_hbm.at[0], tbuf.at[slot], h_sem.at[2 + slot]).wait()
        h = hbuf[slot]
        image = s < n_dev
        table = jnp.concatenate([tbuf[slot, t] for t in range(tbuf.shape[1])], axis=1)
        cos, sin = jnp.where(image, table[:half], 1.0), jnp.where(image, table[half:], 0.0)

        def lanes(v):
            return jnp.concatenate([v] * (rb // LANES), axis=1)

        def proj(part):
            rs = slice(part * nh * LANES, (part + 1) * nh * LANES)
            return lax.dot_general(wt[rs, :], h, (((1,), (1,)), ((), ())), preferred_element_type=jnp.float32)

        def biased(x, j):
            return (x + lanes(bb[head_rows(j), :])).astype(jnp.bfloat16)

        def normed(x, j, g):
            x = biased(x, j).astype(jnp.float32)
            ms = jnp.sum(x * x, axis=0, keepdims=True) * (1.0 / LANES)
            v = x * lax.rsqrt(ms + EPS) * lanes(gg[head_rows(g), :])
            a, b = v[:half], v[half:]
            return jnp.concatenate([a * cos - b * sin, a * sin + b * cos], axis=0).astype(jnp.bfloat16)

        q = proj(0)
        for t in range(nh):
            v = normed(q[head_rows(t)], t, 0).astype(jnp.float32) * (LANES ** -0.5 * LOG2E)
            hi = v.astype(jnp.bfloat16)
            qT_ref[t, :LANES] = hi
            qT_ref[t, LANES:] = (v - hi.astype(jnp.float32)).astype(jnp.bfloat16)
        k = proj(1)
        for t in range(nh):
            k_ref[t] = normed(k[head_rows(t)], nh + t, 1).T
        v = proj(2)
        for t in range(nh):
            vT_ref[t] = biased(v[head_rows(t)], 2 * nh + t)

    @pl.when(s == n_dev)
    def _():
        for copies in [near(own, A, X), near(own, B, X), near(own, B, Y), near(own, A, Y), near(Y, B, X), near(X, A, Y)] + [pair(o, p) for o in (own, X, Y, D) for p in (A, B)]:
            for cp in copies:
                cp.wait_send()
        pltpu.make_async_copy(y_acc, y_hbm, y_sem).wait()
        if with_tables:
            pltpu.make_async_copy(tab_hbm, T.at[slot_of(0)], own_sem).wait()


def block(h, w_in, b_in3, w_out, qk_gain, tables, layer, n_txt, nh, row0, collective_id, hc=512):
    total, d = h.shape
    n_dev = d // LANES // nh
    with_tables = tables.ndim == 3
    ff = w_in.shape[2] - 3 * d
    n = ff // hc
    m = total - row0
    rb = total - n_txt
    assert n_dev * n_txt == rb
    S = n_dev * total
    hbm = pl.BlockSpec(memory_space=pl.ANY)
    dma = pltpu.SemaphoreType.DMA
    bf, f32 = jnp.bfloat16, jnp.float32

    def at(i):
        return jnp.clip(i - (n + 1), 0, n_dev)

    t_shape = tables.shape if with_tables else tables.shape[1:]
    out_shape = [jax.ShapeDtypeStruct((m, d), f32), jax.ShapeDtypeStruct((n_dev, total, d), bf),
                 jax.ShapeDtypeStruct((nh, 2 * LANES, S), bf), jax.ShapeDtypeStruct((nh, S, LANES), bf), jax.ShapeDtypeStruct((nh, LANES, S), bf)]
    out_specs = [hbm, hbm, pl.BlockSpec((nh, 2 * LANES, rb), lambda i: (0, 0, at(i))), pl.BlockSpec((nh, rb, LANES), lambda i: (0, at(i), 0)),
                 pl.BlockSpec((nh, LANES, rb), lambda i: (0, 0, at(i)))]
    sems = [dma((2,)), dma((4,)), dma, dma((6,)), dma((6,)), dma((8,)), dma((8,))]
    if with_tables:
        out_shape.append(jax.ShapeDtypeStruct((n_dev, *tables.shape), f32))
        out_specs.append(hbm)
        sems += [dma((6,)), dma((6,)), dma((8,)), dma((8,)), dma]
    return pl.pallas_call(
        functools.partial(block_kernel, layer=layer, n=n, n_dev=n_dev, nh=nh, n_txt=n_txt, row0=row0, with_tables=with_tables, at_x=n * 5 // 12, at_xx=n * 5 // 6),
        grid=(n + 1 + n_dev + 1,),
        in_specs=[
            whole((total, d), pipeline_mode=pl.Buffered(1)),
            pl.BlockSpec((1, d, hc), lambda i: (layer, 0, 3 * d // hc + jnp.minimum(i, n - 1))),
            pl.BlockSpec((1, 1, hc), lambda i: (layer, 0, 3 * d // hc + jnp.minimum(i, n - 1))),
            pl.BlockSpec((1, hc, d), lambda i: (layer, d // hc + jnp.clip(i - 1, 0, n - 1), 0)),
            pl.BlockSpec((1, 1, b_in3.shape[2]), lambda i: (layer, 0, 0)),
            pl.BlockSpec((1, 2, LANES), lambda i: (layer, 0, 0)),
            hbm, hbm, hbm,
        ],
        out_specs=out_specs,
        out_shape=out_shape,
        scratch_shapes=[
            pltpu.VMEM((m, d), f32), pltpu.VMEM((m, hc), bf), pltpu.VMEM((m, hc), bf), pltpu.VMEM((3 * nh * LANES, d), bf), pltpu.VMEM((2, d, LANES), bf),
            pltpu.VMEM((3 * nh * LANES, LANES), f32), pltpu.VMEM((2 * LANES, LANES), f32), pltpu.VMEM((2, rb, d), bf), pltpu.VMEM((2, *t_shape), f32),
        ] + sems,
        compiler_params=params(**talking(collective_id)),
        cost_estimate=pl.CostEstimate(flops=4 * m * d * ff + 6 * S * d * nh * LANES, bytes_accessed=4 * d * ff + 2 * S * d, transcendentals=m * ff),
        name='block',
    )(h, w_in, b_in3, w_out, b_in3, qk_gain, h, w_in, tables)


def attn_kernel(qT_hbm, k_hbm, vT_hbm, *refs, qt, kc, n_dev, n_img, n_txt, with_txt):
    oi_hbm, *refs = refs
    if with_txt:
        ot_hbm, *refs = refs
        *refs, tbuf, tsend_sem, trecv_sem, town_sem = refs
    qT_ref, k_ref, vT_ref, s_scr, m_scr, part_scr, acc_scr, l_scr, obuf, in_sem, send_sem, recv_sem, own_sem = refs
    nh, S, hd = k_ref.shape
    nk = S // kc
    ahead = 2
    f32 = jnp.float32

    def load(t):
        pairs = ((qT_hbm, qT_ref), (k_hbm, k_ref), (vT_hbm, vT_ref))
        return [pltpu.make_async_copy(src.at[t], dst.at[t], in_sem.at[t, j]) for j, (src, dst) in enumerate(pairs)]

    for t in range(nh):
        for cp in load(t):
            cp.start()
    me = lax.axis_index('cfg') * N_CORE + lax.axis_index('core')
    z = lax.axis_index('z')

    def device(r):
        to, c = related(lax.axis_index('cfg'), lax.axis_index('core'), r)
        return to, z, c

    meet([device(r) for r in range(1, n_dev)])
    for cp in load(0):
        cp.wait()

    def score_chunk(head, q, slot, i, m):
        rows = pl.ds(i * kc, kc)
        k = k_ref[head, rows, :]
        s = dot(jnp.concatenate([k, k], axis=1), q)
        s_scr[slot, rows, :] = s
        return jnp.maximum(m, jnp.max(s.reshape(kc // 8, 8, qt), axis=0))

    def lowest():
        return jnp.full((8, qt), -jnp.inf, f32)

    def full_max(m):
        return jnp.broadcast_to(jnp.max(m, axis=0, keepdims=True), (8, qt))

    def prob_chunk(head, m, slot, i, l, acc):
        rows = pl.ds(i * kc, kc)
        p = jnp.exp2(s_scr[slot, rows, :].reshape(kc // 8, 8, qt) - m[None])
        l = l + jnp.sum(p, axis=0)
        return l, acc + dot(vT_ref[head, :, rows], p.reshape(kc, qt).astype(jnp.bfloat16))

    def load_q(tile):
        head, col = tile
        return qT_ref[head, :, pl.ds(pl.multiple_of(col, qt), qt)]

    def normalized(acc, l):
        return (acc / jnp.sum(l, axis=0, keepdims=True)).T.astype(jnp.bfloat16)

    def stream(n_pairs, tile, put, after, before=None):
        first, second = tile(0), tile(1)
        q, m = load_q(first), lowest()
        for i in range(nk):
            m = score_chunk(first[0], q, 0, i, m)
        m_scr[...] = full_max(m)
        q, m = load_q(second), lowest()
        for i in range(ahead):
            m = score_chunk(second[0], q, 1, i, m)
        part_scr[...] = m
        acc_scr[...] = jnp.zeros_like(acc_scr)
        l_scr[...] = jnp.ones_like(l_scr)

        def pair(p, carry):
            if before is not None:
                before(p)
            later = lax.rem(p + 1, n_pairs)
            tiles = [tile(2 * p), tile(2 * p + 1), tile(2 * later), tile(2 * later + 1)]
            m, top = part_scr[...], m_scr[...]
            put(lax.rem(p + n_pairs - 1, n_pairs), 1, normalized(acc_scr[...], l_scr[...]))
            for half in range(2):
                l, acc = jnp.zeros((8, qt), f32), jnp.zeros((hd, qt), f32)
                q1, q2 = load_q(tiles[half + 1]), load_q(tiles[half + 2])
                for i in range(nk):
                    j = i + ahead
                    if j < nk:
                        m = score_chunk(tiles[half + 1][0], q1, 1 - half, j, m)
                    else:
                        if j == nk:
                            following, m = full_max(m), lowest()
                        m = score_chunk(tiles[half + 2][0], q2, half, j - nk, m)
                    l, acc = prob_chunk(tiles[half][0], top, half, i, l, acc)
                top = following
                if half == 0:
                    put(p, 0, normalized(acc, l))
                else:
                    acc_scr[...] = acc
                    l_scr[...] = l
            part_scr[...] = m
            m_scr[...] = top

            @pl.when(p > 0)
            def _():
                after(p - 1)
            return carry

        lax.fori_loop(0, n_pairs, pair, 0)
        put(n_pairs - 1, 1, normalized(acc_scr[...], l_scr[...]))
        after(n_pairs - 1)

    def relation_of(p):
        return lax.rem(p + 1, n_dev)

    def img_tile(u):
        p = u // 2
        return p // n_dev, relation_of(p) * n_img + lax.rem(u, 2) * qt

    def img_put(p, half, o):
        obuf[p, half * qt:(half + 1) * qt, :] = o

    def img_send(p):
        head, owner = p // n_dev, relation_of(p)

        @pl.when(owner == 0)
        def _():
            pltpu.make_async_copy(obuf.at[p], oi_hbm.at[me, head], own_sem).start()

        @pl.when(owner != 0)
        def _():
            remote(obuf.at[p], oi_hbm.at[me, head], send_sem, recv_sem, device(owner)).start()

    def next_head(p):
        @pl.when((relation_of(p) == 0) & (p < nh * n_dev - 1))
        def _():
            for cp in load(p // n_dev + 1):
                cp.wait()

    stream(nh * n_dev, img_tile, img_put, img_send, next_head)

    if with_txt:
        n_text = n_dev * n_txt
        tiles = n_text // qt
        assert tiles == 2

        def txt_tile(u):
            return u // tiles, n_dev * n_img + lax.rem(u, tiles) * qt

        def txt_put(p, half, o):
            tbuf[p, half * qt:(half + 1) * qt, :] = o

        def txt_send(head):
            for owner in range(n_dev):
                src = tbuf.at[head, pl.ds(owner * n_txt, n_txt), :]
                if owner == 0:
                    pltpu.make_async_copy(src, ot_hbm.at[me, head], town_sem).start()
                else:
                    remote(src, ot_hbm.at[me, head], tsend_sem, trecv_sem, device(owner)).start()

        stream(nh, txt_tile, txt_put, txt_send)

    others = pl.ds(0, n_dev - 1)
    wait_for(oi_hbm.at[others], send_sem)
    wait_for(oi_hbm.at[others], recv_sem)
    wait_for(oi_hbm.at[me], own_sem)
    if with_txt:
        wait_for(ot_hbm.at[others], tsend_sem)
        wait_for(ot_hbm.at[others], trecv_sem)
        wait_for(ot_hbm.at[me], town_sem)


def largest(n, cap, unit):
    return max(c for c in range(unit, cap + 1, unit) if n % c == 0)


def attention(qT, k, vT, n_dev, n_txt, with_txt, collective_id):
    nh, S, hd = k.shape
    n_img = S // n_dev - n_txt
    qt = n_img // 2
    kc = largest(S, 768, 256)
    SQ = n_dev * (n_img + (n_txt if with_txt else 0))
    dma = pltpu.SemaphoreType.DMA
    bf, f32 = jnp.bfloat16, jnp.float32
    out_shape = [jax.ShapeDtypeStruct((n_dev, nh, n_img, hd), bf)]
    stat = pltpu.VMEM((8, qt), f32)
    scratch = [pltpu.VMEM(v.shape, bf) for v in (qT, k, vT)] + [pltpu.VMEM((2, S, qt), f32), stat, stat, pltpu.VMEM((hd, qt), f32), stat, pltpu.VMEM((nh * n_dev, n_img, hd), bf)]
    sems = [dma((nh, 3)), dma, dma, dma]
    if with_txt:
        out_shape.append(jax.ShapeDtypeStruct((n_dev, nh, n_txt, hd), bf))
        sems += [pltpu.VMEM((nh, n_dev * n_txt, hd), bf), dma, dma, dma]
    return pl.pallas_call(
        functools.partial(attn_kernel, qt=qt, kc=kc, n_dev=n_dev, n_img=n_img, n_txt=n_txt, with_txt=with_txt),
        in_specs=[pl.BlockSpec(memory_space=pl.ANY)] * 3,
        out_specs=[pl.BlockSpec(memory_space=pl.ANY)] * len(out_shape),
        out_shape=out_shape,
        scratch_shapes=scratch + sems,
        compiler_params=pltpu.CompilerParams(vmem_limit_bytes=VMEM_BYTES, **talking(collective_id)),
        cost_estimate=pl.CostEstimate(flops=6 * nh * SQ * S * hd, bytes_accessed=8 * nh * S * hd, transcendentals=nh * S * SQ),
        name='attn',
    )(qT, k, vT)


def out_kernel(*refs, nc, ne, n_txt, row0, last, gate_row):
    if last:
        oi_ref, w_ref, bo_ref, mods_ref, wf_ref, bf_ref, x_hbm, y_hbm, vel_hbm, lhs, acc, ybuf, xbuf, hs, vel, sems, own_sem, send_sem, recv_sem = refs
    else:
        oi_ref, ot_ref, w_ref, bo_ref, mods_ref, x_hbm, y_hbm, xo_ref, ho_ref, lhs, acc, ybuf, xbuf, sems = refs
    i = pl.program_id(0)
    R = acc.shape[0]
    er = R // ne
    copy_y = pltpu.make_async_copy(y_hbm, ybuf, sems.at[0])
    copy_x = pltpu.make_async_copy(x_hbm.at[pl.ds(row0, R), :], xbuf, sems.at[1])

    @pl.when(i == 0)
    def _():
        copy_y.start()
        copy_x.start()

    if last:
        cfg, z, core = lax.axis_index('cfg'), lax.axis_index('z'), lax.axis_index('core')

        @pl.when(i == 0)
        def _():
            meet([(z, e, core) for e in range(ne)] + [(e, cfg, core) for e in range(ne)])

    @pl.when(i < nc)
    def _():
        for t in range(oi_ref.shape[0]):
            cols = head_rows(t)
            if last:
                lhs[:, cols] = oi_ref[t, 0]
            else:
                lhs[:n_txt, cols] = ot_ref[t, 0]
                lhs[n_txt:, cols] = oi_ref[t, 0]

    @pl.when(i == 0)
    def _():
        acc[...] = dot(lhs[...], w_ref[0])

    @pl.when((i > 0) & (i < nc))
    def _():
        acc[...] += dot(lhs[...], w_ref[0])

    @pl.when(i == nc)
    def _():
        copy_y.wait()
        copy_x.wait()

    @pl.when(i >= nc)
    def _():
        gate, shift, scale = (mods_ref[r:r + 1, :] for r in range(gate_row, gate_row + 3))
        bo = bo_ref[0].astype(jnp.float32)
        sub = 16 if er % 16 == 0 else 8

        def chunk(c, carry):
            rs = pl.ds(pl.multiple_of((i - nc) * er + c * sub, sub), sub)
            ls = pl.ds(pl.multiple_of(c * sub, sub), sub)
            y = acc[rs, :] + ybuf[rs, :] + bo
            xn = (xbuf[rs, :].astype(jnp.float32) + gate * y).astype(jnp.bfloat16)
            h = ln_mod(xn.astype(jnp.float32), shift, scale)
            if last:
                hs[ls, :] = h
            else:
                xo_ref[ls, :] = xn
                ho_ref[ls, :] = h
            return carry

        lax.fori_loop(0, er // sub, chunk, 0, unroll=3 if (er // sub) % 3 == 0 else 2)

    if last:
        def deliver(e):
            @pl.when((z == cfg) & (e == z))
            def _():
                pltpu.make_async_copy(vel.at[e], vel_hbm.at[cfg], own_sem).start()

            @pl.when((z != cfg) | (e != z))
            def _():
                remote(vel.at[e], vel_hbm.at[cfg], send_sem.at[e], recv_sem.at[cfg], (z, e, core)).start()

        @pl.when(i >= nc)
        def _():
            w = jnp.concatenate([wf_ref[...], jnp.zeros((LANES - wf_ref.shape[0], wf_ref.shape[1]), wf_ref.dtype)], axis=0)
            v = lax.dot_general(hs[...], w, (((1,), (1,)), ((), ())), preferred_element_type=jnp.float32)
            b = bf_ref[...].astype(jnp.float32)
            vel[i - nc] = v + jnp.concatenate([b, jnp.zeros((1, LANES - b.shape[1]), jnp.float32)], axis=1)
            deliver(i - nc)

        @pl.when(i == nc + ne - 1)
        def _():
            for e in range(ne):
                @pl.when((z == cfg) & (e == z))
                def _():
                    pltpu.make_async_copy(vel.at[e], vel_hbm.at[e], own_sem).wait()

                @pl.when((z != cfg) | (e != z))
                def _():
                    remote(vel.at[e], vel_hbm.at[e], send_sem.at[e], recv_sem.at[e], (z, e, core)).wait_send()
                    remote(vel.at[e], vel_hbm.at[e], send_sem.at[e], recv_sem.at[e], (z, e, core)).wait_recv()


def out_proj(os, w_out, b_out3, mods, x, y_mlp, layer, row0, final=None, collective_id=None, kc=512):
    oi = os[0]
    _, nh, n_img, _ = oi.shape
    R = sum(o.shape[2] for o in os)
    ne = 4
    d = w_out.shape[2]
    nc = d // kc
    per = nc // nh
    hp = kc // LANES
    last = final is not None

    def o_map(i):
        j = jnp.minimum(i, nc - 1)
        return lax.rem(j, per), j // per, 0, 0

    in_specs = [pl.BlockSpec((hp, 1, o.shape[2], LANES), o_map) for o in os] + [
        pl.BlockSpec((1, kc, d), lambda i: (layer, jnp.minimum(i, nc - 1), 0)),
        pl.BlockSpec((1, 1, d), lambda i: (layer, 0, 0)),
        whole(mods.shape),
    ]
    args = [*os, w_out, b_out3, mods]
    scratch = [pltpu.VMEM((R, kc), jnp.bfloat16), pltpu.VMEM((R, d), jnp.float32), pltpu.VMEM((R, d), jnp.float32), pltpu.VMEM((R, d), jnp.bfloat16)]
    sems = [pltpu.SemaphoreType.DMA((2,))]
    if last:
        n_out = LANES
        in_specs += [whole(v.shape) for v in final]
        args += list(final)
        out_specs = pl.BlockSpec(memory_space=pl.ANY)
        out_shape = jax.ShapeDtypeStruct((ne, R // ne, n_out), jnp.float32)
        scratch += [pltpu.VMEM((R // ne, d), jnp.bfloat16), pltpu.VMEM((ne, R // ne, n_out), jnp.float32)]
        sems += [pltpu.SemaphoreType.DMA, pltpu.SemaphoreType.DMA((ne,)), pltpu.SemaphoreType.DMA((ne,))]
        compiler_params = params(**talking(collective_id))
    else:
        out_specs = [pl.BlockSpec((R // ne, d), lambda i: (jnp.maximum(i - nc, 0), 0))] * 2
        out_shape = [jax.ShapeDtypeStruct((R, d), jnp.bfloat16)] * 2
        compiler_params = params()
    return pl.pallas_call(
        functools.partial(out_kernel, nc=nc, ne=ne, n_txt=R - n_img, row0=row0, last=last, gate_row=3 * layer + 2),
        grid=(nc + ne,),
        in_specs=in_specs + [pl.BlockSpec(memory_space=pl.ANY)] * 2,
        out_specs=out_specs,
        out_shape=out_shape,
        scratch_shapes=scratch + sems,
        compiler_params=compiler_params,
        cost_estimate=pl.CostEstimate(flops=2 * R * d * d, bytes_accessed=2 * d * d + 14 * R * d, transcendentals=0),
        name='outp',
    )(*args, x, y_mlp)


def enter_kernel(xt_hbm, xi_hbm, cond_ref, wm_ref, wf_ref, bm_ref, bf_ref, cos_hbm, sin_hbm, mods_ref, xo_ref, ho_ref, tab_out,
                 stage, xbuf, cond_buf, s_scr,
                 cond_send, cond_recv, p_send, p_recv, c_send, c_recv, own_sem, t_send, t_recv, town_sem, *, n_mod, n_steps, per_row, per_layer):
    i = pl.program_id(0)
    n, rows, d = xbuf.shape
    tp = xt_hbm.shape[0] // n
    ip = xi_hbm.shape[0] // n
    cfg, z, core = lax.axis_index('cfg'), lax.axis_index('z'), lax.axis_index('core')
    across = [related(cfg, core, r)[0] for r in range(2, 2 * n, 2)]
    heights = [lax.rem(z + s, n) for s in range(1, n)]
    cut = rows // 2

    def piece_refs(j, dst):
        first = cut - tp
        head = [(xt_hbm.at[pl.ds(j * tp, tp), :], dst.at[pl.ds(0, tp), :]), (xi_hbm.at[pl.ds(j * ip, first), :], dst.at[pl.ds(tp, first), :])]
        return head, [(xi_hbm.at[pl.ds(j * ip + first, ip - first), :], dst.at[pl.ds(cut, ip - first), :])]

    def tables(to):
        half = cos_hbm.shape[0]
        cols = pl.ds(pl.multiple_of(cfg * ip, ip), ip)
        return [(src.at[:, cols], to.at[pl.ds(t * half, half), :]) for t, src in enumerate((cos_hbm, sin_hbm))]

    def forward(group, t, part):
        at = pl.ds(part * cut, cut)

        @pl.when(group == z)
        def _():
            xbuf[z, at, :] = stage[group, at, :]

        @pl.when(group != z)
        def _():
            remote(stage.at[group, at, :], xbuf.at[z, at, :], c_send.at[t], c_recv.at[z], (cfg, group, core)).start()

    def silu_of(ref):
        v = ref[...].astype(jnp.float32)
        s_scr[...] = jnp.broadcast_to((v * jax.nn.sigmoid(v)).astype(jnp.bfloat16), s_scr.shape)

    @pl.when(i == 0)
    def _():
        meet([(j, z, core) for j in across] + [(cfg, h, core) for h in heights])

        @pl.when(cfg == z)
        def _():
            for t, j in enumerate(across):
                remote(cond_ref, cond_buf, cond_send.at[t], cond_recv, (j, z, core)).start()
        for t, j in enumerate(across):
            for part, refs in enumerate(piece_refs(j, stage.at[cfg])):
                for src, dst in refs:
                    remote(src, dst, p_send.at[t], p_recv.at[cfg, part], (j, z, core)).start()
        mine = sum(piece_refs(cfg, xbuf.at[z]), [])

        @pl.when(cfg == z)
        def _():
            for src, dst in mine:
                pltpu.make_async_copy(src, dst, own_sem).start()

        @pl.when(cfg != z)
        def _():
            for src, dst in mine:
                remote(src, dst, c_send.at[n - 1], c_recv.at[z], (cfg, cfg, core)).start()
        for t, h in enumerate(heights):
            for src, dst in tables(tab_out.at[z]):
                remote(src, dst, t_send.at[t], t_recv.at[z], (cfg, h, core)).start()
        for src, dst in tables(tab_out.at[z]):
            pltpu.make_async_copy(src, dst, town_sem).start()

        @pl.when(cfg == z)
        def _():
            silu_of(cond_ref)

        @pl.when(cfg != z)
        def _():
            remote(cond_ref, cond_buf, cond_send.at[0], cond_recv, (cfg, z, core)).wait_recv()
            silu_of(cond_buf)

    row, col = i // per_row, lax.rem(i, per_row)
    width = wm_ref.shape[2]
    cols = pl.ds(pl.multiple_of(col * width, width), width)

    @pl.when(i < n_mod)
    def _():
        v = dot(s_scr[...], wm_ref[0])
        b = bm_ref[...].astype(jnp.float32)
        of_layer = lax.broadcasted_iota(jnp.int32, b.shape, 0) == i // per_layer
        mods_ref[pl.ds(row, 1), cols] = v[0:1] + jnp.sum(jnp.where(of_layer, b, 0.0), axis=0, keepdims=True)

    @pl.when(i >= n_mod)
    def _():
        v = dot(s_scr[...], wf_ref[...])
        mods_ref[pl.ds(row, 1), cols] = v[0:1] + bf_ref[...].astype(jnp.float32)

    def arrived(t, part):
        j = across[t]
        wait_for(stage.at[j, pl.ds(part * cut, cut), :], p_recv.at[j, part])
        forward(j, t, part)

    @pl.when(i == n_steps // 5)
    def _():
        arrived(0, 0)

    @pl.when(i == n_steps * 2 // 5)
    def _():
        arrived(0, 1)
        arrived(1, 0)
        arrived(1, 1)

    @pl.when(i == n_steps * 3 // 4)
    def _():
        arrived(2, 0)
        arrived(2, 1)

    @pl.when(i == n_steps - 1)
    def _():
        shift, scale = mods_ref[0:1, :], mods_ref[1:2, :]

        @pl.when(cfg == z)
        def _():
            wait_for(xbuf.at[z], own_sem)

        def norm_rows(k, src, dst, count):
            sub = 16 if count % 16 == 0 else 8

            def chunk(c, carry):
                v = xbuf[k, pl.ds(pl.multiple_of(src + c * sub, sub), sub), :]
                to = pl.ds(pl.multiple_of(dst + c * sub, sub), sub)
                xo_ref[to, :] = v
                ho_ref[to, :] = ln_mod(v.astype(jnp.float32), shift, scale)
                return carry
            lax.fori_loop(0, count // sub, chunk, 0, unroll=min(4, count // sub))

        def height(s, carry):
            k = lax.rem(z + s, n)

            @pl.when(s > 0)
            def _():
                wait_for(xbuf.at[k], c_recv.at[k])
            norm_rows(k, 0, k * tp, tp)
            norm_rows(k, tp, n * tp + k * ip, ip)
            return carry

        lax.fori_loop(0, n, height, 0)

        for t, j in enumerate(across):
            wait_for(xbuf.at[0], p_send.at[t])

            @pl.when(j != z)
            def _():
                wait_for(xbuf.at[0], c_send.at[t])

        @pl.when(cfg != z)
        def _():
            wait_for(xbuf.at[0], c_send.at[n - 1])

        @pl.when(cfg == z)
        def _():
            for t, j in enumerate(across):
                remote(cond_ref, cond_buf, cond_send.at[t], cond_recv, (j, z, core)).wait_send()
        for t, h in enumerate(heights):
            wait_for(tab_out.at[z], t_send.at[t])
            wait_for(tab_out.at[h], t_recv.at[h])
        wait_for(tab_out.at[z], town_sem)


def enter(x_txt, x_img, cond, w_mod, w_fmod, b_mod, b_fmod, cosT, sinT, n, collective_id, width=512):
    n_txt, d = x_txt.shape
    n_img = x_img.shape[0]
    total = n_txt + n_img
    rows = total // n
    n_layers, _, dm = w_mod.shape
    per_layer, n_fin, per_row = dm // width, w_fmod.shape[1] // width, d // width
    n_mod = n_layers * per_layer
    steps = n_mod + n_fin
    dma = pltpu.SemaphoreType.DMA
    bf, f32 = jnp.bfloat16, jnp.float32

    def layer_of(i):
        j = jnp.minimum(i, n_mod - 1)
        return j // per_layer, lax.rem(j, per_layer)

    def last_of(i):
        return 0, jnp.maximum(i - n_mod, 0)

    hbm = pl.BlockSpec(memory_space=pl.ANY)
    out_shape = [jax.ShapeDtypeStruct((steps // per_row, d), f32), jax.ShapeDtypeStruct((total, d), bf), jax.ShapeDtypeStruct((total, d), bf),
                 jax.ShapeDtypeStruct((n, 2 * cosT.shape[0], n_img // n), f32)]
    return pl.pallas_call(
        functools.partial(enter_kernel, n_mod=n_mod, n_steps=steps, per_row=per_row, per_layer=per_layer),
        grid=(steps,),
        in_specs=[hbm, hbm, whole(cond.shape), pl.BlockSpec((1, d, width), lambda i: (layer_of(i)[0], 0, layer_of(i)[1])), pl.BlockSpec((d, width), last_of),
                  pl.BlockSpec((n_layers, width), lambda i: (0, layer_of(i)[1])), pl.BlockSpec((1, width), last_of), hbm, hbm],
        out_specs=[whole(v.shape) for v in out_shape[:-1]] + [hbm],
        out_shape=out_shape,
        scratch_shapes=[pltpu.VMEM((n, rows, d), bf), pltpu.VMEM((n, rows, d), bf), pltpu.VMEM(cond.shape, bf), pltpu.VMEM((16, d), bf),
                        dma((n - 1,)), dma, dma((n - 1,)), dma((n, 2)), dma((n,)), dma((n,)), dma, dma((n - 1,)), dma((n,)), dma],
        compiler_params=params(**talking(collective_id)),
        cost_estimate=pl.CostEstimate(flops=2 * 16 * d * width * steps, bytes_accessed=2 * d * width * steps, transcendentals=0),
        name='enter',
    )(x_txt, x_img, cond, w_mod, w_fmod, b_mod, b_fmod, cosT, sinT)


def solution(mesh):
    n_cfg = mesh.devices.shape[0]
    n_z = mesh.devices.shape[1] // N_CORE
    grid = Mesh(mesh.devices.reshape(n_cfg, n_z, N_CORE), ('cfg', 'z', 'core'))
    assert n_cfg == n_z == 4
    n_dev = n_cfg * N_CORE
    token_spec = P(('cfg', 'z', 'core'), None)
    seq_spec = P(('z', 'core'), None)
    in_specs = (token_spec, token_spec, P('cfg', None), seq_spec, seq_spec, token_spec) + (P(),) * 13

    def body(x_txt, x_img, cond_vec, cos_img, sin_img, z_lat, t_cur, t_next, w_mod, b_mod, w_in, b_in, qk_gain, w_out, b_out, w_fmod, b_fmod, w_final, b_final):
        n_txt, d = x_txt.shape
        n_img = x_img.shape[0]
        n_layers = w_mod.shape[0]
        nh = d // LANES // n_dev
        n_out = w_final.shape[1]

        mods, x, h, own = enter(x_txt, x_img, cond_vec, w_mod, w_fmod, b_mod, b_fmod[None], cos_img.T, sin_img.T, n_cfg, 1)
        b_in3, b_out3 = b_in[:, None, :], b_out[:, None, :]
        for l in range(n_layers):
            last = l == n_layers - 1
            row0 = n_txt if last else 0
            y_mlp, _, qT, k, vT, *more = block(h, w_in, b_in3, w_out, qk_gain, own, l, n_txt, nh, row0, 2 + 2 * l)
            own = more[0] if more else own
            os = attention(qT, k, vT, n_dev, n_txt, not last, 3 + 2 * l)
            if last:
                vel = out_proj(os, w_out, b_out3, mods, x, y_mlp, l, row0, final=(w_final.T, b_final[None]), collective_id=2 + 2 * n_layers)
            else:
                x, h = out_proj(os, w_out, b_out3, mods, x, y_mlp, l, row0)

        return z_lat + (t_next - t_cur) * vel.reshape(n_img, LANES)[:, :n_out]

    return jax.shard_map(body, mesh=grid, in_specs=in_specs, out_specs=token_spec, check_vma=False)
```

```python
import functools
import math

import jax
import jax.numpy as jnp
from jax import lax
from jax.experimental import pallas as pl
from jax.experimental.pallas import tpu as pltpu
from jax.sharding import Mesh, PartitionSpec as P

EPS = 1e-6
LANES = 128
GELU_C = math.sqrt(2.0 / math.pi)
LOG2E = math.log2(math.e)
VMEM_BYTES = 60 * 2**20
N_CORE = 2
MESH = pl.DeviceIdType.MESH


def params(**kw):
    return pltpu.CompilerParams(vmem_limit_bytes=VMEM_BYTES, dimension_semantics=('arbitrary',), **kw)


def talking(collective_id):
    return dict(collective_id=collective_id, has_side_effects=True)


def whole(shape, **kw):
    return pl.BlockSpec(shape, lambda i: (0,) * len(shape), **kw)


def head_rows(j):
    return slice(j * LANES, (j + 1) * LANES)


def columns_of(v):
    return jnp.broadcast_to(v.astype(jnp.float32), (LANES, LANES)).T


def wait_for(ref, sem):
    pltpu.make_async_copy(ref, ref, sem).wait()


def dot(a, b):
    return jnp.dot(a, b, preferred_element_type=jnp.float32)


def remote(src, dst, send_sem, recv_sem, device):
    return pltpu.make_async_remote_copy(src_ref=src, dst_ref=dst, send_sem=send_sem, recv_sem=recv_sem, device_id=device, device_id_type=MESH)


def meet(devices):
    barrier = pltpu.get_barrier_semaphore()
    for device in devices:
        pl.semaphore_signal(barrier, inc=1, device_id=device, device_id_type=MESH)
    pl.semaphore_wait(barrier, len(devices))


def ln_mod(x, shift, scale):
    centered = x - jnp.mean(x, axis=-1, keepdims=True)
    var = jnp.mean(centered * centered, axis=-1, keepdims=True)
    return (centered * lax.rsqrt(var + EPS) * (1.0 + scale) + shift).astype(jnp.bfloat16)


def gelu_tanh(u):
    return u * (0.5 * (1.0 + jnp.tanh(GELU_C * (u + 0.044715 * (u * u * u)))))


def related(cfg, core, r):
    cx, cy = cfg // 2, lax.rem(cfg, 2)
    x = lax.rem(cx + lax.rem(r // 2, 2), 2)
    y = lax.rem(cy + r // 4, 2)
    return x * 2 + y, lax.rem(core + lax.rem(r, 2), 2)


def block_kernel(*refs, layer, n, n_dev, nh, n_txt, row0, with_tables, at_x, at_xx):
    h_ref, w1_ref, b1_ref, w2_ref, bias_ref, gain_ref, h_hbm, w_hbm, tab_hbm, y_hbm, H, qT_ref, k_ref, vT_ref, *refs = refs
    T = tab_hbm
    if with_tables:
        T, *refs = refs
    (y_acc, u_scr, act, wt, wbuf, bb, gg, hbuf, tbuf, w_sem, h_sem, y_sem, *refs) = refs
    i = pl.program_id(0)
    cfg, z, core = lax.axis_index('cfg'), lax.axis_index('z'), lax.axis_index('core')
    rows = y_acc.shape[0]
    total, d = h_hbm.shape
    rb = total - n_txt
    half = LANES // 2
    n_heads = d // LANES
    stride = n_heads // nh

    def device(r):
        to, c = related(cfg, core, r)
        return to, z, c

    def slot_of(r):
        to, c = related(cfg, core, r)
        return to * N_CORE + c

    own, X, Y, D = range(0, n_dev, 2)
    A, B = range(2)

    def part_of(ref, piece):
        size = ref.shape[0] // 2
        return ref.at[pl.ds(piece * size, size)]

    arrays = [(h_hbm, H)] + ([(tab_hbm, T)] if with_tables else [])
    if with_tables:
        own_sem, refs = refs[-1], refs[:-1]

    def move(origin, piece, to, send, recv, k_send, k_recv):
        out = []
        for t, (mine, every) in enumerate(arrays):
            dst = part_of(every.at[slot_of(origin)], piece)
            src = part_of(mine, piece) if origin == own else dst
            out.append(remote(src, dst, send[t].at[k_send], recv[t].at[k_recv], device(to)))
        return out

    near_send, near_recv, pair_send, pair_recv = (refs[t::4] for t in range(4))

    def near(origin, piece, to):
        order = 2 if origin else piece
        return move(origin, piece, to, near_send, near_recv, (to - X) // 2 * 3 + order, (origin ^ to) - X + piece)

    def pair(origin, piece):
        return move(origin, piece, 1, pair_send, pair_recv, origin + piece, origin + piece)

    def start(copies):
        for cp in copies:
            cp.start()

    def landed(sems, k, origin, piece):
        for t, (_, every) in enumerate(arrays):
            wait_for(part_of(every.at[slot_of(origin)], piece), sems[t].at[k])

    def landed_near(origin, piece):
        landed(near_recv, origin - X + piece, origin, piece)

    def landed_pair(origin, piece):
        landed(pair_recv, origin + piece, origin + 1, piece)

    def w_cols(j):
        col = (j // nh * n_heads + lax.rem(j, nh) * stride + cfg * N_CORE + core) * LANES
        return pl.ds(pl.multiple_of(col, LANES), LANES)

    def w_copy(j):
        return pltpu.make_async_copy(w_hbm.at[layer, :, w_cols(j)], wbuf.at[lax.rem(j, 2)], w_sem.at[lax.rem(j, 2)])

    def w_turn(j):
        w_copy(j).wait()
        to = pl.ds(pl.multiple_of(j * LANES, LANES), LANES)
        wt[to, :] = wbuf[lax.rem(j, 2)].T
        bb[to, :] = columns_of(bias_ref[0, :, w_cols(j)])

    def fetch(s, slot):
        @pl.when(s == 0)
        def _():
            pltpu.make_async_copy(h_hbm.at[pl.ds(n_txt, rb), :], hbuf.at[slot], h_sem.at[slot]).start()

        @pl.when((s > 0) & (s < n_dev))
        def _():
            pltpu.make_async_copy(H.at[slot_of(s), pl.ds(n_txt, rb), :], hbuf.at[slot], h_sem.at[slot]).start()

        @pl.when(s == n_dev)
        def _():
            pltpu.make_async_copy(h_hbm.at[pl.ds(0, n_txt), :], hbuf.at[slot, pl.ds(0, n_txt), :], h_sem.at[slot]).start()
            for r in range(1, n_dev):
                pltpu.make_async_copy(H.at[slot_of(r), pl.ds(0, n_txt), :], hbuf.at[slot, pl.ds(r * n_txt, n_txt), :], h_sem.at[slot]).start()

    def fetch_table(s, slot):
        if with_tables:
            @pl.when(s == 0)
            def _():
                pltpu.make_async_copy(tab_hbm, tbuf.at[slot], h_sem.at[2 + slot]).start()

            @pl.when((s > 0) & (s < n_dev))
            def _():
                pltpu.make_async_copy(T.at[slot_of(s)], tbuf.at[slot], h_sem.at[2 + slot]).start()
        else:
            @pl.when(s < n_dev)
            def _():
                pltpu.make_async_copy(T.at[slot_of(s)], tbuf.at[slot], h_sem.at[2 + slot]).start()

    sub = 2
    step = rows // sub

    def up():
        for r in range(sub):
            u = dot(h_ref[row0 + r * step:row0 + (r + 1) * step, :], w1_ref[0])
            u_scr[r * step:(r + 1) * step, :] = (u + b1_ref[0].astype(jnp.float32)).astype(jnp.bfloat16)

    def gelu():
        act[...] = gelu_tanh(u_scr[...].astype(jnp.float32)).astype(jnp.bfloat16)

    def down():
        for r in range(sub):
            rs = slice(r * step, (r + 1) * step)
            y_acc[rs, :] += dot(act[rs, :], w2_ref[0])

    @pl.when(i == 0)
    def _():
        w_copy(0).start()
        w_copy(1).start()
        meet([device(1), device(X), device(Y)])
        start(near(own, A, X))
        start(near(own, B, Y))
        start(pair(own, A))
        start(pair(own, B))
        start(near(own, B, X))
        start(near(own, A, Y))
        if with_tables:
            pltpu.make_async_copy(tab_hbm, T.at[slot_of(0)], own_sem).start()
        for j in range(2):
            gg[head_rows(j), :] = columns_of(gain_ref[0, j:j + 1, :])
        y_acc[...] = jnp.zeros_like(y_acc)
        up()

    @pl.when((i > 0) & (i < n))
    def _():
        gelu()
        up()
        down()

    @pl.when(i == n)
    def _():
        gelu()
        down()

    @pl.when((i > 0) & (i <= 3 * nh))
    def _():
        w_turn(i - 1)

        @pl.when(i + 1 < 3 * nh)
        def _():
            w_copy(i + 1).start()

    @pl.when(i == at_x)
    def _():
        landed_near(X, A)
        start(near(X, A, Y))
        start(pair(X, A))
        landed_near(Y, B)
        start(near(Y, B, X))
        start(pair(Y, B))
        landed_pair(own, A)
        landed_pair(own, B)

    @pl.when(i == at_xx)
    def _():
        landed_near(X, B)
        start(pair(X, B))
        landed_near(Y, A)
        start(pair(Y, A))
        landed_pair(X, A)
        landed_pair(Y, B)

    s = i - (n + 1)
    slot = lax.rem(i, 2)

    @pl.when(i == n)
    def _():
        fetch(0, 1 - slot)
        fetch_table(0, 1 - slot)

    @pl.when(s == 0)
    def _():
        pltpu.make_async_copy(y_acc, y_hbm, y_sem).start()

    @pl.when(s == X)
    def _():
        landed_pair(X, B)
        landed_pair(Y, A)

    @pl.when(s == D)
    def _():
        landed_near(D, A)
        start(pair(D, A))
        landed_near(D, B)
        start(pair(D, B))
        fetch(s, slot)
        fetch_table(s, slot)

    @pl.when(s == D + 1)
    def _():
        landed_pair(D, A)
        landed_pair(D, B)
        fetch(s, slot)
        fetch_table(s, slot)

    @pl.when((s >= 0) & (s < n_dev) & (s != D - 1) & (s != D))
    def _():
        fetch(s + 1, 1 - slot)
        fetch_table(s + 1, 1 - slot)

    @pl.when(s >= 0)
    def _():
        pltpu.make_async_copy(h_hbm.at[pl.ds(0, rb), :], hbuf.at[slot], h_sem.at[slot]).wait()

        @pl.when(s < n_dev)
        def _():
            pltpu.make_async_copy(tab_hbm if with_tables else tab_hbm.at[0], tbuf.at[slot], h_sem.at[2 + slot]).wait()
        h = hbuf[slot]
        image = s < n_dev
        table = jnp.concatenate([tbuf[slot, t] for t in range(tbuf.shape[1])], axis=1)
        cos, sin = jnp.where(image, table[:half], 1.0), jnp.where(image, table[half:], 0.0)

        def lanes(v):
            return jnp.concatenate([v] * (rb // LANES), axis=1)

        def proj(part):
            rs = slice(part * nh * LANES, (part + 1) * nh * LANES)
            return lax.dot_general(wt[rs, :], h, (((1,), (1,)), ((), ())), preferred_element_type=jnp.float32)

        def biased(x, j):
            return (x + lanes(bb[head_rows(j), :])).astype(jnp.bfloat16)

        def normed(x, j, g):
            x = biased(x, j).astype(jnp.float32)
            ms = jnp.sum(x * x, axis=0, keepdims=True) * (1.0 / LANES)
            v = x * lax.rsqrt(ms + EPS) * lanes(gg[head_rows(g), :])
            a, b = v[:half], v[half:]
            return jnp.concatenate([a * cos - b * sin, a * sin + b * cos], axis=0).astype(jnp.bfloat16)

        q = proj(0)
        for t in range(nh):
            v = normed(q[head_rows(t)], t, 0).astype(jnp.float32) * (LANES ** -0.5 * LOG2E)
            hi = v.astype(jnp.bfloat16)
            qT_ref[t, :LANES] = hi
            qT_ref[t, LANES:] = (v - hi.astype(jnp.float32)).astype(jnp.bfloat16)
        k = proj(1)
        for t in range(nh):
            k_ref[t] = normed(k[head_rows(t)], nh + t, 1).T
        v = proj(2)
        for t in range(nh):
            vT_ref[t] = biased(v[head_rows(t)], 2 * nh + t)

    @pl.when(s == n_dev)
    def _():
        for copies in [near(own, A, X), near(own, B, X), near(own, B, Y), near(own, A, Y), near(Y, B, X), near(X, A, Y)] + [pair(o, p) for o in (own, X, Y, D) for p in (A, B)]:
            for cp in copies:
                cp.wait_send()
        pltpu.make_async_copy(y_acc, y_hbm, y_sem).wait()
        if with_tables:
            pltpu.make_async_copy(tab_hbm, T.at[slot_of(0)], own_sem).wait()


def block(h, w_in, b_in3, w_out, qk_gain, tables, layer, n_txt, nh, row0, collective_id, hc=512):
    total, d = h.shape
    n_dev = d // LANES // nh
    with_tables = tables.ndim == 3
    ff = w_in.shape[2] - 3 * d
    n = ff // hc
    m = total - row0
    rb = total - n_txt
    assert n_dev * n_txt == rb
    S = n_dev * total
    hbm = pl.BlockSpec(memory_space=pl.ANY)
    dma = pltpu.SemaphoreType.DMA
    bf, f32 = jnp.bfloat16, jnp.float32

    def at(i):
        return jnp.clip(i - (n + 1), 0, n_dev)

    t_shape = tables.shape if with_tables else tables.shape[1:]
    out_shape = [jax.ShapeDtypeStruct((m, d), f32), jax.ShapeDtypeStruct((n_dev, total, d), bf),
                 jax.ShapeDtypeStruct((nh, 2 * LANES, S), bf), jax.ShapeDtypeStruct((nh, S, LANES), bf), jax.ShapeDtypeStruct((nh, LANES, S), bf)]
    out_specs = [hbm, hbm, pl.BlockSpec((nh, 2 * LANES, rb), lambda i: (0, 0, at(i))), pl.BlockSpec((nh, rb, LANES), lambda i: (0, at(i), 0)),
                 pl.BlockSpec((nh, LANES, rb), lambda i: (0, 0, at(i)))]
    sems = [dma((2,)), dma((4,)), dma, dma((6,)), dma((6,)), dma((8,)), dma((8,))]
    if with_tables:
        out_shape.append(jax.ShapeDtypeStruct((n_dev, *tables.shape), f32))
        out_specs.append(hbm)
        sems += [dma((6,)), dma((6,)), dma((8,)), dma((8,)), dma]
    return pl.pallas_call(
        functools.partial(block_kernel, layer=layer, n=n, n_dev=n_dev, nh=nh, n_txt=n_txt, row0=row0, with_tables=with_tables, at_x=n // 2, at_xx=n),
        grid=(n + 1 + n_dev + 1,),
        in_specs=[
            whole((total, d), pipeline_mode=pl.Buffered(1)),
            pl.BlockSpec((1, d, hc), lambda i: (layer, 0, 3 * d // hc + jnp.minimum(i, n - 1))),
            pl.BlockSpec((1, 1, hc), lambda i: (layer, 0, 3 * d // hc + jnp.minimum(i, n - 1))),
            pl.BlockSpec((1, hc, d), lambda i: (layer, d // hc + jnp.clip(i - 1, 0, n - 1), 0)),
            pl.BlockSpec((1, 1, b_in3.shape[2]), lambda i: (layer, 0, 0)),
            pl.BlockSpec((1, 2, LANES), lambda i: (layer, 0, 0)),
            hbm, hbm, hbm,
        ],
        out_specs=out_specs,
        out_shape=out_shape,
        scratch_shapes=[
            pltpu.VMEM((m, d), f32), pltpu.VMEM((m, hc), bf), pltpu.VMEM((m, hc), bf), pltpu.VMEM((3 * nh * LANES, d), bf), pltpu.VMEM((2, d, LANES), bf),
            pltpu.VMEM((3 * nh * LANES, LANES), f32), pltpu.VMEM((2 * LANES, LANES), f32), pltpu.VMEM((2, rb, d), bf), pltpu.VMEM((2, *t_shape), f32),
        ] + sems,
        compiler_params=params(**talking(collective_id)),
        cost_estimate=pl.CostEstimate(flops=4 * m * d * ff + 6 * S * d * nh * LANES, bytes_accessed=4 * d * ff + 2 * S * d, transcendentals=m * ff),
        name='block',
    )(h, w_in, b_in3, w_out, b_in3, qk_gain, h, w_in, tables)


def attend_kernel(qT_hbm, k_hbm, vT_hbm, w_hbm, bo_ref, mods_ref, *refs, layer, qt, kc, ck, ne, n_dev, n_txt, row0, last):
    if last:
        wf_ref, bf_ref, x_hbm, y_hbm, vel_hbm, *refs = refs
        *refs, vel, vown_sem, vsend_sem, vrecv_sem = refs
    else:
        x_hbm, y_hbm, xo_hbm, ho_hbm, *refs = refs
        *refs, tbuf, t_rows, tsend_sem, trecv_sem, out_sem = refs
    (qT_ref, k_ref, vT_ref, s_scr, m_scr, part_scr, acc_scr, l_scr, obuf, o_rows, w_ring, lhs, y_acc, xbuf, h_ring,
     in_sem, send_sem, recv_sem, w_sem, res_sem) = refs
    nh, S, hd = k_ref.shape
    n_img = o_rows.shape[2]
    R, d = y_acc.shape
    nk = S // kc
    n_ring = w_ring.shape[0]
    nc = d // ck
    ahead = 2
    f32, bf = jnp.float32, jnp.bfloat16
    cfg, z, core = lax.axis_index('cfg'), lax.axis_index('z'), lax.axis_index('core')
    me = cfg * N_CORE + core

    def load(t):
        pairs = ((qT_hbm, qT_ref), (k_hbm, k_ref), (vT_hbm, vT_ref))
        return [pltpu.make_async_copy(src.at[t], dst.at[t], in_sem.at[t, j]) for j, (src, dst) in enumerate(pairs)]

    def w_copy(c):
        slot = lax.rem(c, n_ring)
        return pltpu.make_async_copy(w_hbm.at[layer, pl.ds(pl.multiple_of(c * ck, ck), ck), :], w_ring.at[slot], w_sem.at[slot])

    residual = [pltpu.make_async_copy(y_hbm, y_acc, res_sem.at[0]), pltpu.make_async_copy(x_hbm.at[pl.ds(row0, R), :], xbuf, res_sem.at[1])]

    def device(r):
        to, c = related(cfg, core, r)
        return to, z, c

    for cp in load(0):
        cp.start()
    peers = [device(r) for r in range(1, n_dev)]
    if last:
        peers += [(z, e, core) for e in range(ne)] + [(e, cfg, core) for e in range(ne)]
    meet(peers)
    for cp in load(0):
        cp.wait()
    for t in range(1, nh):
        for cp in load(t):
            cp.start()

    def score_chunk(head, q, slot, i, m):
        rows = pl.ds(i * kc, kc)
        k = k_ref[head, rows, :]
        s = dot(jnp.concatenate([k, k], axis=1), q)
        s_scr[slot, rows, :] = s
        return jnp.maximum(m, jnp.max(s.reshape(kc // 8, 8, qt), axis=0))

    def lowest():
        return jnp.full((8, qt), -jnp.inf, f32)

    def full_max(m):
        return jnp.broadcast_to(jnp.max(m, axis=0, keepdims=True), (8, qt))

    def prob_chunk(head, m, slot, i, l, acc):
        rows = pl.ds(i * kc, kc)
        p = jnp.exp2(s_scr[slot, rows, :].reshape(kc // 8, 8, qt) - m[None])
        l = l + jnp.sum(p, axis=0)
        return l, acc + dot(vT_ref[head, :, rows], p.reshape(kc, qt).astype(bf))

    def load_q(tile):
        head, col = tile
        return qT_ref[head, :, pl.ds(pl.multiple_of(col, qt), qt)]

    def normalized(acc, l):
        return (acc / jnp.sum(l, axis=0, keepdims=True)).T.astype(bf)

    def stream(n_pairs, tile, buf, after, before):
        first, second = tile(0), tile(1)
        q, m = load_q(first), lowest()
        for i in range(nk):
            m = score_chunk(first[0], q, 0, i, m)
        m_scr[...] = full_max(m)
        q, m = load_q(second), lowest()
        for i in range(ahead):
            m = score_chunk(second[0], q, 1, i, m)
        part_scr[...] = m
        acc_scr[...] = jnp.zeros_like(acc_scr)
        l_scr[...] = jnp.ones_like(l_scr)

        def put(p, half, o):
            buf[p, half * qt:(half + 1) * qt, :] = o

        def pair(p, carry):
            before(p)
            later = lax.rem(p + 1, n_pairs)
            tiles = [tile(2 * p), tile(2 * p + 1), tile(2 * later), tile(2 * later + 1)]
            m, top = part_scr[...], m_scr[...]
            put(lax.rem(p + n_pairs - 1, n_pairs), 1, normalized(acc_scr[...], l_scr[...]))
            for half in range(2):
                l, acc = jnp.zeros((8, qt), f32), jnp.zeros((hd, qt), f32)
                q1, q2 = load_q(tiles[half + 1]), load_q(tiles[half + 2])
                for i in range(nk):
                    j = i + ahead
                    if j < nk:
                        m = score_chunk(tiles[half + 1][0], q1, 1 - half, j, m)
                    else:
                        if j == nk:
                            following, m = full_max(m), lowest()
                        m = score_chunk(tiles[half + 2][0], q2, half, j - nk, m)
                    l, acc = prob_chunk(tiles[half][0], top, half, i, l, acc)
                top = following
                if half == 0:
                    put(p, 0, normalized(acc, l))
                else:
                    acc_scr[...] = acc
                    l_scr[...] = l
            part_scr[...] = m
            m_scr[...] = top

            @pl.when(p > 0)
            def _():
                after(p - 1)
            return carry

        lax.fori_loop(0, n_pairs, pair, 0)
        put(n_pairs - 1, 1, normalized(acc_scr[...], l_scr[...]))
        after(n_pairs - 1)

    if not last:
        n_text = n_dev * n_txt
        assert n_text == 2 * qt

        def txt_send(head):
            for owner in range(n_dev):
                part = pl.ds(owner * n_txt, n_txt)
                if owner == 0:
                    t_rows[me, head] = tbuf[head, part, :]
                else:
                    remote(tbuf.at[head, part, :], t_rows.at[me, head], tsend_sem, trecv_sem, device(owner)).start()

        def txt_head(p):
            @pl.when(p < nh - 1)
            def _():
                for cp in load(p + 1):
                    cp.wait()

        stream(nh, lambda u: (u // 2, n_dev * n_img + lax.rem(u, 2) * qt), tbuf, txt_send, txt_head)

    def relation_of(p):
        return lax.rem(p + 1, n_dev)

    def img_tile(u):
        p = u // 2
        return p // n_dev, relation_of(p) * n_img + lax.rem(u, 2) * qt

    def img_send(p):
        head, owner = p // n_dev, relation_of(p)

        @pl.when(owner == 0)
        def _():
            o_rows[me, head] = obuf[p]

        @pl.when(owner != 0)
        def _():
            remote(obuf.at[p], o_rows.at[me, head], send_sem, recv_sem.at[head], device(owner)).start()

    def img_before(p):
        if last:
            @pl.when((relation_of(p) == 0) & (p < nh * n_dev - 1))
            def _():
                for cp in load(p // n_dev + 1):
                    cp.wait()

        @pl.when(p == 2)
        def _():
            for c in range(n_ring):
                w_copy(c).start()
            for cp in residual:
                cp.start()

    stream(nh * n_dev, img_tile, obuf, img_send, img_before)

    for cp in residual:
        cp.wait()
    others = pl.ds(0, n_dev - 1)
    if not last:
        wait_for(t_rows.at[others], trecv_sem)
    per = nc // nh
    wide = ck // LANES

    def chunk_of_w(c, carry):
        head = c // per

        @pl.when(lax.rem(c, per) == 0)
        def _():
            wait_for(o_rows.at[others, head], recv_sem.at[head])
        for t in range(wide):
            src = lax.rem(c, per) * wide + t
            if not last:
                lhs[:n_txt, head_rows(t)] = t_rows[src, head]
            lhs[R - n_img:, head_rows(t)] = o_rows[src, head]
        w_copy(c).wait()
        y_acc[...] += dot(lhs[...], w_ring[lax.rem(c, n_ring)])

        @pl.when(c + n_ring < nc)
        def _():
            w_copy(c + n_ring).start()
        return carry

    lax.fori_loop(0, nc, chunk_of_w, 0)

    gate_row = 3 * layer + 2
    gate, shift, scale = (mods_ref[r:r + 1, :] for r in range(gate_row, gate_row + 3))
    bo = bo_ref[0].astype(f32)
    er = R // ne
    sub = 16 if er % 16 == 0 else 8

    def put_rows(e, slot):
        rows = pl.ds(pl.multiple_of(e * er, sub), er)
        pltpu.make_async_copy(xbuf.at[rows, :], xo_hbm.at[rows, :], out_sem.at[2]).start()
        pltpu.make_async_copy(h_ring.at[slot], ho_hbm.at[rows, :], out_sem.at[slot]).start()

    def deliver(e):
        own = (z == cfg) & (e == z)

        @pl.when(own)
        def _():
            pltpu.make_async_copy(vel.at[e], vel_hbm.at[cfg], vown_sem).start()

        @pl.when(jnp.logical_not(own))
        def _():
            remote(vel.at[e], vel_hbm.at[cfg], vsend_sem.at[e], vrecv_sem.at[cfg], (z, e, core)).start()

    def rows_out(e, carry):
        slot = lax.rem(e, 2)
        if not last:
            @pl.when(e >= 2)
            def _():
                wait_for(h_ring.at[slot], out_sem.at[slot])

        def chunk(c, carry):
            rs = pl.ds(pl.multiple_of(e * er + c * sub, sub), sub)
            xn = (xbuf[rs, :].astype(f32) + gate * (y_acc[rs, :] + bo)).astype(bf)
            h_ring[slot, pl.ds(pl.multiple_of(c * sub, sub), sub), :] = ln_mod(xn.astype(f32), shift, scale)
            if not last:
                xbuf[rs, :] = xn
            return carry

        lax.fori_loop(0, er // sub, chunk, 0, unroll=3 if (er // sub) % 3 == 0 else 2)
        if last:
            w = jnp.concatenate([wf_ref[...], jnp.zeros((LANES - wf_ref.shape[0], d), bf)], axis=0)
            v = lax.dot_general(h_ring[slot], w, (((1,), (1,)), ((), ())), preferred_element_type=f32)
            b = bf_ref[...].astype(f32)
            vel[e] = v + jnp.concatenate([b, jnp.zeros((1, LANES - b.shape[1]), f32)], axis=1)
            deliver(e)
        else:
            put_rows(e, slot)
        return carry

    lax.fori_loop(0, ne, rows_out, 0)

    wait_for(o_rows.at[others], send_sem)
    if last:
        for e in range(ne):
            own = (z == cfg) & (e == z)

            @pl.when(own)
            def _():
                wait_for(vel.at[e], vown_sem)

            @pl.when(jnp.logical_not(own))
            def _():
                wait_for(vel.at[e], vsend_sem.at[e])
                wait_for(vel_hbm.at[e], vrecv_sem.at[e])
    else:
        wait_for(t_rows.at[others], tsend_sem)
        wait_for(xbuf, out_sem.at[2])
        for slot in range(2):
            wait_for(h_ring.at[slot], out_sem.at[slot])


def largest(n, cap, unit):
    return max(c for c in range(unit, cap + 1, unit) if n % c == 0)


def attend(qT, k, vT, w_out, b_out3, mods, x, y_mlp, layer, n_dev, n_txt, row0, collective_id, final=None, ck=512, ne=4):
    nh, S, hd = k.shape
    R, d = y_mlp.shape
    n_img = S // n_dev - n_txt
    last = final is not None
    qt = n_img // 2
    dma = pltpu.SemaphoreType.DMA
    bf, f32 = jnp.bfloat16, jnp.float32
    hbm = pl.BlockSpec(memory_space=pl.ANY)
    stat = pltpu.VMEM((8, qt), f32)
    scratch = [pltpu.VMEM(v.shape, bf) for v in (qT, k, vT)] + [
        pltpu.VMEM((2, S, qt), f32), stat, stat, pltpu.VMEM((hd, qt), f32), stat, pltpu.VMEM((nh * n_dev, n_img, hd), bf), pltpu.VMEM((n_dev, nh, n_img, hd), bf),
        pltpu.VMEM((2, ck, d), bf), pltpu.VMEM((R, ck), bf), pltpu.VMEM((R, d), f32), pltpu.VMEM((R, d), bf), pltpu.VMEM((2, R // ne, d), bf),
        dma((nh, 3)), dma, dma((nh,)), dma((2,)), dma((2,))]
    if last:
        out_shape = jax.ShapeDtypeStruct((ne, R // ne, LANES), f32)
        scratch += [pltpu.VMEM(out_shape.shape, f32), dma, dma((ne,)), dma((ne,))]
    else:
        out_shape = [jax.ShapeDtypeStruct((R, d), bf)] * 2
        scratch += [pltpu.VMEM((nh, n_dev * n_txt, hd), bf), pltpu.VMEM((n_dev, nh, n_txt, hd), bf), dma, dma, dma((3,))]
    extra = list(final or ())
    return pl.pallas_call(
        functools.partial(attend_kernel, layer=layer, qt=qt, kc=largest(S, 768, 256), ck=ck, ne=ne, n_dev=n_dev, n_txt=n_txt, row0=row0, last=last),
        grid=(1,),
        in_specs=[hbm] * 4 + [pl.BlockSpec((1, 1, d), lambda i: (layer, 0, 0)), whole(mods.shape)] + [whole(v.shape) for v in extra] + [hbm] * 2,
        out_specs=hbm if last else [hbm] * 2,
        out_shape=out_shape,
        scratch_shapes=scratch,
        compiler_params=params(**talking(collective_id)),
        cost_estimate=pl.CostEstimate(flops=6 * nh * n_dev * R * S * hd + 2 * R * d * d, bytes_accessed=8 * nh * S * hd + 2 * d * d + 14 * R * d, transcendentals=nh * S * n_dev * R),
        name='attend',
    )(qT, k, vT, w_out, b_out3, mods, *extra, x, y_mlp)


def enter_kernel(xt_hbm, xi_hbm, cond_ref, wm_ref, wf_ref, bm_ref, bf_ref, cos_hbm, sin_hbm, mods_ref, xo_ref, ho_ref, tab_out,
                 stage, xbuf, cond_buf, s_scr,
                 cond_send, cond_recv, p_send, p_recv, c_send, c_recv, own_sem, t_send, t_recv, town_sem, *, n_mod, n_steps, per_row, per_layer):
    i = pl.program_id(0)
    n, rows, d = xbuf.shape
    tp = xt_hbm.shape[0] // n
    ip = xi_hbm.shape[0] // n
    cfg, z, core = lax.axis_index('cfg'), lax.axis_index('z'), lax.axis_index('core')
    across = [related(cfg, core, r)[0] for r in range(2, 2 * n, 2)]
    heights = [lax.rem(z + s, n) for s in range(1, n)]
    cut = rows // 2

    def piece_refs(j, dst):
        first = cut - tp
        head = [(xt_hbm.at[pl.ds(j * tp, tp), :], dst.at[pl.ds(0, tp), :]), (xi_hbm.at[pl.ds(j * ip, first), :], dst.at[pl.ds(tp, first), :])]
        return head, [(xi_hbm.at[pl.ds(j * ip + first, ip - first), :], dst.at[pl.ds(cut, ip - first), :])]

    def tables(to):
        half = cos_hbm.shape[0]
        cols = pl.ds(pl.multiple_of(cfg * ip, ip), ip)
        return [(src.at[:, cols], to.at[pl.ds(t * half, half), :]) for t, src in enumerate((cos_hbm, sin_hbm))]

    def forward(group, t, part):
        at = pl.ds(part * cut, cut)

        @pl.when(group == z)
        def _():
            xbuf[z, at, :] = stage[group, at, :]

        @pl.when(group != z)
        def _():
            remote(stage.at[group, at, :], xbuf.at[z, at, :], c_send.at[t], c_recv.at[z], (cfg, group, core)).start()

    def silu_of(ref):
        v = ref[...].astype(jnp.float32)
        s_scr[...] = jnp.broadcast_to((v * jax.nn.sigmoid(v)).astype(jnp.bfloat16), s_scr.shape)

    @pl.when(i == 0)
    def _():
        meet([(j, z, core) for j in across] + [(cfg, h, core) for h in heights])

        @pl.when(cfg == z)
        def _():
            for t, j in enumerate(across):
                remote(cond_ref, cond_buf, cond_send.at[t], cond_recv, (j, z, core)).start()
        for part in range(2):
            for t, j in ((0, across[0]), (2, across[2]), (1, across[1])):
                for src, dst in piece_refs(j, stage.at[cfg])[part]:
                    remote(src, dst, p_send.at[t], p_recv.at[cfg, part], (j, z, core)).start()
        mine = sum(piece_refs(cfg, xbuf.at[z]), [])

        @pl.when(cfg == z)
        def _():
            for src, dst in mine:
                pltpu.make_async_copy(src, dst, own_sem).start()

        @pl.when(cfg != z)
        def _():
            for src, dst in mine:
                remote(src, dst, c_send.at[n - 1], c_recv.at[z], (cfg, cfg, core)).start()
        for t, h in enumerate(heights):
            for src, dst in tables(tab_out.at[z]):
                remote(src, dst, t_send.at[t], t_recv.at[z], (cfg, h, core)).start()
        for src, dst in tables(tab_out.at[z]):
            pltpu.make_async_copy(src, dst, town_sem).start()

        @pl.when(cfg == z)
        def _():
            silu_of(cond_ref)

        @pl.when(cfg != z)
        def _():
            remote(cond_ref, cond_buf, cond_send.at[0], cond_recv, (cfg, z, core)).wait_recv()
            silu_of(cond_buf)

    row, col = i // per_row, lax.rem(i, per_row)
    width = wm_ref.shape[2]
    cols = pl.ds(pl.multiple_of(col * width, width), width)

    @pl.when(i < n_mod)
    def _():
        v = dot(s_scr[...], wm_ref[0])
        b = bm_ref[...].astype(jnp.float32)
        of_layer = lax.broadcasted_iota(jnp.int32, b.shape, 0) == i // per_layer
        mods_ref[pl.ds(row, 1), cols] = v[0:1] + jnp.sum(jnp.where(of_layer, b, 0.0), axis=0, keepdims=True)

    @pl.when(i >= n_mod)
    def _():
        v = dot(s_scr[...], wf_ref[...])
        mods_ref[pl.ds(row, 1), cols] = v[0:1] + bf_ref[...].astype(jnp.float32)

    def arrived(t, part):
        j = across[t]
        wait_for(stage.at[j, pl.ds(part * cut, cut), :], p_recv.at[j, part])
        forward(j, t, part)

    for at, landing in ((9, ((0, 0),)), (19, ((2, 0), (1, 0))), (25, ((0, 1), (1, 1))), (36, ((2, 1),))):
        @pl.when(i == at)
        def _():
            for t, part in landing:
                arrived(t, part)

    @pl.when(i == n_steps - 1)
    def _():
        shift, scale = mods_ref[0:1, :], mods_ref[1:2, :]

        @pl.when(cfg == z)
        def _():
            wait_for(xbuf.at[z], own_sem)

        def norm_rows(k, src, dst, count):
            sub = 16 if count % 16 == 0 else 8

            def chunk(c, carry):
                v = xbuf[k, pl.ds(pl.multiple_of(src + c * sub, sub), sub), :]
                to = pl.ds(pl.multiple_of(dst + c * sub, sub), sub)
                xo_ref[to, :] = v
                ho_ref[to, :] = ln_mod(v.astype(jnp.float32), shift, scale)
                return carry
            lax.fori_loop(0, count // sub, chunk, 0, unroll=min(4, count // sub))

        def height(s, carry):
            k = lax.rem(z + s, n)

            @pl.when(s > 0)
            def _():
                wait_for(xbuf.at[k], c_recv.at[k])
            norm_rows(k, 0, k * tp, tp)
            norm_rows(k, tp, n * tp + k * ip, ip)
            return carry

        lax.fori_loop(0, n, height, 0)

        for t, j in enumerate(across):
            wait_for(xbuf.at[0], p_send.at[t])

            @pl.when(j != z)
            def _():
                wait_for(xbuf.at[0], c_send.at[t])

        @pl.when(cfg != z)
        def _():
            wait_for(xbuf.at[0], c_send.at[n - 1])

        @pl.when(cfg == z)
        def _():
            for t, j in enumerate(across):
                remote(cond_ref, cond_buf, cond_send.at[t], cond_recv, (j, z, core)).wait_send()
        for t, h in enumerate(heights):
            wait_for(tab_out.at[z], t_send.at[t])
            wait_for(tab_out.at[h], t_recv.at[h])
        wait_for(tab_out.at[z], town_sem)


def enter(x_txt, x_img, cond, w_mod, w_fmod, b_mod, b_fmod, cosT, sinT, n, collective_id, width=512):
    n_txt, d = x_txt.shape
    n_img = x_img.shape[0]
    total = n_txt + n_img
    rows = total // n
    n_layers, _, dm = w_mod.shape
    per_layer, n_fin, per_row = dm // width, w_fmod.shape[1] // width, d // width
    n_mod = n_layers * per_layer
    steps = n_mod + n_fin
    dma = pltpu.SemaphoreType.DMA
    bf, f32 = jnp.bfloat16, jnp.float32

    def layer_of(i):
        j = jnp.minimum(i, n_mod - 1)
        return j // per_layer, lax.rem(j, per_layer)

    def last_of(i):
        return 0, jnp.maximum(i - n_mod, 0)

    hbm = pl.BlockSpec(memory_space=pl.ANY)
    out_shape = [jax.ShapeDtypeStruct((steps // per_row, d), f32), jax.ShapeDtypeStruct((total, d), bf), jax.ShapeDtypeStruct((total, d), bf),
                 jax.ShapeDtypeStruct((n, 2 * cosT.shape[0], n_img // n), f32)]
    return pl.pallas_call(
        functools.partial(enter_kernel, n_mod=n_mod, n_steps=steps, per_row=per_row, per_layer=per_layer),
        grid=(steps,),
        in_specs=[hbm, hbm, whole(cond.shape), pl.BlockSpec((1, d, width), lambda i: (layer_of(i)[0], 0, layer_of(i)[1])), pl.BlockSpec((d, width), last_of),
                  pl.BlockSpec((n_layers, width), lambda i: (0, layer_of(i)[1])), pl.BlockSpec((1, width), last_of), hbm, hbm],
        out_specs=[whole(v.shape) for v in out_shape[:-1]] + [hbm],
        out_shape=out_shape,
        scratch_shapes=[pltpu.VMEM((n, rows, d), bf), pltpu.VMEM((n, rows, d), bf), pltpu.VMEM(cond.shape, bf), pltpu.VMEM((16, d), bf),
                        dma((n - 1,)), dma, dma((n - 1,)), dma((n, 2)), dma((n,)), dma((n,)), dma, dma((n - 1,)), dma((n,)), dma],
        compiler_params=params(**talking(collective_id)),
        cost_estimate=pl.CostEstimate(flops=2 * 16 * d * width * steps, bytes_accessed=2 * d * width * steps, transcendentals=0),
        name='enter',
    )(x_txt, x_img, cond, w_mod, w_fmod, b_mod, b_fmod, cosT, sinT)


def solution(mesh):
    n_cfg = mesh.devices.shape[0]
    n_z = mesh.devices.shape[1] // N_CORE
    grid = Mesh(mesh.devices.reshape(n_cfg, n_z, N_CORE), ('cfg', 'z', 'core'))
    assert n_cfg == n_z == 4
    n_dev = n_cfg * N_CORE
    token_spec = P(('cfg', 'z', 'core'), None)
    seq_spec = P(('z', 'core'), None)
    in_specs = (token_spec, token_spec, P('cfg', None), seq_spec, seq_spec, token_spec) + (P(),) * 13

    def body(x_txt, x_img, cond_vec, cos_img, sin_img, z_lat, t_cur, t_next, w_mod, b_mod, w_in, b_in, qk_gain, w_out, b_out, w_fmod, b_fmod, w_final, b_final):
        n_txt, d = x_txt.shape
        n_img = x_img.shape[0]
        n_layers = w_mod.shape[0]
        nh = d // LANES // n_dev
        n_out = w_final.shape[1]

        mods, x, h, own = enter(x_txt, x_img, cond_vec, w_mod, w_fmod, b_mod, b_fmod[None], cos_img.T, sin_img.T, n_cfg, 1)
        b_in3, b_out3 = b_in[:, None, :], b_out[:, None, :]
        for l in range(n_layers):
            last = l == n_layers - 1
            row0 = n_txt if last else 0
            y_mlp, _, qT, k, vT, *more = block(h, w_in, b_in3, w_out, qk_gain, own, l, n_txt, nh, row0, 2 + 2 * l)
            own = more[0] if more else own
            final = (w_final.T, b_final[None]) if last else None
            done = attend(qT, k, vT, w_out, b_out3, mods, x, y_mlp, l, n_dev, n_txt, row0, 3 + 2 * l, final)
            if not last:
                x, h = done

        return z_lat + (t_next - t_cur) * done.reshape(n_img, LANES)[:, :n_out]

    return jax.shard_map(body, mesh=grid, in_specs=in_specs, out_specs=token_spec, check_vma=False)
```

```python
import functools
import math

import jax
import jax.numpy as jnp
from jax import lax
from jax.experimental import pallas as pl
from jax.experimental.pallas import tpu as pltpu
from jax.sharding import Mesh, PartitionSpec as P

EPS = 1e-6
LANES = 128
GELU_C = math.sqrt(2.0 / math.pi)
LOG2E = math.log2(math.e)
VMEM_BYTES = 60 * 2**20
N_CORE = 2
MESH = pl.DeviceIdType.MESH


def params(**kw):
    return pltpu.CompilerParams(vmem_limit_bytes=VMEM_BYTES, dimension_semantics=('arbitrary',), **kw)


def talking(collective_id):
    return dict(collective_id=collective_id, has_side_effects=True)


def whole(shape, **kw):
    return pl.BlockSpec(shape, lambda i: (0,) * len(shape), **kw)


def head_rows(j):
    return slice(j * LANES, (j + 1) * LANES)


def columns_of(v):
    return jnp.broadcast_to(v.astype(jnp.float32), (LANES, LANES)).T


def wait_for(ref, sem):
    pltpu.make_async_copy(ref, ref, sem).wait()


def dot(a, b):
    return jnp.dot(a, b, preferred_element_type=jnp.float32)


def remote(src, dst, send_sem, recv_sem, device):
    return pltpu.make_async_remote_copy(src_ref=src, dst_ref=dst, send_sem=send_sem, recv_sem=recv_sem, device_id=device, device_id_type=MESH)


def meet(devices):
    barrier = pltpu.get_barrier_semaphore()
    for device in devices:
        pl.semaphore_signal(barrier, inc=1, device_id=device, device_id_type=MESH)
    pl.semaphore_wait(barrier, len(devices))


def ln_mod(x, shift, scale):
    centered = x - jnp.mean(x, axis=-1, keepdims=True)
    var = jnp.mean(centered * centered, axis=-1, keepdims=True)
    return (centered * lax.rsqrt(var + EPS) * (1.0 + scale) + shift).astype(jnp.bfloat16)


def gelu_tanh(u):
    return u * (0.5 * (1.0 + jnp.tanh(GELU_C * (u + 0.044715 * (u * u * u)))))


def related(cfg, core, r):
    cx, cy = cfg // 2, lax.rem(cfg, 2)
    x = lax.rem(cx + lax.rem(r // 2, 2), 2)
    y = lax.rem(cy + r // 4, 2)
    return x * 2 + y, lax.rem(core + lax.rem(r, 2), 2)


def block_kernel(b_in_ref, gain_ref, h_hbm, w_in_hbm, w_out_hbm, T, y_hbm, H, qT_ref, k_ref, vT_ref, h_ref, w1_ring, w2_ring, y_acc, u_scr, act, wt, wbuf, bb, gg, hbuf, tbuf,
                 h_own_sem, w1_sem, w2_sem, w_sem, h_sem, t_sem, y_sem, near_send, near_recv, pair_send, pair_recv, *, layer, n, n_dev, nh, n_txt, row0, at_t, at_x):
    i = pl.program_id(0)
    cfg, z, core = lax.axis_index('cfg'), lax.axis_index('z'), lax.axis_index('core')
    rows = y_acc.shape[0]
    total, d = h_hbm.shape
    hc = u_scr.shape[1]
    rb = total - n_txt
    half = LANES // 2
    n_heads = d // LANES
    stride = n_heads // nh

    def device(r):
        to, c = related(cfg, core, r)
        return to, z, c

    def slot_of(r):
        to, c = related(cfg, core, r)
        return to * N_CORE + c

    own, X, Y, D = range(0, n_dev, 2)
    T_, A, B = range(3)
    spans = ((0, n_txt), (n_txt, rb // 2), (n_txt + rb // 2, rb // 2))
    hops = [(own, T_, X), (own, A, X), (own, B, X), (Y, B, X), (own, T_, Y), (own, B, Y), (own, A, Y), (X, T_, Y), (X, A, Y)]

    def at_core(origin, piece):
        return H.at[slot_of(origin), pl.ds(*spans[piece]), :]

    def move(origin, piece, to, send_sem, recv_sem):
        src = h_hbm.at[pl.ds(*spans[piece]), :] if origin == own else at_core(origin, piece)
        return remote(src, at_core(origin, piece), send_sem, recv_sem, device(to))

    def near(origin, piece, to):
        k = ((origin ^ to) // 2 - 1) * 3 + piece
        return move(origin, piece, to, near_send.at[hops.index((origin, piece, to))], near_recv.at[k])

    def pair(origin, piece):
        k = origin // 2 * 3 + piece
        return move(origin, piece, 1, pair_send.at[k], pair_recv.at[k])

    def landed_near(origin, piece):
        wait_for(at_core(origin, piece), near_recv.at[(origin // 2 - 1) * 3 + piece])

    def landed_pair(origin, *pieces):
        for piece in pieces:
            wait_for(at_core(origin + 1, piece), pair_recv.at[origin // 2 * 3 + piece])

    h_copy = pltpu.make_async_copy(h_hbm, h_ref, h_own_sem)

    def w1_copy(j):
        cols = pl.ds(pl.multiple_of(3 * d + j * hc, hc), hc)
        return pltpu.make_async_copy(w_in_hbm.at[layer, :, cols], w1_ring.at[lax.rem(j, 2)], w1_sem.at[lax.rem(j, 2)])

    def w2_copy(j):
        at = pl.ds(pl.multiple_of(d + j * hc, hc), hc)
        return pltpu.make_async_copy(w_out_hbm.at[layer, at, :], w2_ring.at[lax.rem(j, 2)], w2_sem.at[lax.rem(j, 2)])

    def w_cols(j):
        col = (j // nh * n_heads + lax.rem(j, nh) * stride + cfg * N_CORE + core) * LANES
        return pl.ds(pl.multiple_of(col, LANES), LANES)

    def w_copy(j):
        return pltpu.make_async_copy(w_in_hbm.at[layer, :, w_cols(j)], wbuf.at[lax.rem(j, 2)], w_sem.at[lax.rem(j, 2)])

    def w_turn(j):
        w_copy(j).wait()
        to = pl.ds(pl.multiple_of(j * LANES, LANES), LANES)
        wt[to, :] = wbuf[lax.rem(j, 2)].T
        bb[to, :] = columns_of(b_in_ref[0, :, w_cols(j)])

    def fetch(r, slot):
        pltpu.make_async_copy(T.at[slot_of(r)], tbuf.at[slot], t_sem.at[slot]).start()

        @pl.when(r == 0)
        def _():
            pltpu.make_async_copy(h_hbm.at[pl.ds(n_txt, rb), :], hbuf.at[slot], h_sem.at[slot]).start()

        @pl.when(r > 0)
        def _():
            pltpu.make_async_copy(H.at[slot_of(r), pl.ds(n_txt, rb), :], hbuf.at[slot], h_sem.at[slot]).start()

    def fetch_text(slot):
        for r in range(n_dev):
            src = at_core(r, T_) if r else h_hbm.at[pl.ds(0, n_txt), :]
            pltpu.make_async_copy(src, hbuf.at[slot, pl.ds(r * n_txt, n_txt), :], h_sem.at[slot]).start()

    sub = 2
    step = rows // sub

    def at_rows(r, first=0):
        return pl.ds(pl.multiple_of(first + r * step, 16), step)

    def each(part, rolled):
        if rolled:
            lax.fori_loop(0, sub, lambda r, carry: part(r) or carry, 0)
        else:
            for r in range(sub):
                part(r)

    def up(rolled=False):
        b1 = b_in_ref[0, :, pl.ds(pl.multiple_of(3 * d + i * hc, hc), hc)].astype(jnp.float32)

        def part(r):
            u = dot(h_ref[at_rows(r, row0), :], w1_ring[lax.rem(i, 2)])
            u_scr[at_rows(r), :] = (u + b1).astype(jnp.bfloat16)

        each(part, rolled)

    def gelu():
        act[...] = gelu_tanh(u_scr[...].astype(jnp.float32)).astype(jnp.bfloat16)

    def down(rolled=False):
        def part(r):
            y_acc[at_rows(r), :] += dot(act[at_rows(r), :], w2_ring[lax.rem(i + 1, 2)])

        each(part, rolled)

    @pl.when(i == 0)
    def _():
        w1_copy(0).start()
        h_copy.start()
        meet([device(1), device(X), device(Y)])
        for piece in (T_, A):
            near(own, piece, X).start()
        for piece in (T_, B):
            near(own, piece, Y).start()
        for piece in (T_, A, B):
            pair(own, piece).start()
        w1_copy(1).start()
        w2_copy(0).start()
        w_copy(0).start()
        w_copy(1).start()
        for j in range(2):
            gg[head_rows(j), :] = columns_of(gain_ref[0, j:j + 1, :])
        y_acc[...] = jnp.zeros_like(y_acc)
        h_copy.wait()
        w1_copy(i).wait()
        up(True)

    @pl.when((i > 0) & (i < n))
    def _():
        @pl.when(i + 1 < n)
        def _():
            w1_copy(i + 1).start()
        w2_copy(i).start()
        w2_copy(i - 1).wait()
        w1_copy(i).wait()
        gelu()
        up()
        down()

    @pl.when(i == n)
    def _():
        w2_copy(i - 1).wait()
        gelu()
        down(True)

    @pl.when((i > 0) & (i <= 3 * nh))
    def _():
        w_turn(i - 1)

        @pl.when(i + 1 < 3 * nh)
        def _():
            w_copy(i + 1).start()

    @pl.when(i == at_t)
    def _():
        landed_near(X, T_)
        near(X, T_, Y).start()
        near(own, A, Y).start()
        near(own, B, X).start()
        pair(X, T_).start()
        landed_near(Y, T_)
        pair(Y, T_).start()

    @pl.when(i == at_x)
    def _():
        landed_near(X, A)
        near(X, A, Y).start()
        pair(X, A).start()
        landed_near(Y, B)
        near(Y, B, X).start()
        pair(Y, B).start()
        landed_near(D, T_)
        pair(D, T_).start()
        landed_pair(own, T_, A, B)

    s = i - (n + 1)
    slot = lax.rem(i, 2)

    @pl.when(i == n)
    def _():
        landed_near(X, B)
        pair(X, B).start()
        landed_near(Y, A)
        pair(Y, A).start()
        landed_pair(X, T_, A)
        landed_pair(Y, T_, B)
        fetch(0, 1 - slot)

    @pl.when(s == 0)
    def _():
        pltpu.make_async_copy(y_acc, y_hbm, y_sem).start()

    @pl.when(s == X)
    def _():
        landed_pair(X, B)
        landed_pair(Y, A)

    @pl.when((s >= 0) & (s < D - 1))
    def _():
        fetch(s + 1, 1 - slot)

    @pl.when(s == D - 1)
    def _():
        landed_pair(D, T_)
        fetch_text(1 - slot)

    @pl.when(s == D + 1)
    def _():
        landed_near(D, A)
        pair(D, A).start()
        landed_near(D, B)
        pair(D, B).start()
        fetch(D, slot)

    @pl.when(s == n_dev)
    def _():
        landed_pair(D, A, B)
        fetch(D + 1, slot)

    @pl.when(s >= 0)
    def _():
        image = s != D
        wait_for(hbuf.at[slot], h_sem.at[slot])

        @pl.when(image)
        def _():
            wait_for(tbuf.at[slot], t_sem.at[slot])
        h = hbuf[slot]
        table = jnp.concatenate([tbuf[slot, t] for t in range(tbuf.shape[1])], axis=1)
        cos, sin = jnp.where(image, table[:half], 1.0), jnp.where(image, table[half:], 0.0)

        def lanes(v):
            return jnp.concatenate([v] * (rb // LANES), axis=1)

        def proj(part):
            rs = slice(part * nh * LANES, (part + 1) * nh * LANES)
            return lax.dot_general(wt[rs, :], h, (((1,), (1,)), ((), ())), preferred_element_type=jnp.float32)

        def biased(x, j):
            return (x + lanes(bb[head_rows(j), :])).astype(jnp.bfloat16)

        def normed(x, j, g):
            x = biased(x, j).astype(jnp.float32)
            ms = jnp.sum(x * x, axis=0, keepdims=True) * (1.0 / LANES)
            v = x * lax.rsqrt(ms + EPS) * lanes(gg[head_rows(g), :])
            a, b = v[:half], v[half:]
            return jnp.concatenate([a * cos - b * sin, a * sin + b * cos], axis=0).astype(jnp.bfloat16)

        q = proj(0)
        for t in range(nh):
            v = normed(q[head_rows(t)], t, 0).astype(jnp.float32) * (LANES ** -0.5 * LOG2E)
            hi = v.astype(jnp.bfloat16)
            qT_ref[t, :LANES] = hi
            qT_ref[t, LANES:] = (v - hi.astype(jnp.float32)).astype(jnp.bfloat16)
        k = proj(1)
        for t in range(nh):
            k_ref[t] = normed(k[head_rows(t)], nh + t, 1).T
        v = proj(2)
        for t in range(nh):
            vT_ref[t] = biased(v[head_rows(t)], 2 * nh + t)

    @pl.when(s == n_dev)
    def _():
        for hop in hops:
            near(*hop).wait_send()
        for origin in (own, X, Y, D):
            for piece in (T_, A, B):
                pair(origin, piece).wait_send()
        wait_for(y_acc, y_sem)


def block(h, w_in, b_in3, w_out, qk_gain, tables, layer, n_txt, nh, row0, collective_id, hc=512):
    total, d = h.shape
    n_dev = d // LANES // nh
    ff = w_in.shape[2] - 3 * d
    n = ff // hc
    m = total - row0
    rb = total - n_txt
    assert n_dev * n_txt == rb
    S = n_dev * total
    hbm = pl.BlockSpec(memory_space=pl.ANY)
    dma = pltpu.SemaphoreType.DMA
    bf, f32 = jnp.bfloat16, jnp.float32
    far = n_dev - 2

    def at(i):
        s = jnp.clip(i - (n + 1), 0, n_dev)
        return s + 2 * (s // far) - 3 * (s // (far + 1))

    three = pltpu.SemaphoreType.DMA((12,))
    return pl.pallas_call(
        functools.partial(block_kernel, layer=layer, n=n, n_dev=n_dev, nh=nh, n_txt=n_txt, row0=row0, at_t=n // 4, at_x=n // 2),
        grid=(n + 1 + n_dev + 1,),
        in_specs=[pl.BlockSpec((1, 1, b_in3.shape[2]), lambda i: (layer, 0, 0)), pl.BlockSpec((1, 2, LANES), lambda i: (layer, 0, 0)), hbm, hbm, hbm, hbm],
        out_specs=[hbm, hbm, pl.BlockSpec((nh, 2 * LANES, rb), lambda i: (0, 0, at(i))), pl.BlockSpec((nh, rb, LANES), lambda i: (0, at(i), 0)),
                   pl.BlockSpec((nh, LANES, rb), lambda i: (0, 0, at(i)))],
        out_shape=[jax.ShapeDtypeStruct((m, d), f32), jax.ShapeDtypeStruct((n_dev, total, d), bf),
                   jax.ShapeDtypeStruct((nh, 2 * LANES, S), bf), jax.ShapeDtypeStruct((nh, S, LANES), bf), jax.ShapeDtypeStruct((nh, LANES, S), bf)],
        scratch_shapes=[
            pltpu.VMEM((total, d), bf), pltpu.VMEM((2, d, hc), bf), pltpu.VMEM((2, hc, d), bf),
            pltpu.VMEM((m, d), f32), pltpu.VMEM((m, hc), bf), pltpu.VMEM((m, hc), bf), pltpu.VMEM((3 * nh * LANES, d), bf), pltpu.VMEM((2, d, LANES), bf),
            pltpu.VMEM((3 * nh * LANES, LANES), f32), pltpu.VMEM((2 * LANES, LANES), f32), pltpu.VMEM((2, rb, d), bf), pltpu.VMEM((2, *tables.shape[1:]), f32),
            dma, dma((2,)), dma((2,)), dma((2,)), dma((2,)), dma((2,)), dma, dma((9,)), dma((9,)), three, three,
        ],
        compiler_params=params(**talking(collective_id)),
        cost_estimate=pl.CostEstimate(flops=4 * m * d * ff + 6 * S * d * nh * LANES, bytes_accessed=4 * d * ff + 2 * S * d, transcendentals=m * ff),
        name='block',
    )(b_in3, qk_gain, h, w_in, w_out, tables)


def attend_kernel(qT_hbm, k_hbm, vT_hbm, w_hbm, bo_ref, mods_ref, *refs, layer, qt, kc, ck, ne, n_dev, n_txt, row0, last):
    if last:
        wf_ref, bf_ref, x_hbm, y_hbm, vel_hbm, *refs = refs
        *refs, vel, vown_sem, vsend_sem, vrecv_sem = refs
    else:
        x_hbm, y_hbm, xo_hbm, ho_hbm, *refs = refs
        *refs, tbuf, t_rows, tsend_sem, trecv_sem, out_sem = refs
    (qT_ref, k_ref, vT_ref, s_scr, m_scr, part_scr, acc_scr, l_scr, obuf, o_rows, w_ring, lhs, y_acc, xbuf, h_ring,
     in_sem, send_sem, recv_sem, w_sem, res_sem) = refs
    nh, S, hd = k_ref.shape
    n_img = o_rows.shape[2]
    R, d = y_acc.shape
    nk = S // kc
    n_ring = w_ring.shape[0]
    nc = d // ck
    ahead = 2
    f32, bf = jnp.float32, jnp.bfloat16
    cfg, z, core = lax.axis_index('cfg'), lax.axis_index('z'), lax.axis_index('core')
    me = cfg * N_CORE + core

    def load(t):
        pairs = ((qT_hbm, qT_ref), (k_hbm, k_ref), (vT_hbm, vT_ref))
        return [pltpu.make_async_copy(src.at[t], dst.at[t], in_sem.at[t, j]) for j, (src, dst) in enumerate(pairs)]

    def w_copy(c):
        slot = lax.rem(c, n_ring)
        return pltpu.make_async_copy(w_hbm.at[layer, pl.ds(pl.multiple_of(c * ck, ck), ck), :], w_ring.at[slot], w_sem.at[slot])

    residual = [pltpu.make_async_copy(y_hbm, y_acc, res_sem.at[0]), pltpu.make_async_copy(x_hbm.at[pl.ds(row0, R), :], xbuf, res_sem.at[1])]

    def device(r):
        to, c = related(cfg, core, r)
        return to, z, c

    for cp in load(0):
        cp.start()
    peers = [device(r) for r in range(1, n_dev)]
    if last:
        peers += [(z, e, core) for e in range(ne)] + [(e, cfg, core) for e in range(ne)]
    meet(peers)
    for cp in load(0):
        cp.wait()
    for t in range(1, nh):
        for cp in load(t):
            cp.start()

    def score_chunk(head, q, slot, i, m):
        rows = pl.ds(i * kc, kc)
        k = k_ref[head, rows, :]
        s = dot(jnp.concatenate([k, k], axis=1), q)
        s_scr[slot, rows, :] = s
        return jnp.maximum(m, jnp.max(s.reshape(kc // 8, 8, qt), axis=0))

    def lowest():
        return jnp.full((8, qt), -jnp.inf, f32)

    def full_max(m):
        return jnp.broadcast_to(jnp.max(m, axis=0, keepdims=True), (8, qt))

    def prob_chunk(head, m, slot, i, l, acc):
        rows = pl.ds(i * kc, kc)
        p = jnp.exp2(s_scr[slot, rows, :].reshape(kc // 8, 8, qt) - m[None])
        l = l + jnp.sum(p, axis=0)
        return l, acc + dot(vT_ref[head, :, rows], p.reshape(kc, qt).astype(bf))

    def load_q(tile):
        head, col = tile
        return qT_ref[head, :, pl.ds(pl.multiple_of(col, qt), qt)]

    def normalized(acc, l):
        return (acc / jnp.sum(l, axis=0, keepdims=True)).T.astype(bf)

    def stream(n_pairs, tile, buf, after, before):
        first, second = tile(0), tile(1)
        q, m = load_q(first), lowest()
        for i in range(nk):
            m = score_chunk(first[0], q, 0, i, m)
        m_scr[...] = full_max(m)
        q, m = load_q(second), lowest()
        for i in range(ahead):
            m = score_chunk(second[0], q, 1, i, m)
        part_scr[...] = m
        acc_scr[...] = jnp.zeros_like(acc_scr)
        l_scr[...] = jnp.ones_like(l_scr)

        def put(p, half, o):
            buf[p, half * qt:(half + 1) * qt, :] = o

        def pair(p, carry):
            before(p)
            later = lax.rem(p + 1, n_pairs)
            tiles = [tile(2 * p), tile(2 * p + 1), tile(2 * later), tile(2 * later + 1)]
            m, top = part_scr[...], m_scr[...]
            put(lax.rem(p + n_pairs - 1, n_pairs), 1, normalized(acc_scr[...], l_scr[...]))
            for half in range(2):
                l, acc = jnp.zeros((8, qt), f32), jnp.zeros((hd, qt), f32)
                q1, q2 = load_q(tiles[half + 1]), load_q(tiles[half + 2])
                for i in range(nk):
                    j = i + ahead
                    if j < nk:
                        m = score_chunk(tiles[half + 1][0], q1, 1 - half, j, m)
                    else:
                        if j == nk:
                            following, m = full_max(m), lowest()
                        m = score_chunk(tiles[half + 2][0], q2, half, j - nk, m)
                    l, acc = prob_chunk(tiles[half][0], top, half, i, l, acc)
                top = following
                if half == 0:
                    put(p, 0, normalized(acc, l))
                else:
                    acc_scr[...] = acc
                    l_scr[...] = l
            part_scr[...] = m
            m_scr[...] = top

            @pl.when(p > 0)
            def _():
                after(p - 1)
            return carry

        lax.fori_loop(0, n_pairs, pair, 0)
        put(n_pairs - 1, 1, normalized(acc_scr[...], l_scr[...]))
        after(n_pairs - 1)

    if not last:
        n_text = n_dev * n_txt
        assert n_text == 2 * qt

        def txt_send(head):
            for owner in range(n_dev):
                part = pl.ds(owner * n_txt, n_txt)
                if owner == 0:
                    t_rows[me, head] = tbuf[head, part, :]
                else:
                    remote(tbuf.at[head, part, :], t_rows.at[me, head], tsend_sem, trecv_sem, device(owner)).start()

        def txt_head(p):
            @pl.when(p < nh - 1)
            def _():
                for cp in load(p + 1):
                    cp.wait()

        stream(nh, lambda u: (u // 2, n_dev * n_img + lax.rem(u, 2) * qt), tbuf, txt_send, txt_head)

    def relation_of(p):
        return lax.rem(p + 1, n_dev)

    def img_tile(u):
        p = u // 2
        return p // n_dev, relation_of(p) * n_img + lax.rem(u, 2) * qt

    def img_send(p):
        head, owner = p // n_dev, relation_of(p)

        @pl.when(owner == 0)
        def _():
            o_rows[me, head] = obuf[p]

        @pl.when(owner != 0)
        def _():
            remote(obuf.at[p], o_rows.at[me, head], send_sem, recv_sem.at[head], device(owner)).start()

    def img_before(p):
        if last:
            @pl.when((relation_of(p) == 0) & (p < nh * n_dev - 1))
            def _():
                for cp in load(p // n_dev + 1):
                    cp.wait()

        @pl.when(p == 2)
        def _():
            for c in range(n_ring):
                w_copy(c).start()
            for cp in residual:
                cp.start()

    stream(nh * n_dev, img_tile, obuf, img_send, img_before)

    for cp in residual:
        cp.wait()
    others = pl.ds(0, n_dev - 1)
    if not last:
        wait_for(t_rows.at[others], trecv_sem)
    per = nc // nh
    wide = ck // LANES

    def chunk_of_w(c, carry):
        head = c // per

        @pl.when(lax.rem(c, per) == 0)
        def _():
            wait_for(o_rows.at[others, head], recv_sem.at[head])
        for t in range(wide):
            src = lax.rem(c, per) * wide + t
            if not last:
                lhs[:n_txt, head_rows(t)] = t_rows[src, head]
            lhs[R - n_img:, head_rows(t)] = o_rows[src, head]
        w_copy(c).wait()
        y_acc[...] += dot(lhs[...], w_ring[lax.rem(c, n_ring)])

        @pl.when(c + n_ring < nc)
        def _():
            w_copy(c + n_ring).start()
        return carry

    lax.fori_loop(0, nc, chunk_of_w, 0)

    gate_row = 3 * layer + 2
    gate, shift, scale = (mods_ref[r:r + 1, :] for r in range(gate_row, gate_row + 3))
    bo = bo_ref[0].astype(f32)
    er = R // ne
    sub = 16 if er % 16 == 0 else 8

    def put_rows(e, slot):
        rows = pl.ds(pl.multiple_of(e * er, sub), er)
        pltpu.make_async_copy(xbuf.at[rows, :], xo_hbm.at[rows, :], out_sem.at[2]).start()
        pltpu.make_async_copy(h_ring.at[slot], ho_hbm.at[rows, :], out_sem.at[slot]).start()

    def deliver(e):
        own = (z == cfg) & (e == z)

        @pl.when(own)
        def _():
            pltpu.make_async_copy(vel.at[e], vel_hbm.at[cfg], vown_sem).start()

        @pl.when(jnp.logical_not(own))
        def _():
            remote(vel.at[e], vel_hbm.at[cfg], vsend_sem.at[e], vrecv_sem.at[cfg], (z, e, core)).start()

    def rows_out(e, carry):
        slot = lax.rem(e, 2)
        if not last:
            @pl.when(e >= 2)
            def _():
                wait_for(h_ring.at[slot], out_sem.at[slot])

        def chunk(c, carry):
            rs = pl.ds(pl.multiple_of(e * er + c * sub, sub), sub)
            xn = (xbuf[rs, :].astype(f32) + gate * (y_acc[rs, :] + bo)).astype(bf)
            h_ring[slot, pl.ds(pl.multiple_of(c * sub, sub), sub), :] = ln_mod(xn.astype(f32), shift, scale)
            if not last:
                xbuf[rs, :] = xn
            return carry

        lax.fori_loop(0, er // sub, chunk, 0, unroll=3 if (er // sub) % 3 == 0 else 2)
        if last:
            w = jnp.concatenate([wf_ref[...], jnp.zeros((LANES - wf_ref.shape[0], d), bf)], axis=0)
            v = lax.dot_general(h_ring[slot], w, (((1,), (1,)), ((), ())), preferred_element_type=f32)
            b = bf_ref[...].astype(f32)
            vel[e] = v + jnp.concatenate([b, jnp.zeros((1, LANES - b.shape[1]), f32)], axis=1)
            deliver(e)
        else:
            put_rows(e, slot)
        return carry

    lax.fori_loop(0, ne, rows_out, 0)

    wait_for(o_rows.at[others], send_sem)
    if last:
        for e in range(ne):
            own = (z == cfg) & (e == z)

            @pl.when(own)
            def _():
                wait_for(vel.at[e], vown_sem)

            @pl.when(jnp.logical_not(own))
            def _():
                wait_for(vel.at[e], vsend_sem.at[e])
                wait_for(vel_hbm.at[e], vrecv_sem.at[e])
    else:
        wait_for(t_rows.at[others], tsend_sem)
        wait_for(xbuf, out_sem.at[2])
        for slot in range(2):
            wait_for(h_ring.at[slot], out_sem.at[slot])


def largest(n, cap, unit):
    return max(c for c in range(unit, cap + 1, unit) if n % c == 0)


def attend(qT, k, vT, w_out, b_out3, mods, x, y_mlp, layer, n_dev, n_txt, row0, collective_id, final=None, ck=512, ne=4):
    nh, S, hd = k.shape
    R, d = y_mlp.shape
    n_img = S // n_dev - n_txt
    last = final is not None
    qt = n_img // 2
    dma = pltpu.SemaphoreType.DMA
    bf, f32 = jnp.bfloat16, jnp.float32
    hbm = pl.BlockSpec(memory_space=pl.ANY)
    stat = pltpu.VMEM((8, qt), f32)
    scratch = [pltpu.VMEM(v.shape, bf) for v in (qT, k, vT)] + [
        pltpu.VMEM((2, S, qt), f32), stat, stat, pltpu.VMEM((hd, qt), f32), stat, pltpu.VMEM((nh * n_dev, n_img, hd), bf), pltpu.VMEM((n_dev, nh, n_img, hd), bf),
        pltpu.VMEM((2, ck, d), bf), pltpu.VMEM((R, ck), bf), pltpu.VMEM((R, d), f32), pltpu.VMEM((R, d), bf), pltpu.VMEM((2, R // ne, d), bf),
        dma((nh, 3)), dma, dma((nh,)), dma((2,)), dma((2,))]
    if last:
        out_shape = jax.ShapeDtypeStruct((ne, R // ne, LANES), f32)
        scratch += [pltpu.VMEM(out_shape.shape, f32), dma, dma((ne,)), dma((ne,))]
    else:
        out_shape = [jax.ShapeDtypeStruct((R, d), bf)] * 2
        scratch += [pltpu.VMEM((nh, n_dev * n_txt, hd), bf), pltpu.VMEM((n_dev, nh, n_txt, hd), bf), dma, dma, dma((3,))]
    extra = list(final or ())
    return pl.pallas_call(
        functools.partial(attend_kernel, layer=layer, qt=qt, kc=largest(S, 768, 256), ck=ck, ne=ne, n_dev=n_dev, n_txt=n_txt, row0=row0, last=last),
        grid=(1,),
        in_specs=[hbm] * 4 + [pl.BlockSpec((1, 1, d), lambda i: (layer, 0, 0)), whole(mods.shape)] + [whole(v.shape) for v in extra] + [hbm] * 2,
        out_specs=hbm if last else [hbm] * 2,
        out_shape=out_shape,
        scratch_shapes=scratch,
        compiler_params=params(**talking(collective_id)),
        cost_estimate=pl.CostEstimate(flops=6 * nh * n_dev * R * S * hd + 2 * R * d * d, bytes_accessed=8 * nh * S * hd + 2 * d * d + 14 * R * d, transcendentals=nh * S * n_dev * R),
        name='attend',
    )(qT, k, vT, w_out, b_out3, mods, *extra, x, y_mlp)


def enter_kernel(xt_hbm, xi_hbm, cond_ref, wm_ref, wf_ref, bm_ref, bf_ref, cos_hbm, sin_hbm, mods_ref, xo_ref, ho_ref, tab_out,
                 stage, xbuf, cond_buf, s_scr,
                 cond_send, cond_recv, p_send, p_recv, c_send, c_recv, own_sem, t_send, t_recv, town_sem, q_send, q_recv, *, n_mod, n_steps, per_row, per_layer):
    i = pl.program_id(0)
    n, rows, d = xbuf.shape
    tp = xt_hbm.shape[0] // n
    ip = xi_hbm.shape[0] // n
    cfg, z, core = lax.axis_index('cfg'), lax.axis_index('z'), lax.axis_index('core')
    across = [related(cfg, core, r)[0] for r in range(2, 2 * n, 2)]
    heights = [lax.rem(z + s, n) for s in range(1, n)]
    plane = [(to, z, c) for to, c in (related(cfg, core, r) for r in range(1, 2 * n))]
    mine = tab_out.at[cfg * N_CORE + core]
    cut = rows // 2

    def piece_refs(j, dst):
        first = cut - tp
        head = [(xt_hbm.at[pl.ds(j * tp, tp), :], dst.at[pl.ds(0, tp), :]), (xi_hbm.at[pl.ds(j * ip, first), :], dst.at[pl.ds(tp, first), :])]
        return head, [(xi_hbm.at[pl.ds(j * ip + first, ip - first), :], dst.at[pl.ds(cut, ip - first), :])]

    def tables(to):
        half = cos_hbm.shape[0]
        cols = pl.ds(pl.multiple_of(cfg * ip, ip), ip)
        return [(src.at[:, cols], to.at[pl.ds(t * half, half), :]) for t, src in enumerate((cos_hbm, sin_hbm))]

    def forward(group, t, part):
        at = pl.ds(part * cut, cut)

        @pl.when(group == z)
        def _():
            xbuf[z, at, :] = stage[group, at, :]

        @pl.when(group != z)
        def _():
            remote(stage.at[group, at, :], xbuf.at[z, at, :], c_send.at[t], c_recv.at[z], (cfg, group, core)).start()

    def silu_of(ref):
        v = ref[...].astype(jnp.float32)
        s_scr[...] = jnp.broadcast_to((v * jax.nn.sigmoid(v)).astype(jnp.bfloat16), s_scr.shape)

    @pl.when(i == 0)
    def _():
        meet(plane + [(cfg, h, core) for h in heights])

        @pl.when(cfg == z)
        def _():
            for t, j in enumerate(across):
                remote(cond_ref, cond_buf, cond_send.at[t], cond_recv, (j, z, core)).start()
        for part in range(2):
            for t, j in ((0, across[0]), (2, across[2]), (1, across[1])):
                for src, dst in piece_refs(j, stage.at[cfg])[part]:
                    remote(src, dst, p_send.at[t], p_recv.at[cfg, part], (j, z, core)).start()
        held = sum(piece_refs(cfg, xbuf.at[z]), [])

        @pl.when(cfg == z)
        def _():
            for src, dst in held:
                pltpu.make_async_copy(src, dst, own_sem).start()

        @pl.when(cfg != z)
        def _():
            for src, dst in held:
                remote(src, dst, c_send.at[n - 1], c_recv.at[z], (cfg, cfg, core)).start()
        for t, h in enumerate(heights):
            for src, dst in tables(mine.at[z]):
                remote(src, dst, t_send.at[t], t_recv.at[z], (cfg, h, core)).start()
        for src, dst in tables(mine.at[z]):
            pltpu.make_async_copy(src, dst, town_sem).start()

        @pl.when(cfg == z)
        def _():
            silu_of(cond_ref)

        @pl.when(cfg != z)
        def _():
            remote(cond_ref, cond_buf, cond_send.at[0], cond_recv, (cfg, z, core)).wait_recv()
            silu_of(cond_buf)

    row, col = i // per_row, lax.rem(i, per_row)
    width = wm_ref.shape[2]
    cols = pl.ds(pl.multiple_of(col * width, width), width)

    @pl.when(i < n_mod)
    def _():
        v = dot(s_scr[...], wm_ref[0])
        b = bm_ref[...].astype(jnp.float32)
        of_layer = lax.broadcasted_iota(jnp.int32, b.shape, 0) == i // per_layer
        mods_ref[pl.ds(row, 1), cols] = v[0:1] + jnp.sum(jnp.where(of_layer, b, 0.0), axis=0, keepdims=True)

    @pl.when(i >= n_mod)
    def _():
        v = dot(s_scr[...], wf_ref[...])
        mods_ref[pl.ds(row, 1), cols] = v[0:1] + bf_ref[...].astype(jnp.float32)

    def arrived(t, part):
        j = across[t]
        wait_for(stage.at[j, pl.ds(part * cut, cut), :], p_recv.at[j, part])
        forward(j, t, part)

    @pl.when(i == 42)
    def _():
        for h in heights:
            wait_for(mine.at[h], t_recv.at[h])
        wait_for(mine.at[z], town_sem)
        for peer in plane:
            remote(mine, mine, q_send, q_recv, peer).start()

    for at, landing in ((9, ((0, 0),)), (19, ((2, 0), (1, 0))), (25, ((0, 1), (1, 1))), (36, ((2, 1),))):
        @pl.when(i == at)
        def _():
            for t, part in landing:
                arrived(t, part)

    @pl.when(i == n_steps - 1)
    def _():
        shift, scale = mods_ref[0:1, :], mods_ref[1:2, :]

        @pl.when(cfg == z)
        def _():
            wait_for(xbuf.at[z], own_sem)

        def norm_rows(k, src, dst, count):
            sub = 16 if count % 16 == 0 else 8

            def chunk(c, carry):
                v = xbuf[k, pl.ds(pl.multiple_of(src + c * sub, sub), sub), :]
                to = pl.ds(pl.multiple_of(dst + c * sub, sub), sub)
                xo_ref[to, :] = v
                ho_ref[to, :] = ln_mod(v.astype(jnp.float32), shift, scale)
                return carry
            lax.fori_loop(0, count // sub, chunk, 0, unroll=min(4, count // sub))

        def height(s, carry):
            k = lax.rem(z + s, n)

            @pl.when(s > 0)
            def _():
                wait_for(xbuf.at[k], c_recv.at[k])
            norm_rows(k, 0, k * tp, tp)
            norm_rows(k, tp, n * tp + k * ip, ip)
            return carry

        lax.fori_loop(0, n, height, 0)

        for t, j in enumerate(across):
            wait_for(xbuf.at[0], p_send.at[t])

            @pl.when(j != z)
            def _():
                wait_for(xbuf.at[0], c_send.at[t])

        @pl.when(cfg != z)
        def _():
            wait_for(xbuf.at[0], c_send.at[n - 1])

        @pl.when(cfg == z)
        def _():
            for t, j in enumerate(across):
                remote(cond_ref, cond_buf, cond_send.at[t], cond_recv, (j, z, core)).wait_send()
        for t, h in enumerate(heights):
            wait_for(mine.at[h], t_send.at[t])
        others = tab_out.at[pl.ds(0, 2 * n - 1)]
        wait_for(others, q_send)
        wait_for(others, q_recv)


def enter(x_txt, x_img, cond, w_mod, w_fmod, b_mod, b_fmod, cosT, sinT, n, collective_id, width=512):
    n_txt, d = x_txt.shape
    n_img = x_img.shape[0]
    total = n_txt + n_img
    rows = total // n
    n_layers, _, dm = w_mod.shape
    per_layer, n_fin, per_row = dm // width, w_fmod.shape[1] // width, d // width
    n_mod = n_layers * per_layer
    steps = n_mod + n_fin
    dma = pltpu.SemaphoreType.DMA
    bf, f32 = jnp.bfloat16, jnp.float32

    def layer_of(i):
        j = jnp.minimum(i, n_mod - 1)
        return j // per_layer, lax.rem(j, per_layer)

    def last_of(i):
        return 0, jnp.maximum(i - n_mod, 0)

    hbm = pl.BlockSpec(memory_space=pl.ANY)
    out_shape = [jax.ShapeDtypeStruct((steps // per_row, d), f32), jax.ShapeDtypeStruct((total, d), bf), jax.ShapeDtypeStruct((total, d), bf),
                 jax.ShapeDtypeStruct((N_CORE * n, n, 2 * cosT.shape[0], n_img // n), f32)]
    return pl.pallas_call(
        functools.partial(enter_kernel, n_mod=n_mod, n_steps=steps, per_row=per_row, per_layer=per_layer),
        grid=(steps,),
        in_specs=[hbm, hbm, whole(cond.shape), pl.BlockSpec((1, d, width), lambda i: (layer_of(i)[0], 0, layer_of(i)[1])), pl.BlockSpec((d, width), last_of),
                  pl.BlockSpec((n_layers, width), lambda i: (0, layer_of(i)[1])), pl.BlockSpec((1, width), last_of), hbm, hbm],
        out_specs=[whole(v.shape) for v in out_shape[:-1]] + [hbm],
        out_shape=out_shape,
        scratch_shapes=[pltpu.VMEM((n, rows, d), bf), pltpu.VMEM((n, rows, d), bf), pltpu.VMEM(cond.shape, bf), pltpu.VMEM((16, d), bf),
                        dma((n - 1,)), dma, dma((n - 1,)), dma((n, 2)), dma((n,)), dma((n,)), dma, dma((n - 1,)), dma((n,)), dma, dma, dma],
        compiler_params=params(**talking(collective_id)),
        cost_estimate=pl.CostEstimate(flops=2 * 16 * d * width * steps, bytes_accessed=2 * d * width * steps, transcendentals=0),
        name='enter',
    )(x_txt, x_img, cond, w_mod, w_fmod, b_mod, b_fmod, cosT, sinT)


def solution(mesh):
    n_cfg = mesh.devices.shape[0]
    n_z = mesh.devices.shape[1] // N_CORE
    grid = Mesh(mesh.devices.reshape(n_cfg, n_z, N_CORE), ('cfg', 'z', 'core'))
    assert n_cfg == n_z == 4
    n_dev = n_cfg * N_CORE
    token_spec = P(('cfg', 'z', 'core'), None)
    seq_spec = P(('z', 'core'), None)
    in_specs = (token_spec, token_spec, P('cfg', None), seq_spec, seq_spec, token_spec) + (P(),) * 13

    def body(x_txt, x_img, cond_vec, cos_img, sin_img, z_lat, t_cur, t_next, w_mod, b_mod, w_in, b_in, qk_gain, w_out, b_out, w_fmod, b_fmod, w_final, b_final):
        n_txt, d = x_txt.shape
        n_img = x_img.shape[0]
        n_layers = w_mod.shape[0]
        nh = d // LANES // n_dev
        n_out = w_final.shape[1]

        mods, x, h, tables = enter(x_txt, x_img, cond_vec, w_mod, w_fmod, b_mod, b_fmod[None], cos_img.T, sin_img.T, n_cfg, 1)
        b_in3, b_out3 = b_in[:, None, :], b_out[:, None, :]
        for l in range(n_layers):
            last = l == n_layers - 1
            row0 = n_txt if last else 0
            y_mlp, _, qT, k, vT = block(h, w_in, b_in3, w_out, qk_gain, tables, l, n_txt, nh, row0, 2 + 2 * l)
            final = (w_final.T, b_final[None]) if last else None
            done = attend(qT, k, vT, w_out, b_out3, mods, x, y_mlp, l, n_dev, n_txt, row0, 3 + 2 * l, final)
            if not last:
                x, h = done

        return z_lat + (t_next - t_cur) * done.reshape(n_img, LANES)[:, :n_out]

    return jax.shard_map(body, mesh=grid, in_specs=in_specs, out_specs=token_spec, check_vma=False)
```

```python
import functools
import math

import jax
import jax.numpy as jnp
from jax import lax
from jax.experimental import pallas as pl
from jax.experimental.pallas import tpu as pltpu
from jax.sharding import Mesh, PartitionSpec as P

EPS = 1e-6
LANES = 128
GELU_C = math.sqrt(2.0 / math.pi)
LOG2E = math.log2(math.e)
VMEM_BYTES = 60 * 2**20
N_CORE = 2
MESH = pl.DeviceIdType.MESH


def params(**kw):
    return pltpu.CompilerParams(vmem_limit_bytes=VMEM_BYTES, dimension_semantics=('arbitrary',), **kw)


def talking(collective_id):
    return dict(collective_id=collective_id, has_side_effects=True)


def whole(shape, **kw):
    return pl.BlockSpec(shape, lambda i: (0,) * len(shape), **kw)


def head_rows(j):
    return slice(j * LANES, (j + 1) * LANES)


def columns_of(v):
    return jnp.broadcast_to(v.astype(jnp.float32), (LANES, LANES)).T


def wait_for(ref, sem):
    pltpu.make_async_copy(ref, ref, sem).wait()


def dot(a, b):
    return jnp.dot(a, b, preferred_element_type=jnp.float32)


def remote(src, dst, send_sem, recv_sem, device):
    return pltpu.make_async_remote_copy(src_ref=src, dst_ref=dst, send_sem=send_sem, recv_sem=recv_sem, device_id=device, device_id_type=MESH)


def meet(devices):
    barrier = pltpu.get_barrier_semaphore()
    for device in devices:
        pl.semaphore_signal(barrier, inc=1, device_id=device, device_id_type=MESH)
    pl.semaphore_wait(barrier, len(devices))


def ln_mod(x, shift, scale):
    centered = x - jnp.mean(x, axis=-1, keepdims=True)
    var = jnp.mean(centered * centered, axis=-1, keepdims=True)
    return (centered * lax.rsqrt(var + EPS) * (1.0 + scale) + shift).astype(jnp.bfloat16)


def gelu_tanh(u):
    return u * (0.5 * (1.0 + jnp.tanh(GELU_C * (u + 0.044715 * (u * u * u)))))


def related(cfg, core, r):
    cx, cy = cfg // 2, lax.rem(cfg, 2)
    x = lax.rem(cx + lax.rem(r // 2, 2), 2)
    y = lax.rem(cy + r // 4, 2)
    return x * 2 + y, lax.rem(core + lax.rem(r, 2), 2)


def block_kernel(b_in_ref, gain_ref, h_hbm, w_in_hbm, w_out_hbm, T, wt_hbm, y_hbm, H, qT_ref, k_ref, vT_ref, h_ref, w1_ring, w2_ring, y_acc, u_scr, act, wt, bb, gg, hbuf, tbuf,
                 h_own_sem, w1_sem, w2_sem, w_sem, h_sem, t_sem, y_sem, near_send, near_recv, pair_send, pair_recv, *, layer, n, n_dev, nh, n_txt, row0, at_t, at_x):
    i = pl.program_id(0)
    cfg, z, core = lax.axis_index('cfg'), lax.axis_index('z'), lax.axis_index('core')
    rows = y_acc.shape[0]
    total, d = h_hbm.shape
    hc = u_scr.shape[1]
    rb = total - n_txt
    half = LANES // 2
    n_heads = d // LANES
    stride = n_heads // nh

    def device(r):
        to, c = related(cfg, core, r)
        return to, z, c

    def slot_of(r):
        to, c = related(cfg, core, r)
        return to * N_CORE + c

    own, X, Y, D = range(0, n_dev, 2)
    T_, A, B = range(3)
    spans = ((0, n_txt), (n_txt, rb // 2), (n_txt + rb // 2, rb // 2))
    hops = [(own, T_, X), (own, A, X), (own, B, X), (Y, B, X), (own, T_, Y), (own, B, Y), (own, A, Y), (X, T_, Y), (X, A, Y)]

    def at_core(origin, piece):
        return H.at[slot_of(origin), pl.ds(*spans[piece]), :]

    def move(origin, piece, to, send_sem, recv_sem):
        src = h_hbm.at[pl.ds(*spans[piece]), :] if origin == own else at_core(origin, piece)
        return remote(src, at_core(origin, piece), send_sem, recv_sem, device(to))

    def near(origin, piece, to):
        k = ((origin ^ to) // 2 - 1) * 3 + piece
        return move(origin, piece, to, near_send.at[hops.index((origin, piece, to))], near_recv.at[k])

    def pair(origin, piece):
        k = origin // 2 * 3 + piece
        return move(origin, piece, 1, pair_send.at[k], pair_recv.at[k])

    def landed_near(origin, piece):
        wait_for(at_core(origin, piece), near_recv.at[(origin // 2 - 1) * 3 + piece])

    def landed_pair(origin, *pieces):
        for piece in pieces:
            wait_for(at_core(origin + 1, piece), pair_recv.at[origin // 2 * 3 + piece])

    h_copy = pltpu.make_async_copy(h_hbm, h_ref, h_own_sem)

    def w1_copy(j):
        cols = pl.ds(pl.multiple_of(3 * d + j * hc, hc), hc)
        return pltpu.make_async_copy(w_in_hbm.at[layer, :, cols], w1_ring.at[lax.rem(j, 2)], w1_sem.at[lax.rem(j, 2)])

    def w2_copy(j):
        at = pl.ds(pl.multiple_of(d + j * hc, hc), hc)
        return pltpu.make_async_copy(w_out_hbm.at[layer, at, :], w2_ring.at[lax.rem(j, 2)], w2_sem.at[lax.rem(j, 2)])

    def w_cols(j):
        col = (j // nh * n_heads + lax.rem(j, nh) * stride + cfg * N_CORE + core) * LANES
        return pl.ds(pl.multiple_of(col, LANES), LANES)

    wt_copy = pltpu.make_async_copy(wt_hbm.at[layer], wt, w_sem)

    def fetch(r, slot):
        pltpu.make_async_copy(T.at[slot_of(r)], tbuf.at[slot], t_sem.at[slot]).start()

        @pl.when(r == 0)
        def _():
            pltpu.make_async_copy(h_hbm.at[pl.ds(n_txt, rb), :], hbuf.at[slot], h_sem.at[slot]).start()

        @pl.when(r > 0)
        def _():
            pltpu.make_async_copy(H.at[slot_of(r), pl.ds(n_txt, rb), :], hbuf.at[slot], h_sem.at[slot]).start()

    def fetch_text(slot):
        for r in range(n_dev):
            src = at_core(r, T_) if r else h_hbm.at[pl.ds(0, n_txt), :]
            pltpu.make_async_copy(src, hbuf.at[slot, pl.ds(r * n_txt, n_txt), :], h_sem.at[slot]).start()

    sub = 2
    step = rows // sub

    def at_rows(r, first=0):
        return pl.ds(pl.multiple_of(first + r * step, 16), step)

    def each(part, rolled):
        if rolled:
            lax.fori_loop(0, sub, lambda r, carry: part(r) or carry, 0)
        else:
            for r in range(sub):
                part(r)

    def up(rolled=False):
        b1 = b_in_ref[0, :, pl.ds(pl.multiple_of(3 * d + i * hc, hc), hc)].astype(jnp.float32)

        def part(r):
            u = dot(h_ref[at_rows(r, row0), :], w1_ring[lax.rem(i, 2)])
            u_scr[at_rows(r), :] = (u + b1).astype(jnp.bfloat16)

        each(part, rolled)

    def gelu():
        act[...] = gelu_tanh(u_scr[...].astype(jnp.float32)).astype(jnp.bfloat16)

    def down(rolled=False):
        def part(r):
            y_acc[at_rows(r), :] += dot(act[at_rows(r), :], w2_ring[lax.rem(i + 1, 2)])

        each(part, rolled)

    @pl.when(i == 0)
    def _():
        w1_copy(0).start()
        h_copy.start()
        meet([device(1), device(X), device(Y)])
        for piece in (T_, A):
            near(own, piece, X).start()
        for piece in (T_, B):
            near(own, piece, Y).start()
        for piece in (T_, A, B):
            pair(own, piece).start()
        w1_copy(1).start()
        w2_copy(0).start()
        wt_copy.start()
        for j in range(2):
            gg[head_rows(j), :] = columns_of(gain_ref[0, j:j + 1, :])
        y_acc[...] = jnp.zeros_like(y_acc)
        h_copy.wait()
        w1_copy(i).wait()
        up(True)

    @pl.when((i > 0) & (i < n))
    def _():
        @pl.when(i + 1 < n)
        def _():
            w1_copy(i + 1).start()
        w2_copy(i).start()
        w2_copy(i - 1).wait()
        w1_copy(i).wait()
        gelu()
        up()
        down()

    @pl.when(i == n)
    def _():
        w2_copy(i - 1).wait()
        gelu()
        down(True)

    @pl.when(i == 1)
    def _():
        for j in range(3 * nh):
            bb[head_rows(j), :] = columns_of(b_in_ref[0, :, w_cols(j)])

    @pl.when(i == at_t)
    def _():
        landed_near(X, T_)
        near(X, T_, Y).start()
        near(own, A, Y).start()
        near(own, B, X).start()
        pair(X, T_).start()
        landed_near(Y, T_)
        pair(Y, T_).start()

    @pl.when(i == at_x)
    def _():
        landed_near(X, A)
        near(X, A, Y).start()
        pair(X, A).start()
        landed_near(Y, B)
        near(Y, B, X).start()
        pair(Y, B).start()
        landed_near(D, T_)
        pair(D, T_).start()
        landed_pair(own, T_, A, B)

    s = i - (n + 1)
    slot = lax.rem(i, 2)

    @pl.when(i == n)
    def _():
        landed_near(X, B)
        pair(X, B).start()
        landed_near(Y, A)
        pair(Y, A).start()
        landed_pair(X, T_, A)
        landed_pair(Y, T_, B)
        wt_copy.wait()
        fetch(0, 1 - slot)

    @pl.when(s == 0)
    def _():
        pltpu.make_async_copy(y_acc, y_hbm, y_sem).start()

    @pl.when(s == X)
    def _():
        landed_pair(X, B)
        landed_pair(Y, A)

    @pl.when((s >= 0) & (s < D - 1))
    def _():
        fetch(s + 1, 1 - slot)

    @pl.when(s == D - 1)
    def _():
        landed_pair(D, T_)
        fetch_text(1 - slot)

    @pl.when(s == D + 1)
    def _():
        landed_near(D, A)
        pair(D, A).start()
        landed_near(D, B)
        pair(D, B).start()
        fetch(D, slot)

    @pl.when(s == n_dev)
    def _():
        landed_pair(D, A, B)
        fetch(D + 1, slot)

    @pl.when(s >= 0)
    def _():
        image = s != D
        wait_for(hbuf.at[slot], h_sem.at[slot])

        @pl.when(image)
        def _():
            wait_for(tbuf.at[slot], t_sem.at[slot])
        h = hbuf[slot]
        table = jnp.concatenate([tbuf[slot, t] for t in range(tbuf.shape[1])], axis=1)
        cos, sin = jnp.where(image, table[:half], 1.0), jnp.where(image, table[half:], 0.0)

        def lanes(v):
            return jnp.concatenate([v] * (rb // LANES), axis=1)

        def proj(part):
            rs = slice(part * nh * LANES, (part + 1) * nh * LANES)
            return lax.dot_general(wt[rs, :], h, (((1,), (1,)), ((), ())), preferred_element_type=jnp.float32)

        def biased(x, j):
            return (x + lanes(bb[head_rows(j), :])).astype(jnp.bfloat16)

        def normed(x, j, g):
            x = biased(x, j).astype(jnp.float32)
            ms = jnp.sum(x * x, axis=0, keepdims=True) * (1.0 / LANES)
            v = x * lax.rsqrt(ms + EPS) * lanes(gg[head_rows(g), :])
            a, b = v[:half], v[half:]
            return jnp.concatenate([a * cos - b * sin, a * sin + b * cos], axis=0).astype(jnp.bfloat16)

        q = proj(0)
        for t in range(nh):
            v = normed(q[head_rows(t)], t, 0).astype(jnp.float32) * (LANES ** -0.5 * LOG2E)
            hi = v.astype(jnp.bfloat16)
            qT_ref[t, :LANES] = hi
            qT_ref[t, LANES:] = (v - hi.astype(jnp.float32)).astype(jnp.bfloat16)
        k = proj(1)
        for t in range(nh):
            k_ref[t] = normed(k[head_rows(t)], nh + t, 1).T
        v = proj(2)
        for t in range(nh):
            vT_ref[t] = biased(v[head_rows(t)], 2 * nh + t)

    @pl.when(s == n_dev)
    def _():
        for hop in hops:
            near(*hop).wait_send()
        for origin in (own, X, Y, D):
            for piece in (T_, A, B):
                pair(origin, piece).wait_send()
        wait_for(y_acc, y_sem)


def block(h, w_in, b_in3, w_out, qk_gain, tables, wt, layer, n_txt, nh, row0, collective_id, hc=512):
    total, d = h.shape
    n_dev = d // LANES // nh
    ff = w_in.shape[2] - 3 * d
    n = ff // hc
    m = total - row0
    rb = total - n_txt
    assert n_dev * n_txt == rb
    S = n_dev * total
    hbm = pl.BlockSpec(memory_space=pl.ANY)
    dma = pltpu.SemaphoreType.DMA
    bf, f32 = jnp.bfloat16, jnp.float32
    far = n_dev - 2

    def at(i):
        s = jnp.clip(i - (n + 1), 0, n_dev)
        return s + 2 * (s // far) - 3 * (s // (far + 1))

    three = pltpu.SemaphoreType.DMA((12,))
    return pl.pallas_call(
        functools.partial(block_kernel, layer=layer, n=n, n_dev=n_dev, nh=nh, n_txt=n_txt, row0=row0, at_t=n // 4, at_x=n // 2),
        grid=(n + 1 + n_dev + 1,),
        in_specs=[pl.BlockSpec((1, 1, b_in3.shape[2]), lambda i: (layer, 0, 0)), pl.BlockSpec((1, 2, LANES), lambda i: (layer, 0, 0)), hbm, hbm, hbm, hbm, hbm],
        out_specs=[hbm, hbm, pl.BlockSpec((nh, 2 * LANES, rb), lambda i: (0, 0, at(i))), pl.BlockSpec((nh, rb, LANES), lambda i: (0, at(i), 0)),
                   pl.BlockSpec((nh, LANES, rb), lambda i: (0, 0, at(i)))],
        out_shape=[jax.ShapeDtypeStruct((m, d), f32), jax.ShapeDtypeStruct((n_dev, total, d), bf),
                   jax.ShapeDtypeStruct((nh, 2 * LANES, S), bf), jax.ShapeDtypeStruct((nh, S, LANES), bf), jax.ShapeDtypeStruct((nh, LANES, S), bf)],
        scratch_shapes=[
            pltpu.VMEM((total, d), bf), pltpu.VMEM((2, d, hc), bf), pltpu.VMEM((2, hc, d), bf),
            pltpu.VMEM((m, d), f32), pltpu.VMEM((m, hc), bf), pltpu.VMEM((m, hc), bf), pltpu.VMEM((3 * nh * LANES, d), bf),
            pltpu.VMEM((3 * nh * LANES, LANES), f32), pltpu.VMEM((2 * LANES, LANES), f32), pltpu.VMEM((2, rb, d), bf), pltpu.VMEM((2, *tables.shape[1:]), f32),
            dma, dma((2,)), dma((2,)), dma, dma((2,)), dma((2,)), dma, dma((9,)), dma((9,)), three, three,
        ],
        compiler_params=params(**talking(collective_id)),
        cost_estimate=pl.CostEstimate(flops=4 * m * d * ff + 6 * S * d * nh * LANES, bytes_accessed=4 * d * ff + 2 * S * d, transcendentals=m * ff),
        name='block',
    )(b_in3, qk_gain, h, w_in, w_out, tables, wt)


def attend_kernel(qT_hbm, k_hbm, vT_hbm, w_hbm, bo_ref, mods_ref, *refs, layer, qt, kc, ck, ne, n_dev, n_txt, row0, last):
    if last:
        wf_ref, bf_ref, x_hbm, y_hbm, vel_hbm, *refs = refs
        *refs, vel, vown_sem, vsend_sem, vrecv_sem = refs
    else:
        x_hbm, y_hbm, xo_hbm, ho_hbm, *refs = refs
        *refs, tbuf, t_rows, tsend_sem, trecv_sem, out_sem = refs
    (qT_ref, k_ref, vT_ref, s_scr, m_scr, part_scr, acc_scr, l_scr, obuf, o_rows, w_ring, lhs, y_acc, xbuf, h_ring,
     in_sem, send_sem, recv_sem, w_sem, res_sem) = refs
    nh, S, hd = k_ref.shape
    n_img = o_rows.shape[2]
    R, d = y_acc.shape
    nk = S // kc
    n_ring = w_ring.shape[0]
    nc = d // ck
    ahead = 2
    f32, bf = jnp.float32, jnp.bfloat16
    cfg, z, core = lax.axis_index('cfg'), lax.axis_index('z'), lax.axis_index('core')
    me = cfg * N_CORE + core

    def load(t):
        pairs = ((qT_hbm, qT_ref), (k_hbm, k_ref), (vT_hbm, vT_ref))
        return [pltpu.make_async_copy(src.at[t], dst.at[t], in_sem.at[t, j]) for j, (src, dst) in enumerate(pairs)]

    def w_copy(c):
        slot = lax.rem(c, n_ring)
        return pltpu.make_async_copy(w_hbm.at[layer, pl.ds(pl.multiple_of(c * ck, ck), ck), :], w_ring.at[slot], w_sem.at[slot])

    residual = [pltpu.make_async_copy(y_hbm, y_acc, res_sem.at[0]), pltpu.make_async_copy(x_hbm.at[pl.ds(row0, R), :], xbuf, res_sem.at[1])]

    def device(r):
        to, c = related(cfg, core, r)
        return to, z, c

    for cp in load(0):
        cp.start()
    peers = [device(r) for r in range(1, n_dev)]
    if last:
        peers += [(z, e, core) for e in range(ne)] + [(e, cfg, core) for e in range(ne)]
    meet(peers)
    for cp in load(0):
        cp.wait()
    for t in range(1, nh):
        for cp in load(t):
            cp.start()

    def score_chunk(head, q, slot, i, m):
        rows = pl.ds(i * kc, kc)
        k = k_ref[head, rows, :]
        s = dot(jnp.concatenate([k, k], axis=1), q)
        s_scr[slot, rows, :] = s
        return jnp.maximum(m, jnp.max(s.reshape(kc // 8, 8, qt), axis=0))

    def lowest():
        return jnp.full((8, qt), -jnp.inf, f32)

    def full_max(m):
        return jnp.broadcast_to(jnp.max(m, axis=0, keepdims=True), (8, qt))

    def prob_chunk(head, m, slot, i, l, acc):
        rows = pl.ds(i * kc, kc)
        p = jnp.exp2(s_scr[slot, rows, :].reshape(kc // 8, 8, qt) - m[None])
        l = l + jnp.sum(p, axis=0)
        return l, acc + dot(vT_ref[head, :, rows], p.reshape(kc, qt).astype(bf))

    def load_q(tile):
        head, col = tile
        return qT_ref[head, :, pl.ds(pl.multiple_of(col, qt), qt)]

    def normalized(acc, l):
        return (acc / jnp.sum(l, axis=0, keepdims=True)).T.astype(bf)

    def stream(n_pairs, tile, buf, after, before):
        first, second = tile(0), tile(1)
        q, m = load_q(first), lowest()
        for i in range(nk):
            m = score_chunk(first[0], q, 0, i, m)
        m_scr[...] = full_max(m)
        q, m = load_q(second), lowest()
        for i in range(ahead):
            m = score_chunk(second[0], q, 1, i, m)
        part_scr[...] = m
        acc_scr[...] = jnp.zeros_like(acc_scr)
        l_scr[...] = jnp.ones_like(l_scr)

        def put(p, half, o):
            buf[p, half * qt:(half + 1) * qt, :] = o

        def pair(p, carry):
            before(p)
            later = lax.rem(p + 1, n_pairs)
            tiles = [tile(2 * p), tile(2 * p + 1), tile(2 * later), tile(2 * later + 1)]
            m, top = part_scr[...], m_scr[...]
            put(lax.rem(p + n_pairs - 1, n_pairs), 1, normalized(acc_scr[...], l_scr[...]))
            for half in range(2):
                l, acc = jnp.zeros((8, qt), f32), jnp.zeros((hd, qt), f32)
                q1, q2 = load_q(tiles[half + 1]), load_q(tiles[half + 2])
                for i in range(nk):
                    j = i + ahead
                    if j < nk:
                        m = score_chunk(tiles[half + 1][0], q1, 1 - half, j, m)
                    else:
                        if j == nk:
                            following, m = full_max(m), lowest()
                        m = score_chunk(tiles[half + 2][0], q2, half, j - nk, m)
                    l, acc = prob_chunk(tiles[half][0], top, half, i, l, acc)
                top = following
                if half == 0:
                    put(p, 0, normalized(acc, l))
                else:
                    acc_scr[...] = acc
                    l_scr[...] = l
            part_scr[...] = m
            m_scr[...] = top

            @pl.when(p > 0)
            def _():
                after(p - 1)
            return carry

        lax.fori_loop(0, n_pairs, pair, 0)
        put(n_pairs - 1, 1, normalized(acc_scr[...], l_scr[...]))
        after(n_pairs - 1)

    if not last:
        n_text = n_dev * n_txt
        assert n_text == 2 * qt

        def txt_send(head):
            for owner in range(n_dev):
                part = pl.ds(owner * n_txt, n_txt)
                if owner == 0:
                    t_rows[me, head] = tbuf[head, part, :]
                else:
                    remote(tbuf.at[head, part, :], t_rows.at[me, head], tsend_sem, trecv_sem, device(owner)).start()

        def txt_head(p):
            @pl.when(p < nh - 1)
            def _():
                for cp in load(p + 1):
                    cp.wait()

        stream(nh, lambda u: (u // 2, n_dev * n_img + lax.rem(u, 2) * qt), tbuf, txt_send, txt_head)

    def relation_of(p):
        return lax.rem(p + 1, n_dev)

    def img_tile(u):
        p = u // 2
        return p // n_dev, relation_of(p) * n_img + lax.rem(u, 2) * qt

    def img_send(p):
        head, owner = p // n_dev, relation_of(p)

        @pl.when(owner == 0)
        def _():
            o_rows[me, head] = obuf[p]

        @pl.when(owner != 0)
        def _():
            remote(obuf.at[p], o_rows.at[me, head], send_sem, recv_sem.at[head], device(owner)).start()

    def img_before(p):
        if last:
            @pl.when((relation_of(p) == 0) & (p < nh * n_dev - 1))
            def _():
                for cp in load(p // n_dev + 1):
                    cp.wait()

        @pl.when(p == 2)
        def _():
            for c in range(n_ring):
                w_copy(c).start()
            for cp in residual:
                cp.start()

    stream(nh * n_dev, img_tile, obuf, img_send, img_before)

    for cp in residual:
        cp.wait()
    others = pl.ds(0, n_dev - 1)
    if not last:
        wait_for(t_rows.at[others], trecv_sem)
    per = nc // nh
    wide = ck // LANES

    def chunk_of_w(c, carry):
        head = c // per

        @pl.when(lax.rem(c, per) == 0)
        def _():
            wait_for(o_rows.at[others, head], recv_sem.at[head])
        for t in range(wide):
            src = lax.rem(c, per) * wide + t
            if not last:
                lhs[:n_txt, head_rows(t)] = t_rows[src, head]
            lhs[R - n_img:, head_rows(t)] = o_rows[src, head]
        w_copy(c).wait()
        y_acc[...] += dot(lhs[...], w_ring[lax.rem(c, n_ring)])

        @pl.when(c + n_ring < nc)
        def _():
            w_copy(c + n_ring).start()
        return carry

    lax.fori_loop(0, nc, chunk_of_w, 0)

    gate_row = 3 * layer + 2
    gate, shift, scale = (mods_ref[r:r + 1, :] for r in range(gate_row, gate_row + 3))
    bo = bo_ref[0].astype(f32)
    er = R // ne
    sub = 16 if er % 16 == 0 else 8

    def put_rows(e, slot):
        rows = pl.ds(pl.multiple_of(e * er, sub), er)
        pltpu.make_async_copy(xbuf.at[rows, :], xo_hbm.at[rows, :], out_sem.at[2]).start()
        pltpu.make_async_copy(h_ring.at[slot], ho_hbm.at[rows, :], out_sem.at[slot]).start()

    def deliver(e):
        own = (z == cfg) & (e == z)

        @pl.when(own)
        def _():
            pltpu.make_async_copy(vel.at[e], vel_hbm.at[cfg], vown_sem).start()

        @pl.when(jnp.logical_not(own))
        def _():
            remote(vel.at[e], vel_hbm.at[cfg], vsend_sem.at[e], vrecv_sem.at[cfg], (z, e, core)).start()

    def rows_out(e, carry):
        slot = lax.rem(e, 2)
        if not last:
            @pl.when(e >= 2)
            def _():
                wait_for(h_ring.at[slot], out_sem.at[slot])

        def chunk(c, carry):
            rs = pl.ds(pl.multiple_of(e * er + c * sub, sub), sub)
            xn = (xbuf[rs, :].astype(f32) + gate * (y_acc[rs, :] + bo)).astype(bf)
            h_ring[slot, pl.ds(pl.multiple_of(c * sub, sub), sub), :] = ln_mod(xn.astype(f32), shift, scale)
            if not last:
                xbuf[rs, :] = xn
            return carry

        lax.fori_loop(0, er // sub, chunk, 0, unroll=3 if (er // sub) % 3 == 0 else 2)
        if last:
            w = jnp.concatenate([wf_ref[...], jnp.zeros((LANES - wf_ref.shape[0], d), bf)], axis=0)
            v = lax.dot_general(h_ring[slot], w, (((1,), (1,)), ((), ())), preferred_element_type=f32)
            b = bf_ref[...].astype(f32)
            vel[e] = v + jnp.concatenate([b, jnp.zeros((1, LANES - b.shape[1]), f32)], axis=1)
            deliver(e)
        else:
            put_rows(e, slot)
        return carry

    lax.fori_loop(0, ne, rows_out, 0)

    wait_for(o_rows.at[others], send_sem)
    if last:
        for e in range(ne):
            own = (z == cfg) & (e == z)

            @pl.when(own)
            def _():
                wait_for(vel.at[e], vown_sem)

            @pl.when(jnp.logical_not(own))
            def _():
                wait_for(vel.at[e], vsend_sem.at[e])
                wait_for(vel_hbm.at[e], vrecv_sem.at[e])
    else:
        wait_for(t_rows.at[others], tsend_sem)
        wait_for(xbuf, out_sem.at[2])
        for slot in range(2):
            wait_for(h_ring.at[slot], out_sem.at[slot])


def largest(n, cap, unit):
    return max(c for c in range(unit, cap + 1, unit) if n % c == 0)


def attend(qT, k, vT, w_out, b_out3, mods, x, y_mlp, layer, n_dev, n_txt, row0, collective_id, final=None, ck=512, ne=4):
    nh, S, hd = k.shape
    R, d = y_mlp.shape
    n_img = S // n_dev - n_txt
    last = final is not None
    qt = n_img // 2
    dma = pltpu.SemaphoreType.DMA
    bf, f32 = jnp.bfloat16, jnp.float32
    hbm = pl.BlockSpec(memory_space=pl.ANY)
    stat = pltpu.VMEM((8, qt), f32)
    scratch = [pltpu.VMEM(v.shape, bf) for v in (qT, k, vT)] + [
        pltpu.VMEM((2, S, qt), f32), stat, stat, pltpu.VMEM((hd, qt), f32), stat, pltpu.VMEM((nh * n_dev, n_img, hd), bf), pltpu.VMEM((n_dev, nh, n_img, hd), bf),
        pltpu.VMEM((2, ck, d), bf), pltpu.VMEM((R, ck), bf), pltpu.VMEM((R, d), f32), pltpu.VMEM((R, d), bf), pltpu.VMEM((2, R // ne, d), bf),
        dma((nh, 3)), dma, dma((nh,)), dma((2,)), dma((2,))]
    if last:
        out_shape = jax.ShapeDtypeStruct((ne, R // ne, LANES), f32)
        scratch += [pltpu.VMEM(out_shape.shape, f32), dma, dma((ne,)), dma((ne,))]
    else:
        out_shape = [jax.ShapeDtypeStruct((R, d), bf)] * 2
        scratch += [pltpu.VMEM((nh, n_dev * n_txt, hd), bf), pltpu.VMEM((n_dev, nh, n_txt, hd), bf), dma, dma, dma((3,))]
    extra = list(final or ())
    return pl.pallas_call(
        functools.partial(attend_kernel, layer=layer, qt=qt, kc=largest(S, 768, 256), ck=ck, ne=ne, n_dev=n_dev, n_txt=n_txt, row0=row0, last=last),
        grid=(1,),
        in_specs=[hbm] * 4 + [pl.BlockSpec((1, 1, d), lambda i: (layer, 0, 0)), whole(mods.shape)] + [whole(v.shape) for v in extra] + [hbm] * 2,
        out_specs=hbm if last else [hbm] * 2,
        out_shape=out_shape,
        scratch_shapes=scratch,
        compiler_params=params(**talking(collective_id)),
        cost_estimate=pl.CostEstimate(flops=6 * nh * n_dev * R * S * hd + 2 * R * d * d, bytes_accessed=8 * nh * S * hd + 2 * d * d + 14 * R * d, transcendentals=nh * S * n_dev * R),
        name='attend',
    )(qT, k, vT, w_out, b_out3, mods, *extra, x, y_mlp)


def enter_kernel(xt_hbm, xi_hbm, cond_ref, wm_ref, wf_ref, bm_ref, bf_ref, cos_hbm, sin_hbm, w_in_hbm, mods_ref, xo_hbm, ho_hbm, tab_out, wt_hbm,
                 stage, xbuf, hbuf, cond_buf, s_scr, wbuf, turned, w_sem, wt_sem, out_sem,
                 cond_send, cond_recv, p_send, p_recv, c_send, c_recv, own_sem, t_send, t_recv, town_sem, q_send, q_recv, *, n_mod, n_steps, per_row, per_layer):
    i = pl.program_id(0)
    n, rows, d = xbuf.shape
    tp = xt_hbm.shape[0] // n
    ip = xi_hbm.shape[0] // n
    cfg, z, core = lax.axis_index('cfg'), lax.axis_index('z'), lax.axis_index('core')
    across = [related(cfg, core, r)[0] for r in range(2, 2 * n, 2)]
    heights = [lax.rem(z + s, n) for s in range(1, n)]
    plane = [(to, z, c) for to, c in (related(cfg, core, r) for r in range(1, 2 * n))]
    mine = tab_out.at[cfg * N_CORE + core]
    cut = rows // 2
    first = (cut // 2 + 7) // 8 * 8
    spans = ((0, first), (first, cut - first), (cut, first), (cut + first, cut - first))

    def piece_refs(j, dst):
        out = []
        for at, size in spans:
            head = [(xt_hbm.at[pl.ds(j * tp, tp), :], dst.at[pl.ds(0, tp), :])] if at == 0 else []
            skip = tp if at == 0 else 0
            out.append(head + [(xi_hbm.at[pl.ds(j * ip + at + skip - tp, size - skip), :], dst.at[pl.ds(at + skip, size - skip), :])])
        return out

    def tables(to):
        half = cos_hbm.shape[0]
        cols = pl.ds(pl.multiple_of(cfg * ip, ip), ip)
        return [(src.at[:, cols], to.at[pl.ds(t * half, half), :]) for t, src in enumerate((cos_hbm, sin_hbm))]

    def forward(group, t, part):
        at = pl.ds(*spans[part])

        @pl.when(group == z)
        def _():
            xbuf[z, at, :] = stage[group, at, :]

        @pl.when(group != z)
        def _():
            remote(stage.at[group, at, :], xbuf.at[z, at, :], c_send.at[t], c_recv.at[z], (cfg, group, core)).start()

    def silu_of(ref):
        v = ref[...].astype(jnp.float32)
        s_scr[...] = jnp.broadcast_to((v * jax.nn.sigmoid(v)).astype(jnp.bfloat16), s_scr.shape)

    @pl.when(i == 0)
    def _():
        meet(plane + [(cfg, h, core) for h in heights])

        @pl.when(cfg == z)
        def _():
            for t, j in enumerate(across):
                remote(cond_ref, cond_buf, cond_send.at[t], cond_recv, (j, z, core)).start()
        for part in range(len(spans)):
            for t, j in ((0, across[0]), (2, across[2]), (1, across[1])):
                for src, dst in piece_refs(j, stage.at[cfg])[part]:
                    remote(src, dst, p_send.at[t], p_recv.at[cfg, part], (j, z, core)).start()
        held = sum(piece_refs(cfg, xbuf.at[z]), [])

        @pl.when(cfg == z)
        def _():
            for src, dst in held:
                pltpu.make_async_copy(src, dst, own_sem).start()

        @pl.when(cfg != z)
        def _():
            for src, dst in held:
                remote(src, dst, c_send.at[n - 1], c_recv.at[z], (cfg, cfg, core)).start()
        for t, h in enumerate(heights):
            for src, dst in tables(mine.at[z]):
                remote(src, dst, t_send.at[t], t_recv.at[z], (cfg, h, core)).start()
        for src, dst in tables(mine.at[z]):
            pltpu.make_async_copy(src, dst, town_sem).start()

        @pl.when(cfg == z)
        def _():
            silu_of(cond_ref)

        @pl.when(cfg != z)
        def _():
            remote(cond_ref, cond_buf, cond_send.at[0], cond_recv, (cfg, z, core)).wait_recv()
            silu_of(cond_buf)

    row, col = i // per_row, lax.rem(i, per_row)
    width = wm_ref.shape[2]
    cols = pl.ds(pl.multiple_of(col * width, width), width)

    @pl.when(i < n_mod)
    def _():
        v = dot(s_scr[...], wm_ref[0])
        b = bm_ref[...].astype(jnp.float32)
        of_layer = lax.broadcasted_iota(jnp.int32, b.shape, 0) == i // per_layer
        mods_ref[pl.ds(row, 1), cols] = v[0:1] + jnp.sum(jnp.where(of_layer, b, 0.0), axis=0, keepdims=True)

    @pl.when(i >= n_mod)
    def _():
        v = dot(s_scr[...], wf_ref[...])
        mods_ref[pl.ds(row, 1), cols] = v[0:1] + bf_ref[...].astype(jnp.float32)

    def arrived(t, part):
        j = across[t]
        wait_for(stage.at[j, pl.ds(*spans[part]), :], p_recv.at[j, part])
        forward(j, t, part)

    @pl.when(i == n_steps - 2)
    def _():
        for h in heights:
            wait_for(mine.at[h], t_recv.at[h])
        wait_for(mine.at[z], town_sem)
        for peer in plane:
            remote(mine, mine, q_send, q_recv, peer).start()

    for part in range(len(spans)):
        due = 7 + 9 * part

        @pl.when(i == due)
        def _():
            arrived(0, part)

        @pl.when(i == due + 6)
        def _():
            arrived(2, part)
            arrived(1, part)

    @pl.when(i == n_steps - 1)
    def _():
        shift, scale = mods_ref[0:1, :], mods_ref[1:2, :]

        @pl.when(cfg == z)
        def _():
            wait_for(xbuf.at[z], own_sem)

        d_in, heads = w_in_hbm.shape[1] // LANES, wt_hbm.shape[1] // LANES

        def w_copy(j):
            layer, b = j // heads, lax.rem(j, heads)
            nh = heads // 3
            col = (b // nh * d_in + lax.rem(b, nh) * (d_in // nh) + cfg * N_CORE + core) * LANES
            return pltpu.make_async_copy(w_in_hbm.at[layer, :, pl.ds(pl.multiple_of(col, LANES), LANES)], wbuf.at[lax.rem(j, 2)], w_sem.at[lax.rem(j, 2)])

        def turn(j, carry):
            slot = lax.rem(j, 2)
            w_copy(j).wait()

            @pl.when(j > 1)
            def _():
                wait_for(turned.at[slot], wt_sem.at[slot])
            turned[slot] = wbuf[slot].T

            @pl.when(j + 2 < n_turns)
            def _():
                w_copy(j + 2).start()
            to = pl.ds(pl.multiple_of(lax.rem(j, heads) * LANES, LANES), LANES)
            pltpu.make_async_copy(turned.at[slot], wt_hbm.at[j // heads, to, :], wt_sem.at[slot]).start()
            return carry

        n_turns = wt_hbm.shape[0] * heads
        w_copy(0).start()
        w_copy(1).start()
        lax.fori_loop(0, n_turns, turn, 0)

        def height(s, carry):
            k = lax.rem(z + s, n)

            @pl.when(s > 0)
            def _():
                wait_for(xbuf.at[k], c_recv.at[k])
            sub = 16 if rows % 16 == 0 else 8

            def chunk(c, carry):
                at = pl.ds(pl.multiple_of(c * sub, sub), sub)
                hbuf[k, at, :] = ln_mod(xbuf[k, at, :].astype(jnp.float32), shift, scale)
                return carry

            lax.fori_loop(0, rows // sub, chunk, 0, unroll=3)
            for t, (src, dst) in enumerate(((xbuf, xo_hbm), (hbuf, ho_hbm))):
                for at, size, to in ((0, tp, k * tp), (tp, ip, n * tp + k * ip)):
                    pltpu.make_async_copy(src.at[k, pl.ds(at, size), :], dst.at[pl.ds(to, size), :], out_sem.at[t]).start()
            return carry

        lax.fori_loop(0, n, height, 0)
        for slot in range(2):
            wait_for(turned.at[slot], wt_sem.at[slot])
        wait_for(xbuf, out_sem.at[0])
        wait_for(hbuf, out_sem.at[1])

        for t, j in enumerate(across):
            wait_for(xbuf.at[0], p_send.at[t])

            @pl.when(j != z)
            def _():
                wait_for(xbuf.at[0], c_send.at[t])

        @pl.when(cfg != z)
        def _():
            wait_for(xbuf.at[0], c_send.at[n - 1])

        @pl.when(cfg == z)
        def _():
            for t, j in enumerate(across):
                remote(cond_ref, cond_buf, cond_send.at[t], cond_recv, (j, z, core)).wait_send()
        for t, h in enumerate(heights):
            wait_for(mine.at[h], t_send.at[t])
        others = tab_out.at[pl.ds(0, 2 * n - 1)]
        wait_for(others, q_send)
        wait_for(others, q_recv)


def enter(x_txt, x_img, cond, w_mod, w_fmod, b_mod, b_fmod, cosT, sinT, w_in, nh, n, collective_id, width=512):
    n_txt, d = x_txt.shape
    n_img = x_img.shape[0]
    total = n_txt + n_img
    rows = total // n
    n_layers, _, dm = w_mod.shape
    per_layer, n_fin, per_row = dm // width, w_fmod.shape[1] // width, d // width
    n_mod = n_layers * per_layer
    steps = n_mod + n_fin
    dma = pltpu.SemaphoreType.DMA
    bf, f32 = jnp.bfloat16, jnp.float32

    def layer_of(i):
        j = jnp.minimum(i, n_mod - 1)
        return j // per_layer, lax.rem(j, per_layer)

    def last_of(i):
        return 0, jnp.maximum(i - n_mod, 0)

    hbm = pl.BlockSpec(memory_space=pl.ANY)
    out_shape = [jax.ShapeDtypeStruct((steps // per_row, d), f32), jax.ShapeDtypeStruct((total, d), bf), jax.ShapeDtypeStruct((total, d), bf),
                 jax.ShapeDtypeStruct((N_CORE * n, n, 2 * cosT.shape[0], n_img // n), f32),
                 jax.ShapeDtypeStruct((n_layers, 3 * nh * LANES, d), bf)]
    return pl.pallas_call(
        functools.partial(enter_kernel, n_mod=n_mod, n_steps=steps, per_row=per_row, per_layer=per_layer),
        grid=(steps,),
        in_specs=[hbm, hbm, whole(cond.shape), pl.BlockSpec((1, d, width), lambda i: (layer_of(i)[0], 0, layer_of(i)[1])), pl.BlockSpec((d, width), last_of),
                  pl.BlockSpec((n_layers, width), lambda i: (0, layer_of(i)[1])), pl.BlockSpec((1, width), last_of), hbm, hbm, hbm],
        out_specs=[whole(out_shape[0].shape)] + [hbm] * 4,
        out_shape=out_shape,
        scratch_shapes=[pltpu.VMEM((n, rows, d), bf)] * 3 + [pltpu.VMEM(cond.shape, bf), pltpu.VMEM((16, d), bf), pltpu.VMEM((2, d, LANES), bf), pltpu.VMEM((2, LANES, d), bf),
                        dma((2,)), dma((2,)), dma((2,)), dma((n - 1,)), dma, dma((n - 1,)), dma((n, 4)), dma((n,)), dma((n,)), dma, dma((n - 1,)), dma((n,)), dma, dma, dma],
        compiler_params=params(**talking(collective_id)),
        cost_estimate=pl.CostEstimate(flops=2 * 16 * d * width * steps, bytes_accessed=2 * d * width * steps, transcendentals=0),
        name='enter',
    )(x_txt, x_img, cond, w_mod, w_fmod, b_mod, b_fmod, cosT, sinT, w_in)


def solution(mesh):
    n_cfg = mesh.devices.shape[0]
    n_z = mesh.devices.shape[1] // N_CORE
    grid = Mesh(mesh.devices.reshape(n_cfg, n_z, N_CORE), ('cfg', 'z', 'core'))
    assert n_cfg == n_z == 4
    n_dev = n_cfg * N_CORE
    token_spec = P(('cfg', 'z', 'core'), None)
    seq_spec = P(('z', 'core'), None)
    in_specs = (token_spec, token_spec, P('cfg', None), seq_spec, seq_spec, token_spec) + (P(),) * 13

    def body(x_txt, x_img, cond_vec, cos_img, sin_img, z_lat, t_cur, t_next, w_mod, b_mod, w_in, b_in, qk_gain, w_out, b_out, w_fmod, b_fmod, w_final, b_final):
        n_txt, d = x_txt.shape
        n_img = x_img.shape[0]
        n_layers = w_mod.shape[0]
        nh = d // LANES // n_dev
        n_out = w_final.shape[1]

        mods, x, h, tables, wt = enter(x_txt, x_img, cond_vec, w_mod, w_fmod, b_mod, b_fmod[None], cos_img.T, sin_img.T, w_in, nh, n_cfg, 1)
        b_in3, b_out3 = b_in[:, None, :], b_out[:, None, :]
        for l in range(n_layers):
            last = l == n_layers - 1
            row0 = n_txt if last else 0
            y_mlp, _, qT, k, vT = block(h, w_in, b_in3, w_out, qk_gain, tables, wt, l, n_txt, nh, row0, 2 + 2 * l)
            final = (w_final.T, b_final[None]) if last else None
            done = attend(qT, k, vT, w_out, b_out3, mods, x, y_mlp, l, n_dev, n_txt, row0, 3 + 2 * l, final)
            if not last:
                x, h = done

        return z_lat + (t_next - t_cur) * done.reshape(n_img, LANES)[:, :n_out]

    return jax.shard_map(body, mesh=grid, in_specs=in_specs, out_specs=token_spec, check_vma=False)
```

```python
import functools
import math

import jax
import jax.numpy as jnp
from jax import lax
from jax.experimental import pallas as pl
from jax.experimental.pallas import tpu as pltpu
from jax.sharding import Mesh, PartitionSpec as P

EPS = 1e-6
LANES = 128
GELU_C = math.sqrt(2.0 / math.pi)
LOG2E = math.log2(math.e)
VMEM_BYTES = 60 * 2**20
N_CORE = 2
MESH = pl.DeviceIdType.MESH


def params(**kw):
    return pltpu.CompilerParams(vmem_limit_bytes=VMEM_BYTES, dimension_semantics=('arbitrary',), **kw)


def talking(collective_id):
    return dict(collective_id=collective_id, has_side_effects=True)


def whole(shape, **kw):
    return pl.BlockSpec(shape, lambda i: (0,) * len(shape), **kw)


def head_rows(j):
    return slice(j * LANES, (j + 1) * LANES)


def columns_of(v):
    return jnp.broadcast_to(v.astype(jnp.float32), (LANES, LANES)).T


def wait_for(ref, sem):
    pltpu.make_async_copy(ref, ref, sem).wait()


def dot(a, b):
    return jnp.dot(a, b, preferred_element_type=jnp.float32)


def remote(src, dst, send_sem, recv_sem, device):
    return pltpu.make_async_remote_copy(src_ref=src, dst_ref=dst, send_sem=send_sem, recv_sem=recv_sem, device_id=device, device_id_type=MESH)


def meet(devices):
    barrier = pltpu.get_barrier_semaphore()
    for device in devices:
        pl.semaphore_signal(barrier, inc=1, device_id=device, device_id_type=MESH)
    pl.semaphore_wait(barrier, len(devices))


def ln_mod(x, shift, scale):
    centered = x - jnp.mean(x, axis=-1, keepdims=True)
    var = jnp.mean(centered * centered, axis=-1, keepdims=True)
    return (centered * lax.rsqrt(var + EPS) * (1.0 + scale) + shift).astype(jnp.bfloat16)


def gelu_tanh(u):
    return u * (0.5 * (1.0 + jnp.tanh(GELU_C * (u + 0.044715 * (u * u * u)))))


def related(cfg, core, r):
    cx, cy = cfg // 2, lax.rem(cfg, 2)
    x = lax.rem(cx + lax.rem(r // 2, 2), 2)
    y = lax.rem(cy + r // 4, 2)
    return x * 2 + y, lax.rem(core + lax.rem(r, 2), 2)


def block_kernel(b_in_ref, gain_ref, h_hbm, w_in_hbm, w_out_hbm, T, wt_hbm, y_hbm, H, qT_ref, k_ref, vT_ref, h_ref, w1_ring, w2_ring, y_acc, u_scr, act, wt, bb, gg, hbuf, tbuf,
                 h_own_sem, w1_sem, w2_sem, w_sem, h_sem, t_sem, y_sem, near_send, near_recv, pair_send, pair_recv, *, layer, n, n_dev, nh, n_txt, row0, at_t, at_x):
    i = pl.program_id(0)
    cfg, z, core = lax.axis_index('cfg'), lax.axis_index('z'), lax.axis_index('core')
    rows = y_acc.shape[0]
    total, d = h_hbm.shape
    hc = u_scr.shape[1]
    rb = total - n_txt
    half = LANES // 2
    n_heads = d // LANES
    stride = n_heads // nh

    def device(r):
        to, c = related(cfg, core, r)
        return to, z, c

    def slot_of(r):
        to, c = related(cfg, core, r)
        return to * N_CORE + c

    own, X, Y, D = range(0, n_dev, 2)
    T_, A, B = range(3)
    a_rows = (rb - n_txt) // 2
    spans = ((0, n_txt), (n_txt, a_rows), (n_txt + a_rows, rb - a_rows))
    hops = [(own, T_, X), (own, A, X), (own, B, X), (Y, B, X), (own, T_, Y), (own, B, Y), (own, A, Y), (X, T_, Y), (X, A, Y)]

    def at_core(origin, piece):
        return H.at[slot_of(origin), pl.ds(*spans[piece]), :]

    def move(origin, piece, to, send_sem, recv_sem):
        src = h_ref.at[pl.ds(*spans[piece]), :] if origin == own else at_core(origin, piece)
        return remote(src, at_core(origin, piece), send_sem, recv_sem, device(to))

    def near(origin, piece, to):
        k = ((origin ^ to) // 2 - 1) * 3 + piece
        return move(origin, piece, to, near_send.at[hops.index((origin, piece, to))], near_recv.at[k])

    def pair(origin, piece):
        k = origin // 2 * 3 + piece
        return move(origin, piece, 1, pair_send.at[k], pair_recv.at[k])

    def landed_near(origin, piece):
        wait_for(at_core(origin, piece), near_recv.at[(origin // 2 - 1) * 3 + piece])

    def landed_pair(origin, *pieces):
        for piece in pieces:
            wait_for(at_core(origin + 1, piece), pair_recv.at[origin // 2 * 3 + piece])

    h_copy = pltpu.make_async_copy(h_hbm, h_ref, h_own_sem)

    def w1_copy(j):
        cols = pl.ds(pl.multiple_of(3 * d + j * hc, hc), hc)
        return pltpu.make_async_copy(w_in_hbm.at[layer, :, cols], w1_ring.at[lax.rem(j, 2)], w1_sem.at[lax.rem(j, 2)])

    def w2_copy(j):
        at = pl.ds(pl.multiple_of(d + j * hc, hc), hc)
        return pltpu.make_async_copy(w_out_hbm.at[layer, at, :], w2_ring.at[lax.rem(j, 2)], w2_sem.at[lax.rem(j, 2)])

    def w_cols(j):
        col = (j // nh * n_heads + lax.rem(j, nh) * stride + cfg * N_CORE + core) * LANES
        return pl.ds(pl.multiple_of(col, LANES), LANES)

    wt_copy = pltpu.make_async_copy(wt_hbm.at[layer], wt, w_sem)

    def fetch(r, slot):
        pltpu.make_async_copy(T.at[slot_of(r)], tbuf.at[slot], t_sem.at[slot]).start()

        @pl.when(r == 0)
        def _():
            pltpu.make_async_copy(h_hbm.at[pl.ds(n_txt, rb), :], hbuf.at[slot], h_sem.at[slot]).start()

        @pl.when(r > 0)
        def _():
            pltpu.make_async_copy(H.at[slot_of(r), pl.ds(n_txt, rb), :], hbuf.at[slot], h_sem.at[slot]).start()

    def fetch_text(slot):
        for r in range(n_dev):
            src = at_core(r, T_) if r else h_hbm.at[pl.ds(0, n_txt), :]
            pltpu.make_async_copy(src, hbuf.at[slot, pl.ds(r * n_txt, n_txt), :], h_sem.at[slot]).start()

    sub = 2
    step = rows // sub

    def at_rows(r, first=0):
        return pl.ds(pl.multiple_of(first + r * step, 16), step)

    def each(part, rolled):
        if rolled:
            lax.fori_loop(0, sub, lambda r, carry: part(r) or carry, 0)
        else:
            for r in range(sub):
                part(r)

    def up(rolled=False):
        b1 = b_in_ref[:, pl.ds(pl.multiple_of(3 * d + i * hc, hc), hc)].astype(jnp.float32)[layer:layer + 1]

        def part(r):
            u = dot(h_ref[at_rows(r, row0), :], w1_ring[lax.rem(i, 2)])
            u_scr[at_rows(r), :] = (u + b1).astype(jnp.bfloat16)

        each(part, rolled)

    def gelu():
        act[...] = gelu_tanh(u_scr[...].astype(jnp.float32)).astype(jnp.bfloat16)

    def down(rolled=False):
        def part(r):
            y_acc[at_rows(r), :] += dot(act[at_rows(r), :], w2_ring[lax.rem(i + 1, 2)])

        each(part, rolled)

    @pl.when(i == 0)
    def _():
        h_copy.start()
        w1_copy(0).start()
        meet([device(1), device(X), device(Y)])
        h_copy.wait()
        for piece in (T_, A):
            near(own, piece, X).start()
        for piece in (T_, B):
            near(own, piece, Y).start()
        for piece in (T_, A, B):
            pair(own, piece).start()
        w1_copy(1).start()
        w2_copy(0).start()
        wt_copy.start()
        for j in range(2):
            gg[head_rows(j), :] = columns_of(gain_ref[0, j:j + 1, :])
        y_acc[...] = jnp.zeros_like(y_acc)
        w1_copy(i).wait()
        up(True)

    @pl.when((i > 0) & (i < n))
    def _():
        @pl.when(i + 1 < n)
        def _():
            w1_copy(i + 1).start()
        w2_copy(i).start()
        w2_copy(i - 1).wait()
        w1_copy(i).wait()
        gelu()
        up()
        down()

    @pl.when(i == n)
    def _():
        w2_copy(i - 1).wait()
        gelu()
        down(True)

    @pl.when(i == 1)
    def _():
        for j in range(3 * nh):
            bb[head_rows(j), :] = columns_of(b_in_ref[:, w_cols(j)].astype(jnp.float32)[layer:layer + 1])

    @pl.when(i == at_t)
    def _():
        landed_near(X, T_)
        near(X, T_, Y).start()
        near(own, A, Y).start()
        near(own, B, X).start()
        pair(X, T_).start()
        landed_near(Y, T_)
        pair(Y, T_).start()

    @pl.when(i == at_x)
    def _():
        landed_near(X, A)
        near(X, A, Y).start()
        pair(X, A).start()
        landed_near(Y, B)
        near(Y, B, X).start()
        pair(Y, B).start()
        landed_near(D, T_)
        pair(D, T_).start()
        landed_pair(own, T_, A, B)

    s = i - (n + 1)
    slot = lax.rem(i, 2)

    @pl.when(i == n)
    def _():
        landed_near(X, B)
        pair(X, B).start()
        landed_near(Y, A)
        pair(Y, A).start()
        landed_pair(X, T_, A)
        landed_pair(Y, T_, B)
        wt_copy.wait()
        fetch(0, 1 - slot)

    @pl.when(s == 0)
    def _():
        pltpu.make_async_copy(y_acc, y_hbm, y_sem).start()

    @pl.when(s == X)
    def _():
        landed_pair(X, B)
        landed_pair(Y, A)

    @pl.when((s >= 0) & (s < D - 1))
    def _():
        fetch(s + 1, 1 - slot)

    @pl.when(s == D - 1)
    def _():
        landed_pair(D, T_)
        fetch_text(1 - slot)

    @pl.when(s == D + 1)
    def _():
        landed_near(D, A)
        pair(D, A).start()
        landed_near(D, B)
        pair(D, B).start()
        fetch(D, slot)

    @pl.when(s == n_dev)
    def _():
        landed_pair(D, A, B)
        fetch(D + 1, slot)

    @pl.when(s >= 0)
    def _():
        image = s != D
        wait_for(hbuf.at[slot], h_sem.at[slot])

        @pl.when(image)
        def _():
            wait_for(tbuf.at[slot], t_sem.at[slot])
        h = hbuf[slot]
        table = jnp.concatenate([tbuf[slot, t] for t in range(tbuf.shape[1])], axis=1)
        cos, sin = jnp.where(image, table[:half], 1.0), jnp.where(image, table[half:], 0.0)

        def lanes(v):
            return jnp.concatenate([v] * (rb // LANES), axis=1)

        def proj(part):
            rs = slice(part * nh * LANES, (part + 1) * nh * LANES)
            return lax.dot_general(wt[rs, :], h, (((1,), (1,)), ((), ())), preferred_element_type=jnp.float32)

        def biased(x, j):
            return (x + lanes(bb[head_rows(j), :])).astype(jnp.bfloat16)

        def normed(x, j, g):
            x = biased(x, j).astype(jnp.float32)
            ms = jnp.sum(x * x, axis=0, keepdims=True) * (1.0 / LANES)
            v = x * lax.rsqrt(ms + EPS) * lanes(gg[head_rows(g), :])
            a, b = v[:half], v[half:]
            return jnp.concatenate([a * cos - b * sin, a * sin + b * cos], axis=0).astype(jnp.bfloat16)

        q = proj(0)
        for t in range(nh):
            v = normed(q[head_rows(t)], t, 0).astype(jnp.float32) * (LANES ** -0.5 * LOG2E)
            hi = v.astype(jnp.bfloat16)
            qT_ref[t, :LANES] = hi
            qT_ref[t, LANES:] = (v - hi.astype(jnp.float32)).astype(jnp.bfloat16)
        k = proj(1)
        for t in range(nh):
            k_ref[t] = normed(k[head_rows(t)], nh + t, 1).T
        v = proj(2)
        for t in range(nh):
            vT_ref[t] = biased(v[head_rows(t)], 2 * nh + t)

    @pl.when(s == n_dev)
    def _():
        for hop in hops:
            near(*hop).wait_send()
        for origin in (own, X, Y, D):
            for piece in (T_, A, B):
                pair(origin, piece).wait_send()
        wait_for(y_acc, y_sem)


def block(h, w_in, b_in, w_out, qk_gain, tables, wt, layer, n_txt, nh, row0, collective_id, hc=512):
    total, d = h.shape
    n_dev = d // LANES // nh
    ff = w_in.shape[2] - 3 * d
    n = ff // hc
    m = total - row0
    rb = total - n_txt
    assert n_dev * n_txt == rb
    S = n_dev * total
    hbm = pl.BlockSpec(memory_space=pl.ANY)
    dma = pltpu.SemaphoreType.DMA
    bf, f32 = jnp.bfloat16, jnp.float32
    far = n_dev - 2

    def at(i):
        s = jnp.clip(i - (n + 1), 0, n_dev)
        return s + 2 * (s // far) - 3 * (s // (far + 1))

    three = pltpu.SemaphoreType.DMA((12,))
    return pl.pallas_call(
        functools.partial(block_kernel, layer=layer, n=n, n_dev=n_dev, nh=nh, n_txt=n_txt, row0=row0, at_t=n // 4, at_x=n // 2),
        grid=(n + 1 + n_dev + 1,),
        in_specs=[whole(b_in.shape), pl.BlockSpec((1, 2, LANES), lambda i: (layer, 0, 0)), hbm, hbm, hbm, hbm, hbm],
        out_specs=[hbm, hbm, pl.BlockSpec((nh, 2 * LANES, rb), lambda i: (0, 0, at(i))), pl.BlockSpec((nh, rb, LANES), lambda i: (0, at(i), 0)),
                   pl.BlockSpec((nh, LANES, rb), lambda i: (0, 0, at(i)))],
        out_shape=[jax.ShapeDtypeStruct((m, d), f32), jax.ShapeDtypeStruct((n_dev, total, d), bf),
                   jax.ShapeDtypeStruct((nh, 2 * LANES, S), bf), jax.ShapeDtypeStruct((nh, S, LANES), bf), jax.ShapeDtypeStruct((nh, LANES, S), bf)],
        scratch_shapes=[
            pltpu.VMEM((total, d), bf), pltpu.VMEM((2, d, hc), bf), pltpu.VMEM((2, hc, d), bf),
            pltpu.VMEM((m, d), f32), pltpu.VMEM((m, hc), bf), pltpu.VMEM((m, hc), bf), pltpu.VMEM((3 * nh * LANES, d), bf),
            pltpu.VMEM((3 * nh * LANES, LANES), f32), pltpu.VMEM((2 * LANES, LANES), f32), pltpu.VMEM((2, rb, d), bf), pltpu.VMEM((2, *tables.shape[1:]), f32),
            dma, dma((2,)), dma((2,)), dma, dma((2,)), dma((2,)), dma, dma((9,)), dma((9,)), three, three,
        ],
        compiler_params=params(**talking(collective_id)),
        cost_estimate=pl.CostEstimate(flops=4 * m * d * ff + 6 * S * d * nh * LANES, bytes_accessed=4 * d * ff + 2 * S * d, transcendentals=m * ff),
        name='block',
    )(b_in, qk_gain, h, w_in, w_out, tables, wt)


def attend_kernel(qT_hbm, k_hbm, vT_hbm, w_hbm, bo_ref, mods_ref, *refs, layer, qt, kc, ck, ne, n_dev, n_txt, row0, last):
    if last:
        wf_ref, bf_ref, x_hbm, y_hbm, vel_hbm, *refs = refs
        *refs, vel, vown_sem, vsend_sem, vrecv_sem = refs
    else:
        x_hbm, y_hbm, xo_hbm, ho_hbm, *refs = refs
        *refs, tbuf, t_rows, tsend_sem, trecv_sem, out_sem = refs
    (qT_ref, k_ref, vT_ref, s_scr, m_scr, part_scr, acc_scr, l_scr, obuf, o_rows, w_ring, lhs, y_acc, xbuf, h_ring,
     in_sem, send_sem, recv_sem, w_sem, res_sem) = refs
    nh, S, hd = k_ref.shape
    n_img = o_rows.shape[2]
    R, d = y_acc.shape
    nk = S // kc
    n_ring = w_ring.shape[0]
    nc = d // ck
    ahead = 2
    f32, bf = jnp.float32, jnp.bfloat16
    cfg, z, core = lax.axis_index('cfg'), lax.axis_index('z'), lax.axis_index('core')
    me = cfg * N_CORE + core

    def load(t):
        pairs = ((qT_hbm, qT_ref), (k_hbm, k_ref), (vT_hbm, vT_ref))
        return [pltpu.make_async_copy(src.at[t], dst.at[t], in_sem.at[t, j]) for j, (src, dst) in enumerate(pairs)]

    def w_copy(c):
        slot = lax.rem(c, n_ring)
        return pltpu.make_async_copy(w_hbm.at[layer, pl.ds(pl.multiple_of(c * ck, ck), ck), :], w_ring.at[slot], w_sem.at[slot])

    residual = [pltpu.make_async_copy(y_hbm, y_acc, res_sem.at[0]), pltpu.make_async_copy(x_hbm.at[pl.ds(row0, R), :], xbuf, res_sem.at[1])]

    def device(r):
        to, c = related(cfg, core, r)
        return to, z, c

    for cp in load(0):
        cp.start()
    peers = [device(r) for r in range(1, n_dev)]
    if last:
        peers += [(z, e, core) for e in range(ne)] + [(e, cfg, core) for e in range(ne)]
    meet(peers)
    for cp in load(0):
        cp.wait()
    for t in range(1, nh):
        for cp in load(t):
            cp.start()

    def score_chunk(head, q, slot, i, m):
        rows = pl.ds(i * kc, kc)
        k = k_ref[head, rows, :]
        s = dot(jnp.concatenate([k, k], axis=1), q)
        s_scr[slot, rows, :] = s
        return jnp.maximum(m, jnp.max(s.reshape(kc // 8, 8, qt), axis=0))

    def lowest():
        return jnp.full((8, qt), -jnp.inf, f32)

    def full_max(m):
        return jnp.broadcast_to(jnp.max(m, axis=0, keepdims=True), (8, qt))

    def prob_chunk(head, m, slot, i, l, acc):
        rows = pl.ds(i * kc, kc)
        p = jnp.exp2(s_scr[slot, rows, :].reshape(kc // 8, 8, qt) - m[None])
        l = l + jnp.sum(p, axis=0)
        return l, acc + dot(vT_ref[head, :, rows], p.reshape(kc, qt).astype(bf))

    def load_q(tile):
        head, col = tile
        return qT_ref[head, :, pl.ds(pl.multiple_of(col, qt), qt)]

    def normalized(acc, l):
        return (acc / jnp.sum(l, axis=0, keepdims=True)).T.astype(bf)

    def stream(n_pairs, tile, buf, after, before):
        first, second = tile(0), tile(1)
        q, m = load_q(first), lowest()
        for i in range(nk):
            m = score_chunk(first[0], q, 0, i, m)
        m_scr[...] = full_max(m)
        q, m = load_q(second), lowest()
        for i in range(ahead):
            m = score_chunk(second[0], q, 1, i, m)
        part_scr[...] = m
        acc_scr[...] = jnp.zeros_like(acc_scr)
        l_scr[...] = jnp.ones_like(l_scr)

        def put(p, half, o):
            buf[p, half * qt:(half + 1) * qt, :] = o

        def pair(p, carry):
            before(p)
            later = lax.rem(p + 1, n_pairs)
            tiles = [tile(2 * p), tile(2 * p + 1), tile(2 * later), tile(2 * later + 1)]
            m, top = part_scr[...], m_scr[...]
            put(lax.rem(p + n_pairs - 1, n_pairs), 1, normalized(acc_scr[...], l_scr[...]))
            for half in range(2):
                l, acc = jnp.zeros((8, qt), f32), jnp.zeros((hd, qt), f32)
                q1, q2 = load_q(tiles[half + 1]), load_q(tiles[half + 2])
                for i in range(nk):
                    j = i + ahead
                    if j < nk:
                        m = score_chunk(tiles[half + 1][0], q1, 1 - half, j, m)
                    else:
                        if j == nk:
                            following, m = full_max(m), lowest()
                        m = score_chunk(tiles[half + 2][0], q2, half, j - nk, m)
                    l, acc = prob_chunk(tiles[half][0], top, half, i, l, acc)
                top = following
                if half == 0:
                    put(p, 0, normalized(acc, l))
                else:
                    acc_scr[...] = acc
                    l_scr[...] = l
            part_scr[...] = m
            m_scr[...] = top

            @pl.when(p > 0)
            def _():
                after(p - 1)
            return carry

        lax.fori_loop(0, n_pairs, pair, 0)
        put(n_pairs - 1, 1, normalized(acc_scr[...], l_scr[...]))
        after(n_pairs - 1)

    if not last:
        n_text = n_dev * n_txt
        assert n_text == 2 * qt

        def txt_send(head):
            for owner in range(n_dev):
                part = pl.ds(owner * n_txt, n_txt)
                if owner == 0:
                    t_rows[me, head] = tbuf[head, part, :]
                else:
                    remote(tbuf.at[head, part, :], t_rows.at[me, head], tsend_sem, trecv_sem, device(owner)).start()

        def txt_head(p):
            @pl.when(p < nh - 1)
            def _():
                for cp in load(p + 1):
                    cp.wait()

        stream(nh, lambda u: (u // 2, n_dev * n_img + lax.rem(u, 2) * qt), tbuf, txt_send, txt_head)

    def relation_of(p):
        return lax.rem(p + 1, n_dev)

    def img_tile(u):
        p = u // 2
        return p // n_dev, relation_of(p) * n_img + lax.rem(u, 2) * qt

    def img_send(p):
        head, owner = p // n_dev, relation_of(p)

        @pl.when(owner == 0)
        def _():
            o_rows[me, head] = obuf[p]

        @pl.when(owner != 0)
        def _():
            remote(obuf.at[p], o_rows.at[me, head], send_sem, recv_sem.at[head], device(owner)).start()

    def img_before(p):
        if last:
            @pl.when((relation_of(p) == 0) & (p < nh * n_dev - 1))
            def _():
                for cp in load(p // n_dev + 1):
                    cp.wait()

        @pl.when(p == 2)
        def _():
            for c in range(n_ring):
                w_copy(c).start()
            for cp in residual:
                cp.start()

    stream(nh * n_dev, img_tile, obuf, img_send, img_before)

    for cp in residual:
        cp.wait()
    others = pl.ds(0, n_dev - 1)
    if not last:
        wait_for(t_rows.at[others], trecv_sem)
    per = nc // nh
    wide = ck // LANES

    def chunk_of_w(c, carry):
        head = c // per

        @pl.when(lax.rem(c, per) == 0)
        def _():
            wait_for(o_rows.at[others, head], recv_sem.at[head])
        for t in range(wide):
            src = lax.rem(c, per) * wide + t
            if not last:
                lhs[:n_txt, head_rows(t)] = t_rows[src, head]
            lhs[R - n_img:, head_rows(t)] = o_rows[src, head]
        w_copy(c).wait()
        y_acc[...] += dot(lhs[...], w_ring[lax.rem(c, n_ring)])

        @pl.when(c + n_ring < nc)
        def _():
            w_copy(c + n_ring).start()
        return carry

    lax.fori_loop(0, nc, chunk_of_w, 0)

    gate_row = 3 * layer + 2
    gate, shift, scale = (mods_ref[r:r + 1, :] for r in range(gate_row, gate_row + 3))
    bo = bo_ref[...].astype(f32)[layer:layer + 1]
    er = R // ne
    sub = 16 if er % 16 == 0 else 8

    def put_rows(e, slot):
        rows = pl.ds(pl.multiple_of(e * er, sub), er)
        pltpu.make_async_copy(xbuf.at[rows, :], xo_hbm.at[rows, :], out_sem.at[2]).start()
        pltpu.make_async_copy(h_ring.at[slot], ho_hbm.at[rows, :], out_sem.at[slot]).start()

    def deliver(e):
        own = (z == cfg) & (e == z)

        @pl.when(own)
        def _():
            pltpu.make_async_copy(vel.at[e], vel_hbm.at[cfg], vown_sem).start()

        @pl.when(jnp.logical_not(own))
        def _():
            remote(vel.at[e], vel_hbm.at[cfg], vsend_sem.at[e], vrecv_sem.at[cfg], (z, e, core)).start()

    def rows_out(e, carry):
        slot = lax.rem(e, 2)
        if not last:
            @pl.when(e >= 2)
            def _():
                wait_for(h_ring.at[slot], out_sem.at[slot])

        def chunk(c, carry):
            rs = pl.ds(pl.multiple_of(e * er + c * sub, sub), sub)
            xn = (xbuf[rs, :].astype(f32) + gate * (y_acc[rs, :] + bo)).astype(bf)
            h_ring[slot, pl.ds(pl.multiple_of(c * sub, sub), sub), :] = ln_mod(xn.astype(f32), shift, scale)
            if not last:
                xbuf[rs, :] = xn
            return carry

        lax.fori_loop(0, er // sub, chunk, 0, unroll=3 if (er // sub) % 3 == 0 else 2)
        if last:
            w = jnp.concatenate([wf_ref[...], jnp.zeros((LANES - wf_ref.shape[0], d), bf)], axis=0)
            v = lax.dot_general(h_ring[slot], w, (((1,), (1,)), ((), ())), preferred_element_type=f32)
            b = bf_ref[...].astype(f32)
            vel[e] = v + jnp.concatenate([b, jnp.zeros((1, LANES - b.shape[1]), f32)], axis=1)
            deliver(e)
        else:
            put_rows(e, slot)
        return carry

    lax.fori_loop(0, ne, rows_out, 0)

    wait_for(o_rows.at[others], send_sem)
    if last:
        for e in range(ne):
            own = (z == cfg) & (e == z)

            @pl.when(own)
            def _():
                wait_for(vel.at[e], vown_sem)

            @pl.when(jnp.logical_not(own))
            def _():
                wait_for(vel.at[e], vsend_sem.at[e])
                wait_for(vel_hbm.at[e], vrecv_sem.at[e])
    else:
        wait_for(t_rows.at[others], tsend_sem)
        wait_for(xbuf, out_sem.at[2])
        for slot in range(2):
            wait_for(h_ring.at[slot], out_sem.at[slot])


def largest(n, cap, unit):
    return max(c for c in range(unit, cap + 1, unit) if n % c == 0)


def attend(qT, k, vT, w_out, b_out, mods, x, y_mlp, layer, n_dev, n_txt, row0, collective_id, final=None, ck=512, ne=4):
    nh, S, hd = k.shape
    R, d = y_mlp.shape
    n_img = S // n_dev - n_txt
    last = final is not None
    qt = n_img // 2
    dma = pltpu.SemaphoreType.DMA
    bf, f32 = jnp.bfloat16, jnp.float32
    hbm = pl.BlockSpec(memory_space=pl.ANY)
    stat = pltpu.VMEM((8, qt), f32)
    scratch = [pltpu.VMEM(v.shape, bf) for v in (qT, k, vT)] + [
        pltpu.VMEM((2, S, qt), f32), stat, stat, pltpu.VMEM((hd, qt), f32), stat, pltpu.VMEM((nh * n_dev, n_img, hd), bf), pltpu.VMEM((n_dev, nh, n_img, hd), bf),
        pltpu.VMEM((2, ck, d), bf), pltpu.VMEM((R, ck), bf), pltpu.VMEM((R, d), f32), pltpu.VMEM((R, d), bf), pltpu.VMEM((2, R // ne, d), bf),
        dma((nh, 3)), dma, dma((nh,)), dma((2,)), dma((2,))]
    if last:
        out_shape = jax.ShapeDtypeStruct((ne, R // ne, LANES), f32)
        scratch += [pltpu.VMEM(out_shape.shape, f32), dma, dma((ne,)), dma((ne,))]
    else:
        out_shape = [jax.ShapeDtypeStruct((R, d), bf)] * 2
        scratch += [pltpu.VMEM((nh, n_dev * n_txt, hd), bf), pltpu.VMEM((n_dev, nh, n_txt, hd), bf), dma, dma, dma((3,))]
    extra = list(final or ())
    return pl.pallas_call(
        functools.partial(attend_kernel, layer=layer, qt=qt, kc=largest(S, 768, 256), ck=ck, ne=ne, n_dev=n_dev, n_txt=n_txt, row0=row0, last=last),
        grid=(1,),
        in_specs=[hbm] * 4 + [whole(b_out.shape), whole(mods.shape)] + [whole(v.shape) for v in extra] + [hbm] * 2,
        out_specs=hbm if last else [hbm] * 2,
        out_shape=out_shape,
        scratch_shapes=scratch,
        compiler_params=params(**talking(collective_id)),
        cost_estimate=pl.CostEstimate(flops=6 * nh * n_dev * R * S * hd + 2 * R * d * d, bytes_accessed=8 * nh * S * hd + 2 * d * d + 14 * R * d, transcendentals=nh * S * n_dev * R),
        name='attend',
    )(qT, k, vT, w_out, b_out, mods, *extra, x, y_mlp)


def enter_kernel(xt_hbm, xi_hbm, cond_ref, wm_ref, wf_ref, bm_ref, bf_ref, cos_hbm, sin_hbm, w_in_hbm, mods_ref, xo_hbm, ho_hbm, tab_out, wt_hbm,
                 stage, xbuf, hbuf, cond_buf, s_scr, wbuf, turned, w_sem, wt_sem, out_sem,
                 cond_send, cond_recv, p_send, p_recv, c_send, c_recv, own_sem, t_send, t_recv, town_sem, q_send, q_recv, *, n_mod, n_steps, per_row, per_layer):
    i = pl.program_id(0)
    n, rows, d = xbuf.shape
    tp = xt_hbm.shape[0] // n
    ip = xi_hbm.shape[0] // n
    cfg, z, core = lax.axis_index('cfg'), lax.axis_index('z'), lax.axis_index('core')
    across = [related(cfg, core, r)[0] for r in range(2, 2 * n, 2)]
    heights = [lax.rem(z + s, n) for s in range(1, n)]
    plane = [(to, z, c) for to, c in (related(cfg, core, r) for r in range(1, 2 * n))]
    mine = tab_out.at[cfg * N_CORE + core]
    cut = rows // 2
    first = (cut // 2 + 7) // 8 * 8
    spans = ((0, first), (first, cut - first), (cut, first), (cut + first, cut - first))

    def piece_refs(j, dst):
        out = []
        for at, size in spans:
            head = [(xt_hbm.at[pl.ds(j * tp, tp), :], dst.at[pl.ds(0, tp), :])] if at == 0 else []
            skip = tp if at == 0 else 0
            out.append(head + [(xi_hbm.at[pl.ds(j * ip + at + skip - tp, size - skip), :], dst.at[pl.ds(at + skip, size - skip), :])])
        return out

    def tables(to):
        half = cos_hbm.shape[0]
        cols = pl.ds(pl.multiple_of(cfg * ip, ip), ip)
        return [(src.at[:, cols], to.at[pl.ds(t * half, half), :]) for t, src in enumerate((cos_hbm, sin_hbm))]

    def forward(group, t, part):
        at = pl.ds(*spans[part])

        @pl.when(group == z)
        def _():
            xbuf[z, at, :] = stage[group, at, :]

        @pl.when(group != z)
        def _():
            remote(stage.at[group, at, :], xbuf.at[z, at, :], c_send.at[t], c_recv.at[z], (cfg, group, core)).start()

    def silu_of(ref):
        v = ref[...].astype(jnp.float32)
        s_scr[...] = jnp.broadcast_to((v * jax.nn.sigmoid(v)).astype(jnp.bfloat16), s_scr.shape)

    @pl.when(i == 0)
    def _():
        meet(plane + [(cfg, h, core) for h in heights])

        @pl.when(cfg == z)
        def _():
            for t, j in enumerate(across):
                remote(cond_ref, cond_buf, cond_send.at[t], cond_recv, (j, z, core)).start()
        for part in range(len(spans)):
            for t, j in ((0, across[0]), (2, across[2]), (1, across[1])):
                for src, dst in piece_refs(j, stage.at[cfg])[part]:
                    remote(src, dst, p_send.at[t], p_recv.at[cfg, part], (j, z, core)).start()
        held = sum(piece_refs(cfg, xbuf.at[z]), [])

        @pl.when(cfg == z)
        def _():
            for src, dst in held:
                pltpu.make_async_copy(src, dst, own_sem).start()

        @pl.when(cfg != z)
        def _():
            for src, dst in held:
                remote(src, dst, c_send.at[n - 1], c_recv.at[z], (cfg, cfg, core)).start()
        for t, h in enumerate(heights):
            for src, dst in tables(mine.at[z]):
                remote(src, dst, t_send.at[t], t_recv.at[z], (cfg, h, core)).start()
        for src, dst in tables(mine.at[z]):
            pltpu.make_async_copy(src, dst, town_sem).start()

        @pl.when(cfg == z)
        def _():
            silu_of(cond_ref)

        @pl.when(cfg != z)
        def _():
            remote(cond_ref, cond_buf, cond_send.at[0], cond_recv, (cfg, z, core)).wait_recv()
            silu_of(cond_buf)

    row, col = i // per_row, lax.rem(i, per_row)
    width = wm_ref.shape[2]
    cols = pl.ds(pl.multiple_of(col * width, width), width)

    @pl.when(i < n_mod)
    def _():
        v = dot(s_scr[...], wm_ref[0])
        b = bm_ref[...].astype(jnp.float32)
        of_layer = lax.broadcasted_iota(jnp.int32, b.shape, 0) == i // per_layer
        mods_ref[pl.ds(row, 1), cols] = v[0:1] + jnp.sum(jnp.where(of_layer, b, 0.0), axis=0, keepdims=True)

    @pl.when(i >= n_mod)
    def _():
        v = dot(s_scr[...], wf_ref[...])
        mods_ref[pl.ds(row, 1), cols] = v[0:1] + bf_ref[...].astype(jnp.float32)

    def arrived(t, part):
        j = across[t]
        wait_for(stage.at[j, pl.ds(*spans[part]), :], p_recv.at[j, part])
        forward(j, t, part)

    @pl.when(i == n_steps - 2)
    def _():
        for h in heights:
            wait_for(mine.at[h], t_recv.at[h])
        wait_for(mine.at[z], town_sem)
        for peer in plane:
            remote(mine, mine, q_send, q_recv, peer).start()

    for part in range(len(spans)):
        due = 7 + 9 * part

        @pl.when(i == due)
        def _():
            arrived(0, part)

        @pl.when(i == due + 6)
        def _():
            arrived(2, part)
            arrived(1, part)

    @pl.when(i == n_steps - 1)
    def _():
        shift, scale = mods_ref[0:1, :], mods_ref[1:2, :]

        @pl.when(cfg == z)
        def _():
            wait_for(xbuf.at[z], own_sem)

        d_in, heads = w_in_hbm.shape[1] // LANES, wt_hbm.shape[1] // LANES

        def w_copy(j):
            layer, b = j // heads, lax.rem(j, heads)
            nh = heads // 3
            col = (b // nh * d_in + lax.rem(b, nh) * (d_in // nh) + cfg * N_CORE + core) * LANES
            return pltpu.make_async_copy(w_in_hbm.at[layer, :, pl.ds(pl.multiple_of(col, LANES), LANES)], wbuf.at[lax.rem(j, 2)], w_sem.at[lax.rem(j, 2)])

        def turn(j, carry):
            slot = lax.rem(j, 2)
            w_copy(j).wait()

            @pl.when(j > 1)
            def _():
                wait_for(turned.at[slot], wt_sem.at[slot])
            turned[slot] = wbuf[slot].T

            @pl.when(j + 2 < n_turns)
            def _():
                w_copy(j + 2).start()
            to = pl.ds(pl.multiple_of(lax.rem(j, heads) * LANES, LANES), LANES)
            pltpu.make_async_copy(turned.at[slot], wt_hbm.at[j // heads, to, :], wt_sem.at[slot]).start()
            return carry

        n_turns = wt_hbm.shape[0] * heads
        w_copy(0).start()
        w_copy(1).start()
        lax.fori_loop(0, n_turns, turn, 0)

        def height(s, carry):
            k = lax.rem(z + s, n)

            @pl.when(s > 0)
            def _():
                wait_for(xbuf.at[k], c_recv.at[k])
            sub = 16 if rows % 16 == 0 else 8

            def chunk(c, carry):
                at = pl.ds(pl.multiple_of(c * sub, sub), sub)
                hbuf[k, at, :] = ln_mod(xbuf[k, at, :].astype(jnp.float32), shift, scale)
                return carry

            lax.fori_loop(0, rows // sub, chunk, 0, unroll=3)
            for t, (src, dst) in enumerate(((xbuf, xo_hbm), (hbuf, ho_hbm))):
                for at, size, to in ((0, tp, k * tp), (tp, ip, n * tp + k * ip)):
                    pltpu.make_async_copy(src.at[k, pl.ds(at, size), :], dst.at[pl.ds(to, size), :], out_sem.at[t]).start()
            return carry

        lax.fori_loop(0, n, height, 0)
        for slot in range(2):
            wait_for(turned.at[slot], wt_sem.at[slot])
        wait_for(xbuf, out_sem.at[0])
        wait_for(hbuf, out_sem.at[1])

        for t, j in enumerate(across):
            wait_for(xbuf.at[0], p_send.at[t])

            @pl.when(j != z)
            def _():
                wait_for(xbuf.at[0], c_send.at[t])

        @pl.when(cfg != z)
        def _():
            wait_for(xbuf.at[0], c_send.at[n - 1])

        @pl.when(cfg == z)
        def _():
            for t, j in enumerate(across):
                remote(cond_ref, cond_buf, cond_send.at[t], cond_recv, (j, z, core)).wait_send()
        for t, h in enumerate(heights):
            wait_for(mine.at[h], t_send.at[t])
        others = tab_out.at[pl.ds(0, 2 * n - 1)]
        wait_for(others, q_send)
        wait_for(others, q_recv)


def enter(x_txt, x_img, cond, w_mod, w_fmod, b_mod, b_fmod, cosT, sinT, w_in, nh, n, collective_id, width=512):
    n_txt, d = x_txt.shape
    n_img = x_img.shape[0]
    total = n_txt + n_img
    rows = total // n
    n_layers, _, dm = w_mod.shape
    per_layer, n_fin, per_row = dm // width, w_fmod.shape[1] // width, d // width
    n_mod = n_layers * per_layer
    steps = n_mod + n_fin
    dma = pltpu.SemaphoreType.DMA
    bf, f32 = jnp.bfloat16, jnp.float32

    def layer_of(i):
        j = jnp.minimum(i, n_mod - 1)
        return j // per_layer, lax.rem(j, per_layer)

    def last_of(i):
        return 0, jnp.maximum(i - n_mod, 0)

    hbm = pl.BlockSpec(memory_space=pl.ANY)
    out_shape = [jax.ShapeDtypeStruct((steps // per_row, d), f32), jax.ShapeDtypeStruct((total, d), bf), jax.ShapeDtypeStruct((total, d), bf),
                 jax.ShapeDtypeStruct((N_CORE * n, n, 2 * cosT.shape[0], n_img // n), f32),
                 jax.ShapeDtypeStruct((n_layers, 3 * nh * LANES, d), bf)]
    return pl.pallas_call(
        functools.partial(enter_kernel, n_mod=n_mod, n_steps=steps, per_row=per_row, per_layer=per_layer),
        grid=(steps,),
        in_specs=[hbm, hbm, whole(cond.shape), pl.BlockSpec((1, d, width), lambda i: (layer_of(i)[0], 0, layer_of(i)[1])), pl.BlockSpec((d, width), last_of),
                  pl.BlockSpec((n_layers, width), lambda i: (0, layer_of(i)[1])), pl.BlockSpec((1, width), last_of), hbm, hbm, hbm],
        out_specs=[whole(out_shape[0].shape)] + [hbm] * 4,
        out_shape=out_shape,
        scratch_shapes=[pltpu.VMEM((n, rows, d), bf)] * 3 + [pltpu.VMEM(cond.shape, bf), pltpu.VMEM((16, d), bf), pltpu.VMEM((2, d, LANES), bf), pltpu.VMEM((2, LANES, d), bf),
                        dma((2,)), dma((2,)), dma((2,)), dma((n - 1,)), dma, dma((n - 1,)), dma((n, 4)), dma((n,)), dma((n,)), dma, dma((n - 1,)), dma((n,)), dma, dma, dma],
        compiler_params=params(**talking(collective_id)),
        cost_estimate=pl.CostEstimate(flops=2 * 16 * d * width * steps, bytes_accessed=2 * d * width * steps, transcendentals=0),
        name='enter',
    )(x_txt, x_img, cond, w_mod, w_fmod, b_mod, b_fmod, cosT, sinT, w_in)


def solution(mesh):
    n_cfg = mesh.devices.shape[0]
    n_z = mesh.devices.shape[1] // N_CORE
    grid = Mesh(mesh.devices.reshape(n_cfg, n_z, N_CORE), ('cfg', 'z', 'core'))
    assert n_cfg == n_z == 4
    n_dev = n_cfg * N_CORE
    token_spec = P(('cfg', 'z', 'core'), None)
    seq_spec = P(('z', 'core'), None)
    in_specs = (token_spec, token_spec, P('cfg', None), seq_spec, seq_spec, token_spec) + (P(),) * 13

    def body(x_txt, x_img, cond_vec, cos_img, sin_img, z_lat, t_cur, t_next, w_mod, b_mod, w_in, b_in, qk_gain, w_out, b_out, w_fmod, b_fmod, w_final, b_final):
        n_txt, d = x_txt.shape
        n_img = x_img.shape[0]
        n_layers = w_mod.shape[0]
        nh = d // LANES // n_dev
        n_out = w_final.shape[1]

        mods, x, h, tables, wt = enter(x_txt, x_img, cond_vec, w_mod, w_fmod, b_mod, b_fmod[None], cos_img.T, sin_img.T, w_in, nh, n_cfg, 1)
        for l in range(n_layers):
            last = l == n_layers - 1
            row0 = n_txt if last else 0
            y_mlp, _, qT, k, vT = block(h, w_in, b_in, w_out, qk_gain, tables, wt, l, n_txt, nh, row0, 2 + 2 * l)
            final = (w_final.T, b_final[None]) if last else None
            done = attend(qT, k, vT, w_out, b_out, mods, x, y_mlp, l, n_dev, n_txt, row0, 3 + 2 * l, final)
            if not last:
                x, h = done

        return z_lat + (t_next - t_cur) * done.reshape(n_img, LANES)[:, :n_out]

    return jax.shard_map(body, mesh=grid, in_specs=in_specs, out_specs=token_spec, check_vma=False)
```

```python
import functools
import math

import jax
import jax.numpy as jnp
from jax import lax
from jax.experimental import pallas as pl
from jax.experimental.pallas import tpu as pltpu
from jax.sharding import Mesh, PartitionSpec as P

EPS = 1e-6
LANES = 128
GELU_C = math.sqrt(2.0 / math.pi)
LOG2E = math.log2(math.e)
VMEM_BYTES = 60 * 2**20
N_CORE = 2
MESH = pl.DeviceIdType.MESH


def params(**kw):
    return pltpu.CompilerParams(vmem_limit_bytes=VMEM_BYTES, dimension_semantics=('arbitrary',), **kw)


def talking(collective_id):
    return dict(collective_id=collective_id, has_side_effects=True)


def whole(shape, **kw):
    return pl.BlockSpec(shape, lambda i: (0,) * len(shape), **kw)


def head_rows(j):
    return slice(j * LANES, (j + 1) * LANES)


def columns_of(v):
    return jnp.broadcast_to(v.astype(jnp.float32), (LANES, LANES)).T


def wait_for(ref, sem):
    pltpu.make_async_copy(ref, ref, sem).wait()


def dot(a, b):
    return jnp.dot(a, b, preferred_element_type=jnp.float32)


def remote(src, dst, send_sem, recv_sem, device):
    return pltpu.make_async_remote_copy(src_ref=src, dst_ref=dst, send_sem=send_sem, recv_sem=recv_sem, device_id=device, device_id_type=MESH)


def meet(devices):
    barrier = pltpu.get_barrier_semaphore()
    for device in devices:
        pl.semaphore_signal(barrier, inc=1, device_id=device, device_id_type=MESH)
    pl.semaphore_wait(barrier, len(devices))


def ln_mod(x, shift, scale):
    centered = x - jnp.mean(x, axis=-1, keepdims=True)
    var = jnp.mean(centered * centered, axis=-1, keepdims=True)
    return (centered * lax.rsqrt(var + EPS) * (1.0 + scale) + shift).astype(jnp.bfloat16)


def gelu_tanh(u):
    return u * (0.5 * (1.0 + jnp.tanh(GELU_C * (u + 0.044715 * (u * u * u)))))


def related(cfg, core, r):
    cx, cy = cfg // 2, lax.rem(cfg, 2)
    x = lax.rem(cx + lax.rem(r // 2, 2), 2)
    y = lax.rem(cy + r // 4, 2)
    return x * 2 + y, lax.rem(core + lax.rem(r, 2), 2)


def block_kernel(b_in_ref, gain_ref, h_hbm, w_in_hbm, w_out_hbm, T, wt_hbm, y_hbm, H, qT_ref, k_ref, vT_ref, h_ref, w1_ring, w2_ring, y_acc, u_scr, act, wt, bb, gg, hbuf, tbuf,
                 h_own_sem, w1_sem, w2_sem, w_sem, h_sem, t_sem, y_sem, near_send, near_recv, pair_send, pair_recv, *, layer, n, n_dev, nh, n_txt, row0, at_t, at_x):
    i = pl.program_id(0)
    cfg, z, core = lax.axis_index('cfg'), lax.axis_index('z'), lax.axis_index('core')
    rows = y_acc.shape[0]
    total, d = h_hbm.shape
    hc = u_scr.shape[1]
    rb = total - n_txt
    half = LANES // 2
    n_heads = d // LANES
    stride = n_heads // nh

    def device(r):
        to, c = related(cfg, core, r)
        return to, z, c

    def slot_of(r):
        to, c = related(cfg, core, r)
        return to * N_CORE + c

    own, X, Y, D = range(0, n_dev, 2)
    T_, A, B = range(3)
    a_rows = (rb - n_txt) // 2
    spans = ((0, n_txt), (n_txt, a_rows), (n_txt + a_rows, rb - a_rows))
    hops = [(own, T_, X), (own, A, X), (own, B, X), (Y, B, X), (own, T_, Y), (own, B, Y), (own, A, Y), (X, T_, Y), (X, A, Y)]

    def at_core(origin, piece):
        return H.at[slot_of(origin), pl.ds(*spans[piece]), :]

    def move(origin, piece, to, send_sem, recv_sem):
        src = h_hbm.at[pl.ds(*spans[piece]), :] if origin == own else at_core(origin, piece)
        return remote(src, at_core(origin, piece), send_sem, recv_sem, device(to))

    def near(origin, piece, to):
        k = ((origin ^ to) // 2 - 1) * 3 + piece
        return move(origin, piece, to, near_send.at[hops.index((origin, piece, to))], near_recv.at[k])

    def pair(origin, piece):
        k = origin // 2 * 3 + piece
        return move(origin, piece, 1, pair_send.at[k], pair_recv.at[k])

    def landed_near(origin, piece):
        wait_for(at_core(origin, piece), near_recv.at[(origin // 2 - 1) * 3 + piece])

    def landed_pair(origin, *pieces):
        for piece in pieces:
            wait_for(at_core(origin + 1, piece), pair_recv.at[origin // 2 * 3 + piece])

    h_copy = pltpu.make_async_copy(h_hbm, h_ref, h_own_sem)

    def w1_copy(j):
        cols = pl.ds(pl.multiple_of(3 * d + j * hc, hc), hc)
        return pltpu.make_async_copy(w_in_hbm.at[layer, :, cols], w1_ring.at[lax.rem(j, 2)], w1_sem.at[lax.rem(j, 2)])

    def w2_copy(j):
        at = pl.ds(pl.multiple_of(d + j * hc, hc), hc)
        return pltpu.make_async_copy(w_out_hbm.at[layer, at, :], w2_ring.at[lax.rem(j, 2)], w2_sem.at[lax.rem(j, 2)])

    def w_cols(j):
        col = (j // nh * n_heads + lax.rem(j, nh) * stride + cfg * N_CORE + core) * LANES
        return pl.ds(pl.multiple_of(col, LANES), LANES)

    wt_copy = pltpu.make_async_copy(wt_hbm.at[layer], wt, w_sem)

    def fetch(r, slot):
        pltpu.make_async_copy(T.at[slot_of(r)], tbuf.at[slot], t_sem.at[slot]).start()

        @pl.when(r == 0)
        def _():
            pltpu.make_async_copy(h_hbm.at[pl.ds(n_txt, rb), :], hbuf.at[slot], h_sem.at[slot]).start()

        @pl.when(r > 0)
        def _():
            pltpu.make_async_copy(H.at[slot_of(r), pl.ds(n_txt, rb), :], hbuf.at[slot], h_sem.at[slot]).start()

    def fetch_text(slot):
        for r in range(n_dev):
            src = at_core(r, T_) if r else h_hbm.at[pl.ds(0, n_txt), :]
            pltpu.make_async_copy(src, hbuf.at[slot, pl.ds(r * n_txt, n_txt), :], h_sem.at[slot]).start()

    sub = 2
    step = rows // sub

    def at_rows(r, first=0):
        return pl.ds(pl.multiple_of(first + r * step, 16), step)

    def each(part, rolled):
        if rolled:
            lax.fori_loop(0, sub, lambda r, carry: part(r) or carry, 0)
        else:
            for r in range(sub):
                part(r)

    def up(rolled=False):
        b1 = b_in_ref[:, pl.ds(pl.multiple_of(3 * d + i * hc, hc), hc)].astype(jnp.float32)[layer:layer + 1]

        def part(r):
            u = dot(h_ref[at_rows(r, row0), :], w1_ring[lax.rem(i, 2)])
            u_scr[at_rows(r), :] = (u + b1).astype(jnp.bfloat16)

        each(part, rolled)

    def gelu():
        act[...] = gelu_tanh(u_scr[...].astype(jnp.float32)).astype(jnp.bfloat16)

    def down(rolled=False):
        def part(r):
            y_acc[at_rows(r), :] += dot(act[at_rows(r), :], w2_ring[lax.rem(i + 1, 2)])

        each(part, rolled)

    @pl.when(i == 0)
    def _():
        w1_copy(0).start()
        h_copy.start()
        meet([device(1), device(X), device(Y)])
        for piece in (T_, A):
            near(own, piece, X).start()
        for piece in (T_, B):
            near(own, piece, Y).start()
        for piece in (T_, A, B):
            pair(own, piece).start()
        w1_copy(1).start()
        w2_copy(0).start()
        wt_copy.start()
        for j in range(2):
            gg[head_rows(j), :] = columns_of(gain_ref[0, j:j + 1, :])
        y_acc[...] = jnp.zeros_like(y_acc)
        h_copy.wait()
        w1_copy(i).wait()
        up(True)

    @pl.when((i > 0) & (i < n))
    def _():
        @pl.when(i + 1 < n)
        def _():
            w1_copy(i + 1).start()
        w2_copy(i).start()
        w2_copy(i - 1).wait()
        w1_copy(i).wait()
        gelu()
        up()
        down()

    @pl.when(i == n)
    def _():
        w2_copy(i - 1).wait()
        gelu()
        down(True)

    @pl.when(i == 1)
    def _():
        for j in range(3 * nh):
            bb[head_rows(j), :] = columns_of(b_in_ref[:, w_cols(j)].astype(jnp.float32)[layer:layer + 1])

    @pl.when(i == at_t)
    def _():
        landed_near(X, T_)
        near(X, T_, Y).start()
        near(own, A, Y).start()
        near(own, B, X).start()
        pair(X, T_).start()
        landed_near(Y, T_)
        pair(Y, T_).start()

    @pl.when(i == at_x)
    def _():
        landed_near(X, A)
        near(X, A, Y).start()
        pair(X, A).start()
        landed_near(Y, B)
        near(Y, B, X).start()
        pair(Y, B).start()
        landed_near(D, T_)
        pair(D, T_).start()
        landed_pair(own, T_, A, B)

    s = i - (n + 1)
    slot = lax.rem(i, 2)

    @pl.when(i == n)
    def _():
        landed_pair(X, T_, A)
        landed_pair(Y, T_, B)
        wt_copy.wait()
        fetch(0, 1 - slot)

    @pl.when(s == 0)
    def _():
        pltpu.make_async_copy(y_acc, y_hbm, y_sem).start()
        landed_near(X, B)
        pair(X, B).start()
        landed_near(Y, A)
        pair(Y, A).start()

    @pl.when(s == X)
    def _():
        landed_pair(X, B)
        landed_pair(Y, A)

    @pl.when((s >= 0) & (s < D - 1))
    def _():
        fetch(s + 1, 1 - slot)

    @pl.when(s == D - 1)
    def _():
        landed_pair(D, T_)
        fetch_text(1 - slot)

    @pl.when(s == D + 1)
    def _():
        landed_near(D, A)
        pair(D, A).start()
        landed_near(D, B)
        pair(D, B).start()
        fetch(D, slot)

    @pl.when(s == n_dev)
    def _():
        landed_pair(D, A, B)
        fetch(D + 1, slot)

    @pl.when(s >= 0)
    def _():
        image = s != D
        wait_for(hbuf.at[slot], h_sem.at[slot])

        @pl.when(image)
        def _():
            wait_for(tbuf.at[slot], t_sem.at[slot])
        h = hbuf[slot]
        table = jnp.concatenate([tbuf[slot, t] for t in range(tbuf.shape[1])], axis=1)
        cos, sin = jnp.where(image, table[:half], 1.0), jnp.where(image, table[half:], 0.0)

        def lanes(v):
            return jnp.concatenate([v] * (rb // LANES), axis=1)

        def proj(part):
            rs = slice(part * nh * LANES, (part + 1) * nh * LANES)
            return lax.dot_general(wt[rs, :], h, (((1,), (1,)), ((), ())), preferred_element_type=jnp.float32)

        def biased(x, j):
            return (x + lanes(bb[head_rows(j), :])).astype(jnp.bfloat16)

        def normed(x, j, g):
            x = biased(x, j).astype(jnp.float32)
            ms = jnp.sum(x * x, axis=0, keepdims=True) * (1.0 / LANES)
            v = x * lax.rsqrt(ms + EPS) * lanes(gg[head_rows(g), :])
            a, b = v[:half], v[half:]
            return jnp.concatenate([a * cos - b * sin, a * sin + b * cos], axis=0).astype(jnp.bfloat16)

        q = proj(0)
        for t in range(nh):
            v = normed(q[head_rows(t)], t, 0).astype(jnp.float32) * (LANES ** -0.5 * LOG2E)
            hi = v.astype(jnp.bfloat16)
            qT_ref[t, :LANES] = hi
            qT_ref[t, LANES:] = (v - hi.astype(jnp.float32)).astype(jnp.bfloat16)
        k = proj(1)
        for t in range(nh):
            k_ref[t] = normed(k[head_rows(t)], nh + t, 1).T
        v = proj(2)
        for t in range(nh):
            vT_ref[t] = biased(v[head_rows(t)], 2 * nh + t)

    @pl.when(s == n_dev)
    def _():
        for hop in hops:
            near(*hop).wait_send()
        for origin in (own, X, Y, D):
            for piece in (T_, A, B):
                pair(origin, piece).wait_send()
        wait_for(y_acc, y_sem)


def block(h, w_in, b_in, w_out, qk_gain, tables, wt, layer, n_txt, nh, row0, collective_id, hc=512):
    total, d = h.shape
    n_dev = d // LANES // nh
    ff = w_in.shape[2] - 3 * d
    n = ff // hc
    m = total - row0
    rb = total - n_txt
    assert n_dev * n_txt == rb
    S = n_dev * total
    hbm = pl.BlockSpec(memory_space=pl.ANY)
    dma = pltpu.SemaphoreType.DMA
    bf, f32 = jnp.bfloat16, jnp.float32
    far = n_dev - 2

    def at(i):
        s = jnp.clip(i - (n + 1), 0, n_dev)
        return s + 2 * (s // far) - 3 * (s // (far + 1))

    three = pltpu.SemaphoreType.DMA((12,))
    return pl.pallas_call(
        functools.partial(block_kernel, layer=layer, n=n, n_dev=n_dev, nh=nh, n_txt=n_txt, row0=row0, at_t=n // 4, at_x=n // 2 + 1),
        grid=(n + 1 + n_dev + 1,),
        in_specs=[whole(b_in.shape), pl.BlockSpec((1, 2, LANES), lambda i: (layer, 0, 0)), hbm, hbm, hbm, hbm, hbm],
        out_specs=[hbm, hbm, pl.BlockSpec((nh, 2 * LANES, rb), lambda i: (0, 0, at(i))), pl.BlockSpec((nh, rb, LANES), lambda i: (0, at(i), 0)),
                   pl.BlockSpec((nh, LANES, rb), lambda i: (0, 0, at(i)))],
        out_shape=[jax.ShapeDtypeStruct((m, d), f32), jax.ShapeDtypeStruct((n_dev, total, d), bf),
                   jax.ShapeDtypeStruct((nh, 2 * LANES, S), bf), jax.ShapeDtypeStruct((nh, S, LANES), bf), jax.ShapeDtypeStruct((nh, LANES, S), bf)],
        scratch_shapes=[
            pltpu.VMEM((total, d), bf), pltpu.VMEM((2, d, hc), bf), pltpu.VMEM((2, hc, d), bf),
            pltpu.VMEM((m, d), f32), pltpu.VMEM((m, hc), bf), pltpu.VMEM((m, hc), bf), pltpu.VMEM((3 * nh * LANES, d), bf),
            pltpu.VMEM((3 * nh * LANES, LANES), f32), pltpu.VMEM((2 * LANES, LANES), f32), pltpu.VMEM((2, rb, d), bf), pltpu.VMEM((2, *tables.shape[1:]), f32),
            dma, dma((2,)), dma((2,)), dma, dma((2,)), dma((2,)), dma, dma((9,)), dma((9,)), three, three,
        ],
        compiler_params=params(**talking(collective_id)),
        cost_estimate=pl.CostEstimate(flops=4 * m * d * ff + 6 * S * d * nh * LANES, bytes_accessed=4 * d * ff + 2 * S * d, transcendentals=m * ff),
        name='block',
    )(b_in, qk_gain, h, w_in, w_out, tables, wt)


def attend_kernel(qT_hbm, k_hbm, vT_hbm, w_hbm, bo_ref, mods_ref, *refs, layer, qt, kc, ck, ne, n_dev, n_txt, row0, last):
    if last:
        wf_ref, bf_ref, x_hbm, y_hbm, vel_hbm, *refs = refs
        *refs, vel, vown_sem, vsend_sem, vrecv_sem = refs
    else:
        x_hbm, y_hbm, xo_hbm, ho_hbm, *refs = refs
        *refs, tbuf, t_rows, tsend_sem, trecv_sem, out_sem = refs
    (qT_ref, k_ref, vT_ref, s_scr, m_scr, part_scr, acc_scr, l_scr, obuf, o_rows, w_ring, lhs, y_acc, xbuf, h_ring,
     in_sem, send_sem, recv_sem, w_sem, res_sem) = refs
    nh, S, hd = k_ref.shape
    n_img = o_rows.shape[2]
    R, d = y_acc.shape
    nk = S // kc
    n_ring = w_ring.shape[0]
    nc = d // ck
    ahead = 2
    f32, bf = jnp.float32, jnp.bfloat16
    cfg, z, core = lax.axis_index('cfg'), lax.axis_index('z'), lax.axis_index('core')
    me = cfg * N_CORE + core

    def load(t):
        pairs = ((qT_hbm, qT_ref), (k_hbm, k_ref), (vT_hbm, vT_ref))
        return [pltpu.make_async_copy(src.at[t], dst.at[t], in_sem.at[t, j]) for j, (src, dst) in enumerate(pairs)]

    def w_copy(c):
        slot = lax.rem(c, n_ring)
        return pltpu.make_async_copy(w_hbm.at[layer, pl.ds(pl.multiple_of(c * ck, ck), ck), :], w_ring.at[slot], w_sem.at[slot])

    residual = [pltpu.make_async_copy(y_hbm, y_acc, res_sem.at[0]), pltpu.make_async_copy(x_hbm.at[pl.ds(row0, R), :], xbuf, res_sem.at[1])]

    def device(r):
        to, c = related(cfg, core, r)
        return to, z, c

    for cp in load(0):
        cp.start()
    peers = [device(r) for r in range(1, n_dev)]
    if last:
        peers += [(z, e, core) for e in range(ne)] + [(e, cfg, core) for e in range(ne)]
    meet(peers)
    for cp in load(0):
        cp.wait()
    for t in range(1, nh):
        for cp in load(t):
            cp.start()

    def score_chunk(head, q, slot, i, m):
        rows = pl.ds(i * kc, kc)
        k = k_ref[head, rows, :]
        s = dot(jnp.concatenate([k, k], axis=1), q)
        s_scr[slot, rows, :] = s
        return jnp.maximum(m, jnp.max(s.reshape(kc // 8, 8, qt), axis=0))

    def lowest():
        return jnp.full((8, qt), -jnp.inf, f32)

    def full_max(m):
        return jnp.broadcast_to(jnp.max(m, axis=0, keepdims=True), (8, qt))

    def prob_chunk(head, m, slot, i, l, acc):
        rows = pl.ds(i * kc, kc)
        p = jnp.exp2(s_scr[slot, rows, :].reshape(kc // 8, 8, qt) - m[None])
        l = l + jnp.sum(p, axis=0)
        return l, acc + dot(vT_ref[head, :, rows], p.reshape(kc, qt).astype(bf))

    def load_q(tile):
        head, col = tile
        return qT_ref[head, :, pl.ds(pl.multiple_of(col, qt), qt)]

    def normalized(acc, l):
        return (acc / jnp.sum(l, axis=0, keepdims=True)).T.astype(bf)

    def stream(n_pairs, tile, buf, after, before):
        first, second = tile(0), tile(1)
        q, m = load_q(first), lowest()
        for i in range(nk):
            m = score_chunk(first[0], q, 0, i, m)
        m_scr[...] = full_max(m)
        q, m = load_q(second), lowest()
        for i in range(ahead):
            m = score_chunk(second[0], q, 1, i, m)
        part_scr[...] = m
        acc_scr[...] = jnp.zeros_like(acc_scr)
        l_scr[...] = jnp.ones_like(l_scr)

        def put(p, half, o):
            buf[p, half * qt:(half + 1) * qt, :] = o

        def pair(p, carry):
            before(p)
            later = lax.rem(p + 1, n_pairs)
            tiles = [tile(2 * p), tile(2 * p + 1), tile(2 * later), tile(2 * later + 1)]
            m, top = part_scr[...], m_scr[...]
            put(lax.rem(p + n_pairs - 1, n_pairs), 1, normalized(acc_scr[...], l_scr[...]))
            for half in range(2):
                l, acc = jnp.zeros((8, qt), f32), jnp.zeros((hd, qt), f32)
                q1, q2 = load_q(tiles[half + 1]), load_q(tiles[half + 2])
                for i in range(nk):
                    j = i + ahead
                    if j < nk:
                        m = score_chunk(tiles[half + 1][0], q1, 1 - half, j, m)
                    else:
                        if j == nk:
                            following, m = full_max(m), lowest()
                        m = score_chunk(tiles[half + 2][0], q2, half, j - nk, m)
                    l, acc = prob_chunk(tiles[half][0], top, half, i, l, acc)
                top = following
                if half == 0:
                    put(p, 0, normalized(acc, l))
                else:
                    acc_scr[...] = acc
                    l_scr[...] = l
            part_scr[...] = m
            m_scr[...] = top

            @pl.when(p > 0)
            def _():
                after(p - 1)
            return carry

        lax.fori_loop(0, n_pairs, pair, 0)
        put(n_pairs - 1, 1, normalized(acc_scr[...], l_scr[...]))
        after(n_pairs - 1)

    if not last:
        n_text = n_dev * n_txt
        assert n_text == 2 * qt

        def txt_send(head):
            for owner in range(n_dev):
                part = pl.ds(owner * n_txt, n_txt)
                if owner == 0:
                    t_rows[me, head] = tbuf[head, part, :]
                else:
                    remote(tbuf.at[head, part, :], t_rows.at[me, head], tsend_sem, trecv_sem, device(owner)).start()

        def txt_head(p):
            @pl.when(p < nh - 1)
            def _():
                for cp in load(p + 1):
                    cp.wait()

        stream(nh, lambda u: (u // 2, n_dev * n_img + lax.rem(u, 2) * qt), tbuf, txt_send, txt_head)

    def relation_of(p):
        return lax.rem(p + 1, n_dev)

    def img_tile(u):
        p = u // 2
        return p // n_dev, relation_of(p) * n_img + lax.rem(u, 2) * qt

    def img_send(p):
        head, owner = p // n_dev, relation_of(p)

        @pl.when(owner == 0)
        def _():
            o_rows[me, head] = obuf[p]

        @pl.when(owner != 0)
        def _():
            remote(obuf.at[p], o_rows.at[me, head], send_sem, recv_sem.at[head], device(owner)).start()

    def img_before(p):
        if last:
            @pl.when((relation_of(p) == 0) & (p < nh * n_dev - 1))
            def _():
                for cp in load(p // n_dev + 1):
                    cp.wait()

        @pl.when(p == 2)
        def _():
            for c in range(n_ring):
                w_copy(c).start()
            for cp in residual:
                cp.start()

    stream(nh * n_dev, img_tile, obuf, img_send, img_before)

    for cp in residual:
        cp.wait()
    others = pl.ds(0, n_dev - 1)
    if not last:
        wait_for(t_rows.at[others], trecv_sem)
    per = nc // nh
    wide = ck // LANES

    def chunk_of_w(c, carry):
        head = c // per

        @pl.when(lax.rem(c, per) == 0)
        def _():
            wait_for(o_rows.at[others, head], recv_sem.at[head])
        for t in range(wide):
            src = lax.rem(c, per) * wide + t
            if not last:
                lhs[:n_txt, head_rows(t)] = t_rows[src, head]
            lhs[R - n_img:, head_rows(t)] = o_rows[src, head]
        w_copy(c).wait()
        y_acc[...] += dot(lhs[...], w_ring[lax.rem(c, n_ring)])

        @pl.when(c + n_ring < nc)
        def _():
            w_copy(c + n_ring).start()
        return carry

    lax.fori_loop(0, nc, chunk_of_w, 0)

    gate_row = 3 * layer + 2
    gate, shift, scale = (mods_ref[r:r + 1, :] for r in range(gate_row, gate_row + 3))
    bo = bo_ref[...].astype(f32)[layer:layer + 1]
    er = R // ne
    sub = 16 if er % 16 == 0 else 8

    def put_rows(e, slot):
        rows = pl.ds(pl.multiple_of(e * er, sub), er)
        pltpu.make_async_copy(xbuf.at[rows, :], xo_hbm.at[rows, :], out_sem.at[2]).start()
        pltpu.make_async_copy(h_ring.at[slot], ho_hbm.at[rows, :], out_sem.at[slot]).start()

    def deliver(e):
        own = (z == cfg) & (e == z)

        @pl.when(own)
        def _():
            pltpu.make_async_copy(vel.at[e], vel_hbm.at[cfg], vown_sem).start()

        @pl.when(jnp.logical_not(own))
        def _():
            remote(vel.at[e], vel_hbm.at[cfg], vsend_sem.at[e], vrecv_sem.at[cfg], (z, e, core)).start()

    def rows_out(e, carry):
        slot = lax.rem(e, 2)
        if not last:
            @pl.when(e >= 2)
            def _():
                wait_for(h_ring.at[slot], out_sem.at[slot])

        def chunk(c, carry):
            rs = pl.ds(pl.multiple_of(e * er + c * sub, sub), sub)
            xn = (xbuf[rs, :].astype(f32) + gate * (y_acc[rs, :] + bo)).astype(bf)
            h_ring[slot, pl.ds(pl.multiple_of(c * sub, sub), sub), :] = ln_mod(xn.astype(f32), shift, scale)
            if not last:
                xbuf[rs, :] = xn
            return carry

        lax.fori_loop(0, er // sub, chunk, 0, unroll=3 if (er // sub) % 3 == 0 else 2)
        if last:
            w = jnp.concatenate([wf_ref[...], jnp.zeros((LANES - wf_ref.shape[0], d), bf)], axis=0)
            v = lax.dot_general(h_ring[slot], w, (((1,), (1,)), ((), ())), preferred_element_type=f32)
            b = bf_ref[...].astype(f32)
            vel[e] = v + jnp.concatenate([b, jnp.zeros((1, LANES - b.shape[1]), f32)], axis=1)
            deliver(e)
        else:
            put_rows(e, slot)
        return carry

    lax.fori_loop(0, ne, rows_out, 0)

    wait_for(o_rows.at[others], send_sem)
    if last:
        for e in range(ne):
            own = (z == cfg) & (e == z)

            @pl.when(own)
            def _():
                wait_for(vel.at[e], vown_sem)

            @pl.when(jnp.logical_not(own))
            def _():
                wait_for(vel.at[e], vsend_sem.at[e])
                wait_for(vel_hbm.at[e], vrecv_sem.at[e])
    else:
        wait_for(t_rows.at[others], tsend_sem)
        wait_for(xbuf, out_sem.at[2])
        for slot in range(2):
            wait_for(h_ring.at[slot], out_sem.at[slot])


def largest(n, cap, unit):
    return max(c for c in range(unit, cap + 1, unit) if n % c == 0)


def attend(qT, k, vT, w_out, b_out, mods, x, y_mlp, layer, n_dev, n_txt, row0, collective_id, final=None, ck=512, ne=4):
    nh, S, hd = k.shape
    R, d = y_mlp.shape
    n_img = S // n_dev - n_txt
    last = final is not None
    qt = n_img // 2
    dma = pltpu.SemaphoreType.DMA
    bf, f32 = jnp.bfloat16, jnp.float32
    hbm = pl.BlockSpec(memory_space=pl.ANY)
    stat = pltpu.VMEM((8, qt), f32)
    scratch = [pltpu.VMEM(v.shape, bf) for v in (qT, k, vT)] + [
        pltpu.VMEM((2, S, qt), f32), stat, stat, pltpu.VMEM((hd, qt), f32), stat, pltpu.VMEM((nh * n_dev, n_img, hd), bf), pltpu.VMEM((n_dev, nh, n_img, hd), bf),
        pltpu.VMEM((2, ck, d), bf), pltpu.VMEM((R, ck), bf), pltpu.VMEM((R, d), f32), pltpu.VMEM((R, d), bf), pltpu.VMEM((2, R // ne, d), bf),
        dma((nh, 3)), dma, dma((nh,)), dma((2,)), dma((2,))]
    if last:
        out_shape = jax.ShapeDtypeStruct((ne, R // ne, LANES), f32)
        scratch += [pltpu.VMEM(out_shape.shape, f32), dma, dma((ne,)), dma((ne,))]
    else:
        out_shape = [jax.ShapeDtypeStruct((R, d), bf)] * 2
        scratch += [pltpu.VMEM((nh, n_dev * n_txt, hd), bf), pltpu.VMEM((n_dev, nh, n_txt, hd), bf), dma, dma, dma((3,))]
    extra = list(final or ())
    return pl.pallas_call(
        functools.partial(attend_kernel, layer=layer, qt=qt, kc=largest(S, 768, 256), ck=ck, ne=ne, n_dev=n_dev, n_txt=n_txt, row0=row0, last=last),
        grid=(1,),
        in_specs=[hbm] * 4 + [whole(b_out.shape), whole(mods.shape)] + [whole(v.shape) for v in extra] + [hbm] * 2,
        out_specs=hbm if last else [hbm] * 2,
        out_shape=out_shape,
        scratch_shapes=scratch,
        compiler_params=params(**talking(collective_id)),
        cost_estimate=pl.CostEstimate(flops=6 * nh * n_dev * R * S * hd + 2 * R * d * d, bytes_accessed=8 * nh * S * hd + 2 * d * d + 14 * R * d, transcendentals=nh * S * n_dev * R),
        name='attend',
    )(qT, k, vT, w_out, b_out, mods, *extra, x, y_mlp)


def enter_kernel(xt_hbm, xi_hbm, cond_ref, wm_ref, wf_ref, bm_ref, bf_ref, cos_hbm, sin_hbm, w_in_hbm, mods_ref, xo_hbm, ho_hbm, tab_out, wt_hbm,
                 stage, xbuf, hbuf, cond_buf, s_scr, wbuf, turned, w_sem, wt_sem, out_sem,
                 cond_send, cond_recv, p_send, p_recv, c_send, c_recv, own_sem, t_send, t_recv, town_sem, q_send, q_recv, *, n_mod, n_steps, per_row, per_layer):
    i = pl.program_id(0)
    n, rows, d = xbuf.shape
    tp = xt_hbm.shape[0] // n
    ip = xi_hbm.shape[0] // n
    cfg, z, core = lax.axis_index('cfg'), lax.axis_index('z'), lax.axis_index('core')
    across = [related(cfg, core, r)[0] for r in range(2, 2 * n, 2)]
    heights = [lax.rem(z + s, n) for s in range(1, n)]
    plane = [(to, z, c) for to, c in (related(cfg, core, r) for r in range(1, 2 * n))]
    mine = tab_out.at[cfg * N_CORE + core]
    cut = rows // 2
    first = (cut // 2 + 7) // 8 * 8
    spans = ((0, first), (first, cut - first), (cut, first), (cut + first, cut - first))

    def piece_refs(j, dst):
        out = []
        for at, size in spans:
            head = [(xt_hbm.at[pl.ds(j * tp, tp), :], dst.at[pl.ds(0, tp), :])] if at == 0 else []
            skip = tp if at == 0 else 0
            out.append(head + [(xi_hbm.at[pl.ds(j * ip + at + skip - tp, size - skip), :], dst.at[pl.ds(at + skip, size - skip), :])])
        return out

    def tables(to):
        half = cos_hbm.shape[0]
        cols = pl.ds(pl.multiple_of(cfg * ip, ip), ip)
        return [(src.at[:, cols], to.at[pl.ds(t * half, half), :]) for t, src in enumerate((cos_hbm, sin_hbm))]

    def forward(group, t, part):
        at = pl.ds(*spans[part])

        @pl.when(group == z)
        def _():
            xbuf[z, at, :] = stage[group, at, :]

        @pl.when(group != z)
        def _():
            remote(stage.at[group, at, :], xbuf.at[z, at, :], c_send.at[t], c_recv.at[z], (cfg, group, core)).start()

    def silu_of(ref):
        v = ref[...].astype(jnp.float32)
        s_scr[...] = jnp.broadcast_to((v * jax.nn.sigmoid(v)).astype(jnp.bfloat16), s_scr.shape)

    @pl.when(i == 0)
    def _():
        meet(plane + [(cfg, h, core) for h in heights])

        @pl.when(cfg == z)
        def _():
            for t, j in enumerate(across):
                remote(cond_ref, cond_buf, cond_send.at[t], cond_recv, (j, z, core)).start()
        for part in range(len(spans)):
            for t, j in ((0, across[0]), (2, across[2]), (1, across[1])):
                for src, dst in piece_refs(j, stage.at[cfg])[part]:
                    remote(src, dst, p_send.at[t], p_recv.at[cfg, part], (j, z, core)).start()
        held = sum(piece_refs(cfg, xbuf.at[z]), [])

        @pl.when(cfg == z)
        def _():
            for src, dst in held:
                pltpu.make_async_copy(src, dst, own_sem).start()

        @pl.when(cfg != z)
        def _():
            for src, dst in held:
                remote(src, dst, c_send.at[n - 1], c_recv.at[z], (cfg, cfg, core)).start()
        for t, h in enumerate(heights):
            for src, dst in tables(mine.at[z]):
                remote(src, dst, t_send.at[t], t_recv.at[z], (cfg, h, core)).start()
        for src, dst in tables(mine.at[z]):
            pltpu.make_async_copy(src, dst, town_sem).start()

        @pl.when(cfg == z)
        def _():
            silu_of(cond_ref)

        @pl.when(cfg != z)
        def _():
            remote(cond_ref, cond_buf, cond_send.at[0], cond_recv, (cfg, z, core)).wait_recv()
            silu_of(cond_buf)

    row, col = i // per_row, lax.rem(i, per_row)
    width = wm_ref.shape[2]
    cols = pl.ds(pl.multiple_of(col * width, width), width)

    @pl.when(i < n_mod)
    def _():
        v = dot(s_scr[...], wm_ref[0])
        b = bm_ref[...].astype(jnp.float32)
        of_layer = lax.broadcasted_iota(jnp.int32, b.shape, 0) == i // per_layer
        mods_ref[pl.ds(row, 1), cols] = v[0:1] + jnp.sum(jnp.where(of_layer, b, 0.0), axis=0, keepdims=True)

    @pl.when(i >= n_mod)
    def _():
        v = dot(s_scr[...], wf_ref[...])
        mods_ref[pl.ds(row, 1), cols] = v[0:1] + bf_ref[...].astype(jnp.float32)

    def arrived(t, part):
        j = across[t]
        wait_for(stage.at[j, pl.ds(*spans[part]), :], p_recv.at[j, part])
        forward(j, t, part)

    @pl.when(i == n_steps - 2)
    def _():
        for h in heights:
            wait_for(mine.at[h], t_recv.at[h])
        wait_for(mine.at[z], town_sem)
        for peer in plane:
            remote(mine, mine, q_send, q_recv, peer).start()

    for part in range(len(spans)):
        due = 7 + 9 * part

        @pl.when(i == due)
        def _():
            arrived(0, part)

        @pl.when(i == due + 6)
        def _():
            arrived(2, part)
            arrived(1, part)

    @pl.when(i == n_steps - 1)
    def _():
        shift, scale = mods_ref[0:1, :], mods_ref[1:2, :]

        @pl.when(cfg == z)
        def _():
            wait_for(xbuf.at[z], own_sem)

        d_in, heads = w_in_hbm.shape[1] // LANES, wt_hbm.shape[1] // LANES

        def w_copy(j):
            layer, b = j // heads, lax.rem(j, heads)
            nh = heads // 3
            col = (b // nh * d_in + lax.rem(b, nh) * (d_in // nh) + cfg * N_CORE + core) * LANES
            return pltpu.make_async_copy(w_in_hbm.at[layer, :, pl.ds(pl.multiple_of(col, LANES), LANES)], wbuf.at[lax.rem(j, 2)], w_sem.at[lax.rem(j, 2)])

        def turn(j, carry):
            slot = lax.rem(j, 2)
            w_copy(j).wait()

            @pl.when(j > 1)
            def _():
                wait_for(turned.at[slot], wt_sem.at[slot])
            turned[slot] = wbuf[slot].T

            @pl.when(j + 2 < n_turns)
            def _():
                w_copy(j + 2).start()
            to = pl.ds(pl.multiple_of(lax.rem(j, heads) * LANES, LANES), LANES)
            pltpu.make_async_copy(turned.at[slot], wt_hbm.at[j // heads, to, :], wt_sem.at[slot]).start()
            return carry

        n_turns = wt_hbm.shape[0] * heads
        w_copy(0).start()
        w_copy(1).start()
        lax.fori_loop(0, n_turns, turn, 0)

        def height(s, carry):
            k = lax.rem(z + s, n)

            @pl.when(s > 0)
            def _():
                wait_for(xbuf.at[k], c_recv.at[k])
            sub = 16 if rows % 16 == 0 else 8

            def chunk(c, carry):
                at = pl.ds(pl.multiple_of(c * sub, sub), sub)
                hbuf[k, at, :] = ln_mod(xbuf[k, at, :].astype(jnp.float32), shift, scale)
                return carry

            lax.fori_loop(0, rows // sub, chunk, 0, unroll=3)
            for t, (src, dst) in enumerate(((xbuf, xo_hbm), (hbuf, ho_hbm))):
                for at, size, to in ((0, tp, k * tp), (tp, ip, n * tp + k * ip)):
                    pltpu.make_async_copy(src.at[k, pl.ds(at, size), :], dst.at[pl.ds(to, size), :], out_sem.at[t]).start()
            return carry

        lax.fori_loop(0, n, height, 0)
        for slot in range(2):
            wait_for(turned.at[slot], wt_sem.at[slot])
        wait_for(xbuf, out_sem.at[0])
        wait_for(hbuf, out_sem.at[1])

        for t, j in enumerate(across):
            wait_for(xbuf.at[0], p_send.at[t])

            @pl.when(j != z)
            def _():
                wait_for(xbuf.at[0], c_send.at[t])

        @pl.when(cfg != z)
        def _():
            wait_for(xbuf.at[0], c_send.at[n - 1])

        @pl.when(cfg == z)
        def _():
            for t, j in enumerate(across):
                remote(cond_ref, cond_buf, cond_send.at[t], cond_recv, (j, z, core)).wait_send()
        for t, h in enumerate(heights):
            wait_for(mine.at[h], t_send.at[t])
        others = tab_out.at[pl.ds(0, 2 * n - 1)]
        wait_for(others, q_send)
        wait_for(others, q_recv)


def enter(x_txt, x_img, cond, w_mod, w_fmod, b_mod, b_fmod, cosT, sinT, w_in, nh, n, collective_id, width=512):
    n_txt, d = x_txt.shape
    n_img = x_img.shape[0]
    total = n_txt + n_img
    rows = total // n
    n_layers, _, dm = w_mod.shape
    per_layer, n_fin, per_row = dm // width, w_fmod.shape[1] // width, d // width
    n_mod = n_layers * per_layer
    steps = n_mod + n_fin
    dma = pltpu.SemaphoreType.DMA
    bf, f32 = jnp.bfloat16, jnp.float32

    def layer_of(i):
        j = jnp.minimum(i, n_mod - 1)
        return j // per_layer, lax.rem(j, per_layer)

    def last_of(i):
        return 0, jnp.maximum(i - n_mod, 0)

    hbm = pl.BlockSpec(memory_space=pl.ANY)
    out_shape = [jax.ShapeDtypeStruct((steps // per_row, d), f32), jax.ShapeDtypeStruct((total, d), bf), jax.ShapeDtypeStruct((total, d), bf),
                 jax.ShapeDtypeStruct((N_CORE * n, n, 2 * cosT.shape[0], n_img // n), f32),
                 jax.ShapeDtypeStruct((n_layers, 3 * nh * LANES, d), bf)]
    return pl.pallas_call(
        functools.partial(enter_kernel, n_mod=n_mod, n_steps=steps, per_row=per_row, per_layer=per_layer),
        grid=(steps,),
        in_specs=[hbm, hbm, whole(cond.shape), pl.BlockSpec((1, d, width), lambda i: (layer_of(i)[0], 0, layer_of(i)[1])), pl.BlockSpec((d, width), last_of),
                  pl.BlockSpec((n_layers, width), lambda i: (0, layer_of(i)[1])), pl.BlockSpec((1, width), last_of), hbm, hbm, hbm],
        out_specs=[whole(out_shape[0].shape)] + [hbm] * 4,
        out_shape=out_shape,
        scratch_shapes=[pltpu.VMEM((n, rows, d), bf)] * 3 + [pltpu.VMEM(cond.shape, bf), pltpu.VMEM((16, d), bf), pltpu.VMEM((2, d, LANES), bf), pltpu.VMEM((2, LANES, d), bf),
                        dma((2,)), dma((2,)), dma((2,)), dma((n - 1,)), dma, dma((n - 1,)), dma((n, 4)), dma((n,)), dma((n,)), dma, dma((n - 1,)), dma((n,)), dma, dma, dma],
        compiler_params=params(**talking(collective_id)),
        cost_estimate=pl.CostEstimate(flops=2 * 16 * d * width * steps, bytes_accessed=2 * d * width * steps, transcendentals=0),
        name='enter',
    )(x_txt, x_img, cond, w_mod, w_fmod, b_mod, b_fmod, cosT, sinT, w_in)


def solution(mesh):
    n_cfg = mesh.devices.shape[0]
    n_z = mesh.devices.shape[1] // N_CORE
    grid = Mesh(mesh.devices.reshape(n_cfg, n_z, N_CORE), ('cfg', 'z', 'core'))
    assert n_cfg == n_z == 4
    n_dev = n_cfg * N_CORE
    token_spec = P(('cfg', 'z', 'core'), None)
    seq_spec = P(('z', 'core'), None)
    in_specs = (token_spec, token_spec, P('cfg', None), seq_spec, seq_spec, token_spec) + (P(),) * 13

    def body(x_txt, x_img, cond_vec, cos_img, sin_img, z_lat, t_cur, t_next, w_mod, b_mod, w_in, b_in, qk_gain, w_out, b_out, w_fmod, b_fmod, w_final, b_final):
        n_txt, d = x_txt.shape
        n_img = x_img.shape[0]
        n_layers = w_mod.shape[0]
        nh = d // LANES // n_dev
        n_out = w_final.shape[1]

        mods, x, h, tables, wt = enter(x_txt, x_img, cond_vec, w_mod, w_fmod, b_mod, b_fmod[None], cos_img.T, sin_img.T, w_in, nh, n_cfg, 1)
        for l in range(n_layers):
            last = l == n_layers - 1
            row0 = n_txt if last else 0
            y_mlp, _, qT, k, vT = block(h, w_in, b_in, w_out, qk_gain, tables, wt, l, n_txt, nh, row0, 2 + 2 * l)
            final = (w_final.T, b_final[None]) if last else None
            done = attend(qT, k, vT, w_out, b_out, mods, x, y_mlp, l, n_dev, n_txt, row0, 3 + 2 * l, final)
            if not last:
                x, h = done

        return z_lat + (t_next - t_cur) * done.reshape(n_img, LANES)[:, :n_out]

    return jax.shard_map(body, mesh=grid, in_specs=in_specs, out_specs=token_spec, check_vma=False)
```
